32 devices in a mesh: dp: 8 (over y, x, core), expert: 4 (over z).
Axes of the slice: x: 2, y: 2, z: 4, core: 2. Of those that a mesh axis runs over, the one named last changes fastest.
Arguments:
- grad_out: bfloat16 [4, 2048, 1024], P(None, ('dp', 'expert')), may hold values from -12 to 12
- routes: int32 [4, 2048, 8], P(None, ('dp', 'expert')), may hold values from 0 to 127, all different within a row; in each aligned block of 64 rows (0 to 63, 64 to 127, ..., all dimensions but the last counted through in order) at most 8 rows name the same one
- route_probs: bfloat16 [4, 2048, 8], P(None, ('dp', 'expert')), may hold values from 0.049804688 to 0.3984375
- dispatched: bfloat16 [4, 1024, 1024], P(None, ('dp', 'expert')), may hold values from -12 to 12, as said below
- w_gate: bfloat16 [1024, 1024], P(None, 'expert'), may hold values from -0.1875 to 0.1875
- w_up: bfloat16 [1024, 1024], P(None, 'expert'), may hold values from -0.1875 to 0.1875
- w_down: bfloat16 [1024, 1024], P('expert'), may hold values from -0.25 to 0.25
Outputs:
- grad_in: bfloat16 [4, 2048, 1024], P(None, ('dp', 'expert'))
- grad_gate: float32 [1024, 1024], P('dp', 'expert')
- grad_up: float32 [1024, 1024], P('dp', 'expert')
- grad_down_t: float32 [1024, 1024], P('dp', 'expert')
The draws below stay inside these ranges and needn't reach their ends.
Inputs may be any that keep to these rules, and one draw needn't show every extreme that they name: `routes`: in each micro-batch, among the 64 rows of one device no expert is named more than 8 times, a bound that some expert reaches in some of these blocks. `dispatched`: within each group of 4 consecutive blocks of 32 rows, blocks 2e and 2e + 1 are equal.
All inputs are finite; a program needn't handle non-finite values.
Results may differ from the reference program's by a relative error of at most 0.0058.
Values may be sent and summed in bfloat16 or wider, within the bound.
A program may use at most 64 MiB of HBM per device.

```python
import math
import jax
import jax.numpy as jnp
import numpy as np
from jax import lax

D = 1024
F = 512
NEXP = 128
TOPK = 8
MB = 4
TOK_DEV = 64
CAPS = 8
EXPERTS = 2
TOKENS = 2048
N_DP = 8
N_EXPERT = 4


def draw_dispatched(key, part):
    shape = (MB, N_DP, N_EXPERT // 2, N_EXPERT * CAPS, D)
    values = jax.random.truncated_normal(key, -4.0, 4.0, shape, jnp.float32)
    doubled = jnp.repeat(values, 2, axis=2)
    return doubled.reshape(MB, N_DP * N_EXPERT * N_EXPERT * CAPS, D).astype(jnp.bfloat16)


def levels(key, shape, shards, smallest, largest):
    gain, own = 1.0, jax.random.fold_in(key, 6)
    for dim, blocks in shards:
        steps = jnp.exp(jax.random.uniform(jax.random.fold_in(own, dim), (blocks,), jnp.float32, smallest / len(shards), largest / len(shards)))
        gain = gain * jnp.repeat(steps, shape[dim] // blocks).reshape([-1 if axis == dim else 1 for axis in range(len(shape))])
    return gain


def shared_out(rng, own, number, rows, number_of, top, limit, skew):
    sequence = jax.random.permutation(rng, number_of)
    heavy_load, ordinary = portions_of(number_of, rows * top, limit, skew, True), portions_of(number_of, rows * top, limit, skew, False)
    places = jnp.arange(number_of)

    def named(lengths, rotation):
        used = int((lengths > 0).sum())
        fixed = max(1, used // 4)
        passed = fixed + (places - fixed + rotation * (used - fixed)) % max(1, number_of - fixed)
        return jnp.zeros((number_of,), jnp.int32).at[sequence[jnp.where(places < fixed, places, passed)]].set(jnp.asarray(lengths, jnp.int32))

    lengths = jnp.where(number % 4 == 0, named(heavy_load, number // 4), named(ordinary, number - number // 4 - 1))
    mixed = jax.random.permutation(jax.random.fold_in(own, 3), number_of)
    source_of, taker = mixed[0:number_of // 2 * 2:2], mixed[1:number_of // 2 * 2:2]
    margin = jnp.minimum(lengths[source_of] - 1, limit - lengths[taker]) // 2
    margin = jnp.where((source_of == sequence[0]) | (taker == sequence[0]) | (lengths[taker] == 0), 0, jnp.maximum(margin, 0))
    passed = jax.random.randint(jax.random.fold_in(own, 4), (number_of // 2,), 0, 1 << 20) % (margin + 1)
    lengths = lengths.at[source_of].add(-passed).at[taker].add(passed)
    items = jnp.searchsorted(jnp.cumsum(lengths), jnp.arange(rows * top), side="right").astype(jnp.int32)
    table = items.reshape(top, rows).T
    table = table[jax.random.permutation(jax.random.fold_in(own, 1), rows)]
    rotation = jax.random.randint(jax.random.fold_in(own, 2), (rows, 1), 0, top)
    return jnp.take_along_axis(table, (jnp.arange(top)[None, :] + rotation) % top, axis=1)


def portions_of(count, total, reach, lean, full):
    loads = [(1 << 20) // math.isqrt(grade ** lean) + 1 for grade in range(1, count + 1)]
    largest = reach if full else min(reach, max(-(-total // count), total * loads[0] // sum(loads)))
    least = 1 if total - largest >= count - 1 else 0
    given, spare = [largest] + [least] * (count - 1), total - largest - least * (count - 1)
    while spare > 0:
        free = [i for i in range(1, count) if given[i] < largest] or [i for i in range(1, count) if given[i] < reach]
        pool, left = sum([loads[i] for i in free]), spare
        for i in free:
            addition = min(reach - given[i], max(1, left * loads[i] // pool), spare)
            given[i] = given[i] + addition
            spare = spare - addition
    return np.array(given)


def scatter_about(own_key, extent, deviation, bound, cuts=(), kind=jnp.bfloat16):
    result = jax.random.normal(own_key, extent, jnp.float32) * deviation
    if len(cuts) > 0:
        result = levels(own_key, extent, cuts, -0.22, 0.18) * result
    return jnp.clip(result, min=-bound, max=bound).astype(kind)


def setup_inputs(seed: int = 0) -> dict:
    splits = jax.random.split(jax.random.key(seed), 8)
    grad_out = scatter_about(splits[0], (MB, TOKENS, D), 3.0, 12.0, ((1, 32),))
    routes_keys = jax.random.split(jax.random.fold_in(splits[1], 1), MB * TOKENS // TOK_DEV)
    routes_turns = jax.random.permutation(jax.random.fold_in(splits[1], 3), MB * TOKENS // TOK_DEV)
    routes = jax.vmap(lambda own, number: shared_out(jax.random.fold_in(splits[1], 2), own, number, TOK_DEV, NEXP, TOPK, CAPS, 1))(routes_keys, routes_turns).reshape((MB, TOKENS, TOPK))
    route_probs = jnp.clip(0.049804688 + 0.3486328 * jax.random.uniform(splits[2], (MB, TOKENS, TOPK), jnp.float32) ** levels(splits[2], (MB, TOKENS, TOPK), ((1, 32),), -0.2, 0.2), 0.049804688, 0.3984375).astype(jnp.bfloat16)
    dispatched = draw_dispatched(jax.random.fold_in(splits[7], 71), 0)
    w_gate = scatter_about(splits[4], (D, EXPERTS * F), D ** -0.5, 0.1875, ((1, 4),))
    w_up = scatter_about(splits[5], (D, EXPERTS * F), D ** -0.5, 0.1875, ((1, 4),))
    w_down = scatter_about(splits[6], (EXPERTS * F, D), F ** -0.5, 0.25, ((0, 4),))
    return {"grad_out": grad_out, "routes": routes, "route_probs": route_probs, "dispatched": dispatched, "w_gate": w_gate, "w_up": w_up, "w_down": w_down}


def expert_backward(rows_in, row_grads, gate_mat, up_mat, down_mat):
    gate_pre = jnp.dot(rows_in, gate_mat, preferred_element_type=jnp.float32)
    up_pre = jnp.dot(rows_in, up_mat, preferred_element_type=jnp.float32)
    sigmoid = jax.nn.sigmoid(gate_pre)
    activated = gate_pre * sigmoid
    hidden = (activated * up_pre).astype(jnp.bfloat16)
    d_down = jnp.dot(row_grads.T, hidden, preferred_element_type=jnp.float32)
    dhidden = jnp.dot(row_grads, down_mat.T, preferred_element_type=jnp.float32)
    d_gate = (dhidden * up_pre * sigmoid * (1.0 + gate_pre * (1.0 - sigmoid))).astype(jnp.bfloat16)
    d_up = (dhidden * activated).astype(jnp.bfloat16)
    grad_gate_e = jnp.dot(rows_in.T, d_gate, preferred_element_type=jnp.float32)
    grad_up_e = jnp.dot(rows_in.T, d_up, preferred_element_type=jnp.float32)
    slot_grad = jnp.dot(d_gate, gate_mat.T, preferred_element_type=jnp.float32) + jnp.dot(d_up, up_mat.T, preferred_element_type=jnp.float32)
    return slot_grad, grad_gate_e, grad_up_e, d_down


def reference(grad_out, routes, route_probs, dispatched, w_gate, w_up, w_down):
    groups = N_EXPERT
    window = N_EXPERT // 2
    row_count = N_EXPERT * CAPS
    gate_blocks = w_gate.reshape(D, window, F).transpose(1, 0, 2)
    up_blocks = w_up.reshape(D, window, F).transpose(1, 0, 2)
    down_blocks = w_down.reshape(window, F, D)
    inputs = dispatched.reshape(MB * N_DP, groups, row_count, D)[:, ::2]
    out_grads = grad_out.reshape(MB * N_DP, groups * TOK_DEV, D)
    route_ids = routes.reshape(MB * N_DP, groups, TOK_DEV * TOPK)
    weights_all = route_probs.reshape(MB * N_DP, groups, TOK_DEV, TOPK)

    def group_step(totals, pieces):
        group_x, group_dy, group_ids, group_probs = pieces
        hitting = (group_ids[:, :, None] == jnp.arange(window, dtype=jnp.int32)[None, None, :]).astype(jnp.int32)
        ranking = jnp.sum((jnp.cumsum(hitting, axis=1) - 1) * hitting, axis=2)
        source = jnp.arange(groups, dtype=jnp.int32)[:, None]
        where_to = jnp.where(group_ids < window, group_ids * row_count + source * CAPS + ranking, window * row_count).astype(jnp.int32)
        scaled = (group_probs[..., None].astype(jnp.float32) * group_dy.reshape(groups, TOK_DEV, 1, D).astype(jnp.float32)).astype(jnp.bfloat16)
        buffer = jnp.zeros((window * row_count + 1, D), jnp.bfloat16).at[where_to.reshape(-1)].set(scaled.reshape(-1, D))
        slot_grads = buffer[:-1].reshape(window, row_count, D)

        def one_expert(packed):
            return expert_backward(packed[0], packed[1], packed[2], packed[3], packed[4])

        slot_grad, grad_gate_e, grad_up_e, d_down = lax.map(one_expert, (group_x, slot_grads, gate_blocks, up_blocks, down_blocks))
        padded = jnp.concatenate([slot_grad.reshape(window * row_count, D), jnp.zeros((1, D), jnp.float32)], axis=0)
        per_route = padded[where_to.reshape(-1)].reshape(groups * TOK_DEV, TOPK, D)
        grad_tokens = jnp.sum(per_route, axis=1).astype(jnp.bfloat16)
        totals = (totals[0] + grad_gate_e, totals[1] + grad_up_e, totals[2] + d_down)
        return totals, grad_tokens

    start = (jnp.zeros((window, D, F), jnp.float32), jnp.zeros((window, D, F), jnp.float32), jnp.zeros((window, D, F), jnp.float32))
    totals, grad_tokens = lax.scan(group_step, start, (inputs, out_grads, route_ids, weights_all))
    factor = 1.0 / (MB * N_DP)
    grad_gate = (totals[0] * factor).transpose(1, 0, 2).reshape(D, window * F)
    grad_up = (totals[1] * factor).transpose(1, 0, 2).reshape(D, window * F)
    grad_down_t = (totals[2] * factor).transpose(1, 0, 2).reshape(D, window * F)
    grad_in = grad_tokens.reshape(MB, N_DP * groups * TOK_DEV, D)
    return grad_in, grad_gate, grad_up, grad_down_t
```

```python
import functools

import jax
import jax.numpy as jnp
from jax import lax
from jax.experimental import pallas as pl
from jax.experimental.pallas import tpu as pltpu
from jax.sharding import PartitionSpec as P

CAPS = 8
MESH = pl.DeviceIdType.MESH
BF16 = jnp.bfloat16
F32 = jnp.float32


def dot(left, right, lc, rc):
    return lax.dot_general(
        left, right, (((lc,), (rc,)), ((), ())), preferred_element_type=F32
    )


def flipped(index, bits):
    step = 1
    while step <= bits:
        if bits & step:
            index = index + step - 2 * step * lax.rem(lax.div(index, step), 2)
        step *= 2
    return index


def kernel(
    micro,
    n_exp,
    n_dp,
    routes_ref,
    probs_ref,
    go_hbm,
    x_hbm,
    wg_hbm,
    wu_hbm,
    wd_hbm,
    gin_ref,
    gg_ref,
    gu_ref,
    gd_ref,
    go_v,
    x_v,
    wg_v,
    wu_v,
    wd_v,
    a_send,
    a_buf,
    r_send,
    r_buf,
    acc,
    p1_send,
    p1_buf,
    p2_send,
    p2_buf,
    s_all,
    h_all,
    load_sem,
    a_ssem,
    a_rsem,
    r_ssem,
    r_rsem,
    p1_ssem,
    p1_rsem,
    p2_ssem,
    p2_rsem,
    s_ssem,
    s_rsem,
    h_ssem,
    h_rsem,
):
    member = lax.axis_index("expert")
    replica = lax.axis_index("dp")
    core = lax.rem(replica, 2)
    chip = lax.div(replica, 2)
    chips = n_dp // 2
    partner = {"dp": chip * 2 + 1 - core}
    window = n_exp // 2
    tokens = go_v.shape[0]
    width = go_v.shape[1]
    tok_dev = tokens // micro
    part = micro * CAPS
    rows = n_exp * part
    row_block = width // n_dp
    gather = row_block % 128 == 0

    def member_at(k):
        return flipped(member, k)

    def chip_at(k):
        return {"dp": flipped(chip, k) * 2 + core}

    loads = [
        pltpu.make_async_copy(src, dst, load_sem.at[i])
        for i, (src, dst) in enumerate(
            ((go_hbm, go_v), (x_hbm, x_v), (wg_hbm, wg_v), (wu_hbm, wu_v), (wd_hbm, wd_v))
        )
    ]
    for load in loads:
        load.start()

    barrier = pltpu.get_barrier_semaphore()
    for k in range(1, n_exp):
        pl.semaphore_signal(
            barrier, inc=1, device_id={"expert": member_at(k)}, device_id_type=MESH
        )
    for k in range(1, n_dp):
        pl.semaphore_signal(
            barrier, inc=1, device_id={"dp": flipped(replica, k)}, device_id_type=MESH
        )

    ids = jnp.concatenate([routes_ref[m] for m in range(micro)], axis=1)
    probs = jnp.concatenate([probs_ref[m].astype(F32) for m in range(micro)], axis=1)
    pad = max(window, 8)
    expert_row = lax.broadcasted_iota(jnp.int32, (pad, tokens), 0)
    hits, weights = [], []
    table = jnp.zeros((pad, tokens), F32)
    for e in range(window):
        named = ids == e
        hits.append(jnp.sum(jnp.where(named, 1.0, 0.0), axis=0, keepdims=True))
        weights.append(jnp.sum(jnp.where(named, probs, 0.0), axis=0, keepdims=True))
        table = jnp.where(expert_row == e, hits[e], table)
    ti = lax.broadcasted_iota(jnp.int32, (tokens, tokens), 0)
    tj = lax.broadcasted_iota(jnp.int32, (tokens, tokens), 1)
    earlier = jnp.where((ti < tj) & (lax.div(ti, tok_dev) == lax.div(tj, tok_dev)), 1.0, 0.0)
    ranking = dot(table.astype(BF16), earlier.astype(BF16), 1, 0)
    slot = lax.broadcasted_iota(jnp.int32, (CAPS, tokens), 0).astype(F32)
    batch = lax.div(lax.broadcasted_iota(jnp.int32, (CAPS, tokens), 1), tok_dev)
    ones, scales = [], []
    for h in range(n_exp):
        e = h // 2
        chosen = (hits[e] > 0.5) & (ranking[e : e + 1] == slot)
        for m in range(micro):
            here = chosen & (batch == m)
            ones.append(jnp.where(here, 1.0, 0.0))
            scales.append(jnp.where(here, weights[e], 0.0))
    mixing = jnp.concatenate(ones, axis=0).astype(BF16)
    picking = jnp.concatenate(scales, axis=0).astype(BF16)

    loads[0].wait()
    sending = dot(picking, go_v[...], 1, 0).astype(BF16)
    for h in range(n_exp):
        a_send[h] = sending[h * part : (h + 1) * part]
    pl.semaphore_wait(barrier, n_exp - 1 + n_dp - 1)
    def a_copy(k, src, slot, to):
        return pltpu.make_async_remote_copy(
            src_ref=src,
            dst_ref=a_buf.at[slot],
            send_sem=a_ssem.at[k - 1],
            recv_sem=a_rsem.at[k - 1],
            device_id={"expert": to},
            device_id_type=MESH,
        )

    a_copies = {}
    for k in range(1, n_exp):
        a_copies[k] = a_copy(k, a_send.at[member_at(k)], member, member_at(k))
        a_copies[k].start()
    a_buf[member] = a_send[member]

    loads[1].wait()
    ri = lax.broadcasted_iota(jnp.int32, (rows, rows), 0)
    rj = lax.broadcasted_iota(jnp.int32, (rows, rows), 1)
    wanted = (
        lax.rem(lax.div(ri, CAPS), micro) * (n_exp * CAPS)
        + lax.div(ri, part) * CAPS
        + lax.rem(ri, CAPS)
    )
    inputs = dot(jnp.where(rj == wanted, 1.0, 0.0).astype(BF16), x_v[...], 1, 0).astype(BF16)
    loads[2].wait()
    gate = dot(inputs, wg_v[...], 1, 0)
    loads[3].wait()
    up = dot(inputs, wu_v[...], 1, 0)
    sigmoid = jax.nn.sigmoid(gate)
    activated = gate * sigmoid
    hidden = (activated * up).astype(BF16)
    h_copies, s_copies = [], []
    if gather:
        h_all[replica] = hidden
        for k in range(n_dp - 1, 0, -1):
            copy = pltpu.make_async_remote_copy(
                src_ref=h_all.at[replica],
                dst_ref=h_all.at[replica],
                send_sem=h_ssem.at[k - 1],
                recv_sem=h_rsem.at[k - 1],
                device_id={"dp": flipped(replica, k)},
                device_id_type=MESH,
            )
            copy.start()
            h_copies.append(copy)
    slope = up * sigmoid * (1.0 + gate * (1.0 - sigmoid))
    loads[4].wait()

    def p1_copy(o):
        return pltpu.make_async_remote_copy(
            src_ref=p1_send.at[o, 1 - core],
            dst_ref=p1_buf.at[o],
            send_sem=p1_ssem.at[o],
            recv_sem=p1_rsem.at[o],
            device_id=partner,
            device_id_type=MESH,
        )

    def store_terms(o, value):
        for d in range(n_dp):
            block = value[d * row_block : (d + 1) * row_block]
            acc[o, d % 2, d // 2] = block
            p1_send[o, d % 2, d // 2] = block.astype(BF16)

    p1_copies, p2_copies = {}, {}

    def start_p1(o, value):
        store_terms(o, value)
        p1_copies[o] = p1_copy(o)
        p1_copies[o].start()

    def start_p2(o):
        p1_copies[o].wait_recv()
        for k in range(chips - 1, 0, -1):
            q = flipped(chip, k)
            p2_send[o, q] = (acc[o, core, q] + p1_buf[o, q].astype(F32)).astype(BF16)
            copy = pltpu.make_async_remote_copy(
                src_ref=p2_send.at[o, q],
                dst_ref=p2_buf.at[o, k - 1],
                send_sem=p2_ssem.at[o, k - 1],
                recv_sem=p2_rsem.at[o, k - 1],
                device_id=chip_at(k),
                device_id_type=MESH,
            )
            copy.start()
            p2_copies[o, k] = copy

    for k in range(1, n_exp):
        a_copies[k].wait_recv()
    scaled = a_buf[...].reshape(rows, width)
    if gather:
        for k in range(n_dp - 1, 0, -1):
            peer = flipped(replica, k)
            columns = pl.ds(pl.multiple_of(peer * row_block, row_block), row_block)
            copy = pltpu.make_async_remote_copy(
                src_ref=a_buf.at[:, :, columns],
                dst_ref=s_all.at[replica],
                send_sem=s_ssem.at[k - 1],
                recv_sem=s_rsem.at[k - 1],
                device_id={"dp": peer},
                device_id_type=MESH,
            )
            copy.start()
            s_copies.append(copy)
    else:
        start_p1(0, dot(scaled, hidden, 0, 0))
    dhidden = dot(scaled, wd_v[...], 1, 1)
    d_gate = (dhidden * slope).astype(BF16)
    d_up = (dhidden * activated).astype(BF16)
    returning = (dot(d_gate, wg_v[...], 1, 1) + dot(d_up, wu_v[...], 1, 1)).astype(BF16)
    for h in range(n_exp):
        r_send[h] = returning[h * part : (h + 1) * part]
    r_copies = []
    for k in range(n_exp - 1, 0, -1):
        copy = pltpu.make_async_remote_copy(
            src_ref=r_send.at[member_at(k)],
            dst_ref=r_buf.at[member],
            send_sem=r_ssem.at[k - 1],
            recv_sem=r_rsem.at[k - 1],
            device_id={"expert": member_at(k)},
            device_id_type=MESH,
        )
        copy.start()
        r_copies.append(copy)
    start_p1(1, dot(inputs, d_gate, 0, 0))
    start_p1(2, dot(inputs, d_up, 0, 0))
    if not gather:
        start_p2(0)
    r_buf[member] = r_send[member]
    start_p2(1)
    start_p2(2)

    if gather:
        own = pl.ds(pl.multiple_of(replica * row_block, row_block), row_block)
        s_all[replica] = a_buf[:, :, own]
        for copy in h_copies + s_copies:
            copy.wait_recv()
        slots = n_dp * rows
        down = dot(
            s_all[...].reshape(slots, row_block), h_all[...].reshape(slots, wg_v.shape[1]), 0, 0
        )
        gd_ref[...] = down * (1.0 / (micro * n_dp))
    for copy in r_copies:
        copy.wait_recv()
    gin_ref[...] = dot(mixing, r_buf[...].reshape(rows, width), 0, 0).astype(BF16)

    factor = 1.0 / (micro * n_dp)
    for o, out in enumerate((gd_ref, gg_ref, gu_ref)):
        if o not in p1_copies:
            continue
        total = acc[o, core, chip] + p1_buf[o, chip].astype(F32)
        for k in range(chips - 1, 0, -1):
            p2_copies[o, k].wait_recv()
            total = total + p2_buf[o, k - 1].astype(F32)
        out[...] = total * factor
    started = [*a_copies.values(), *p1_copies.values(), *p2_copies.values()]
    for copy in started + r_copies + h_copies + s_copies:
        copy.wait_send()


def pooled_kernel(
    micro,
    n_exp,
    n_dp,
    routes_hbm,
    probs_hbm,
    go_hbm,
    x_hbm,
    wg_hbm,
    wu_hbm,
    wd_hbm,
    gin_ref,
    gg_ref,
    gu_ref,
    gd_ref,
    routes_v,
    probs_v,
    go_v,
    x_v,
    x_par,
    xt_v,
    wg_v,
    wu_v,
    wd_v,
    a_send,
    a_buf,
    r_send,
    r_buf,
    mix_v,
    d_all,
    relay_send,
    relay_buf,
    last_send,
    last_buf,
    s_all,
    h_all,
    down_v,
    down_buf,
    load_sem,
    a_ssem,
    a_rsem,
    r_ssem,
    r_rsem,
    x_sem,
    d_sem,
    relay_ssem,
    relay_rsem,
    last_ssem,
    last_rsem,
    s_ssem,
    s_rsem,
    h_ssem,
    h_rsem,
    down_sem,
):
    member = lax.axis_index("expert")
    replica = lax.axis_index("dp")
    core = lax.rem(replica, 2)
    chip = lax.div(replica, 2)
    chips = n_dp // 2
    partner = {"dp": chip * 2 + 1 - core}
    window = n_exp // 2
    tokens, width = go_v.shape
    cols = wg_v.shape[1]
    tok_dev = tokens // micro
    part = micro * CAPS
    rows = n_exp * part
    row_block = width // n_dp
    pair_block = 2 * row_block
    hops = range(chips - 1, 0, -1)

    loads = [
        pltpu.make_async_copy(src, dst, load_sem.at[i])
        for i, (src, dst) in enumerate(
            (
                (routes_hbm, routes_v),
                (probs_hbm, probs_v),
                (go_hbm, go_v),
                *((x_hbm.at[m], x_v.at[:, pl.ds(m * CAPS, CAPS), :]) for m in range(micro)),
                (wg_hbm, wg_v),
                (wu_hbm, wu_v),
                (wd_hbm, wd_v),
            )
        )
    ]
    for load in loads:
        load.start()

    def chip_at(k):
        return flipped(chip, k)

    def peer_at(k):
        return {"dp": chip_at(k) * 2 + core}

    barrier = pltpu.get_barrier_semaphore()
    for k in range(1, n_exp):
        pl.semaphore_signal(
            barrier, inc=1, device_id={"expert": flipped(member, k)}, device_id_type=MESH
        )
    for k in hops:
        pl.semaphore_signal(barrier, inc=1, device_id=peer_at(k), device_id_type=MESH)
    pl.semaphore_signal(barrier, inc=1, device_id=partner, device_id_type=MESH)

    started = []

    def remote(src, dst, send_sem, recv_sem, device):
        copy = pltpu.make_async_remote_copy(
            src_ref=src,
            dst_ref=dst,
            send_sem=send_sem,
            recv_sem=recv_sem,
            device_id=device,
            device_id_type=MESH,
        )
        copy.start()
        started.append(copy)
        return copy

    pad = max(window, 8)
    expert_row = lax.broadcasted_iota(jnp.int32, (pad, tokens), 0)
    ti = lax.broadcasted_iota(jnp.int32, (tokens, tokens), 0)
    tj = lax.broadcasted_iota(jnp.int32, (tokens, tokens), 1)
    earlier = jnp.where((ti < tj) & (lax.div(ti, tok_dev) == lax.div(tj, tok_dev)), 1.0, 0.0)
    loads[0].wait()
    loads[1].wait()
    ids = jnp.concatenate([routes_v[m] for m in range(micro)], axis=1)
    probs = jnp.concatenate([probs_v[m].astype(F32) for m in range(micro)], axis=1)
    hits, weights = [], []
    table = jnp.zeros((pad, tokens), F32)
    for e in range(window):
        named = ids == e
        hits.append(jnp.sum(jnp.where(named, 1.0, 0.0), axis=0, keepdims=True))
        weights.append(jnp.sum(jnp.where(named, probs, 0.0), axis=0, keepdims=True))
        table = jnp.where(expert_row == e, hits[e], table)
    ranking = dot(table.astype(BF16), earlier.astype(BF16), 1, 0)
    slot = lax.broadcasted_iota(jnp.int32, (CAPS, tokens), 0).astype(F32)
    batch = lax.div(lax.broadcasted_iota(jnp.int32, (CAPS, tokens), 1), tok_dev)
    ones, scales = [], []
    for e in range(window):
        chosen = (hits[e] > 0.5) & (ranking[e : e + 1] == slot)
        for m in range(micro):
            here = chosen & (batch == m)
            ones.append(jnp.where(here, 1.0, 0.0))
            scales.append(jnp.where(here, weights[e], 0.0))
    picking = jnp.concatenate(scales, axis=0).astype(BF16)

    loads[2].wait()
    sending = dot(picking, go_v[...], 1, 0).astype(BF16)
    for e in range(window):
        a_send[e] = sending[e * part : (e + 1) * part]
    pl.semaphore_wait(barrier, n_exp - 1 + chips)

    order = [flipped(member, k) for k in range(n_exp - 1, 0, -1)]
    nearest = order[::-1]
    for j, to in enumerate(order):
        remote(
            a_send.at[lax.div(to, 2)],
            a_buf.at[member],
            a_ssem.at[j],
            a_rsem.at[member],
            {"expert": to},
        )
    a_buf[member] = a_send[lax.div(member, 2)]

    def a_arrival(source):
        return pltpu.make_async_remote_copy(
            src_ref=a_send.at[0],
            dst_ref=a_buf.at[source],
            send_sem=a_ssem.at[0],
            recv_sem=a_rsem.at[source],
            device_id={"expert": source},
            device_id_type=MESH,
        )

    for m in range(micro):
        loads[3 + m].wait()
    x_copy = remote(x_v, x_par, x_sem.at[0], x_sem.at[1], partner)

    inputs = x_v[...].reshape(rows, width)
    loads[3 + micro].wait()
    gate = dot(inputs, wg_v[...], 1, 0)
    loads[4 + micro].wait()
    up = dot(inputs, wu_v[...], 1, 0)
    sigmoid = jax.nn.sigmoid(gate)
    activated = gate * sigmoid
    h_all[chip] = (activated * up).astype(BF16)
    h_copies = {
        k: remote(
            h_all.at[chip], h_all.at[chip], h_ssem.at[k - 1], h_rsem.at[k - 1], peer_at(k)
        )
        for k in hops
    }
    slope = up * sigmoid * (1.0 + gate * (1.0 - sigmoid))

    def blocks(q):
        return pl.ds(pl.multiple_of(q * pair_block, pair_block), pair_block)

    def send_slices(source, j):
        for k in hops:
            remote(
                a_buf.at[source, :, blocks(chip_at(k))],
                s_all.at[chip, source],
                s_ssem.at[j, k - 1],
                s_rsem.at[k - 1],
                peer_at(k),
            )

    send_slices(member, 0)

    mix_v[...] = jnp.concatenate(
        [jnp.concatenate(ones[e * micro : (e + 1) * micro], axis=0) for e in range(window) for _ in range(2)],
        axis=0,
    ).astype(BF16)
    loads[5 + micro].wait()
    x_copy.wait_recv()
    for k in range(chips):
        q = chip_at(k) if k else chip
        own = pl.ds(pl.multiple_of((q * 2 + core) * row_block, row_block), row_block)
        mine = x_v[:, :, own].reshape(rows, row_block)
        other = x_par[:, :, own].reshape(rows, row_block)
        xt_v[k] = jnp.concatenate([mine, other], axis=0).T

    for j, source in enumerate(nearest):
        a_arrival(source).wait_recv()
        if j < n_exp - 2:
            send_slices(source, j + 1)
    scaled = a_buf[...].reshape(rows, width)
    dhidden = dot(scaled, wd_v[...], 1, 1)
    d_gate = (dhidden * slope).astype(BF16)
    d_up = (dhidden * activated).astype(BF16)
    d_all[0, :, :cols] = d_gate
    d_all[0, :, cols:] = d_up
    d_copy = remote(d_all.at[0], d_all.at[1], d_sem.at[0], d_sem.at[1], partner)
    send_slices(nearest[-1], n_exp - 1)

    returning = (dot(d_gate, wg_v[...], 1, 1) + dot(d_up, wu_v[...], 1, 1)).astype(BF16)
    for h in range(n_exp):
        r_send[h] = returning[h * part : (h + 1) * part]
    r_copies = [
        remote(
            r_send.at[to], r_buf.at[member], r_ssem.at[k - 1], r_rsem.at[k - 1], {"expert": to}
        )
        for k, to in zip(range(n_exp - 1, 0, -1), order)
    ]

    d_copy.wait_recv()
    factors = d_all[...].reshape(2 * rows, 2 * cols)
    far = dot(xt_v[3], factors, 1, 0).astype(BF16)
    relays = []
    for i, k in enumerate((1, 2)):
        relay_send[i] = far[:, i * cols : (i + 1) * cols]
        relays.append(
            remote(
                relay_send.at[i],
                relay_buf.at[i],
                relay_ssem.at[i],
                relay_rsem.at[i],
                peer_at(k),
            )
        )

    def send_last(i, k, value):
        last_send[i] = value.astype(BF16)
        return remote(
            last_send.at[i], last_buf.at[i], last_ssem.at[i], last_rsem.at[i], peer_at(k)
        )

    near = [dot(xt_v[k], factors, 1, 0) for k in (1, 2)]
    last_copies = [
        send_last(0, 1, near[0][:, :cols]),
        send_last(1, 2, near[1][:, cols:]),
    ]
    total = dot(xt_v[0], factors, 1, 0)
    r_buf[member] = r_send[member]
    s_all[chip] = a_buf[:, :, blocks(chip)]
    relays[0].wait_recv()
    last_copies.append(send_last(2, 2, near[1][:, :cols] + relay_buf[0].astype(F32)))
    relays[1].wait_recv()
    last_copies.append(send_last(3, 1, near[0][:, cols:] + relay_buf[1].astype(F32)))
    for k in hops:
        h_copies[k].wait_recv()
        pltpu.make_async_remote_copy(
            src_ref=s_all.at[chip],
            dst_ref=s_all.at[chip_at(k)],
            send_sem=s_ssem.at[0, k - 1],
            recv_sem=s_rsem.at[k - 1],
            device_id=peer_at(k),
            device_id_type=MESH,
        ).wait_recv()
    slots = chips * rows
    down = dot(s_all[...].reshape(slots, pair_block), h_all[...].reshape(slots, cols), 0, 0)
    down_v[0] = down[:row_block]
    down_v[1] = down[row_block:]
    down_copy = remote(down_v.at[1 - core], down_buf, down_sem.at[0], down_sem.at[1], partner)

    for copy in r_copies:
        copy.wait_recv()
    gin_ref[...] = dot(mix_v[...], r_buf[...].reshape(rows, width), 0, 0).astype(BF16)

    factor = 1.0 / (micro * n_dp)
    down_copy.wait_recv()
    gd_ref[...] = (down_v[core] + down_buf[...]) * factor
    for copy in last_copies:
        copy.wait_recv()
    gates = total[:, :cols] + last_buf[0].astype(F32) + last_buf[2].astype(F32)
    ups = total[:, cols:] + last_buf[1].astype(F32) + last_buf[3].astype(F32)
    gg_ref[...] = gates * factor
    gu_ref[...] = ups * factor
    for copy in started:
        copy.wait_send()


def settle(*refs):
    count = len(refs) // 2
    sem = refs[-1]
    copies = [
        pltpu.make_async_copy(refs[i], refs[count + i], sem.at[i]) for i in range(count)
    ]
    for copy in copies:
        copy.start()
    for copy in copies:
        copy.wait()


def settled(arrays):
    anywhere = pl.BlockSpec(memory_space=pl.ANY)
    return pl.pallas_call(
        settle,
        out_shape=tuple(jax.ShapeDtypeStruct(a.shape, a.dtype) for a in arrays),
        in_specs=[pl.BlockSpec(memory_space=pltpu.VMEM)] * len(arrays),
        out_specs=(anywhere,) * len(arrays),
        scratch_shapes=[pltpu.SemaphoreType.DMA((len(arrays),))],
    )(*[pltpu.with_memory_space_constraint(a, pltpu.VMEM) for a in arrays])


def pooled_call(n_exp, n_dp, grad_out, routes, route_probs, dispatched, w_gate, w_up, w_down):
    micro, tok_dev, width = grad_out.shape
    cols = w_gate.shape[1]
    tokens = micro * tok_dev
    part = micro * CAPS
    rows = n_exp * part
    chips = n_dp // 2
    row_block = width // n_dp
    vmem = pl.BlockSpec(memory_space=pltpu.VMEM)
    hbm = pl.BlockSpec(memory_space=pl.ANY)
    grad = pltpu.VMEM((row_block, cols), F32)
    dma = pltpu.SemaphoreType.DMA
    return pl.pallas_call(
        functools.partial(pooled_kernel, micro, n_exp, n_dp),
        out_shape=(pltpu.VMEM((tokens, width), BF16), grad, grad, grad),
        in_specs=[hbm] * 7,
        out_specs=(vmem, vmem, vmem, vmem),
        scratch_shapes=[
            pltpu.VMEM((micro, routes.shape[2], tok_dev), jnp.int32),
            pltpu.VMEM((micro, routes.shape[2], tok_dev), BF16),
            pltpu.VMEM((tokens, width), BF16),
            pltpu.VMEM((n_exp, part, width), BF16),
            pltpu.VMEM((n_exp, part, width), BF16),
            pltpu.VMEM((chips, row_block, 2 * rows), BF16),
            pltpu.VMEM((width, cols), BF16),
            pltpu.VMEM((width, cols), BF16),
            pltpu.VMEM((cols, width), BF16),
            pltpu.VMEM((n_exp // 2, part, width), BF16),
            pltpu.VMEM((n_exp, part, width), BF16),
            pltpu.VMEM((n_exp, part, width), BF16),
            pltpu.VMEM((n_exp, part, width), BF16),
            pltpu.VMEM((rows, tokens), BF16),
            pltpu.VMEM((2, rows, 2 * cols), BF16),
            pltpu.VMEM((2, row_block, cols), BF16),
            pltpu.VMEM((2, row_block, cols), BF16),
            pltpu.VMEM((4, row_block, cols), BF16),
            pltpu.VMEM((4, row_block, cols), BF16),
            pltpu.VMEM((chips, n_exp, part, 2 * row_block), BF16),
            pltpu.VMEM((chips, rows, cols), BF16),
            pltpu.VMEM((2, row_block, cols), F32),
            pltpu.VMEM((row_block, cols), F32),
            dma((6 + micro,)),
            dma((n_exp - 1,)),
            dma((n_exp,)),
            dma((n_exp - 1,)),
            dma((n_exp - 1,)),
            dma((2,)),
            dma((2,)),
            dma((2,)),
            dma((2,)),
            dma((4,)),
            dma((4,)),
            dma((n_exp, chips - 1)),
            dma((chips - 1,)),
            dma((chips - 1,)),
            dma((chips - 1,)),
            dma((2,)),
        ],
        compiler_params=pltpu.CompilerParams(collective_id=0, has_side_effects=True),
    )(
        routes.transpose(0, 2, 1),
        route_probs.transpose(0, 2, 1),
        grad_out.reshape(tokens, width),
        dispatched.reshape(micro, n_exp, CAPS, width),
        w_gate,
        w_up,
        w_down,
    )


def spread_call(n_exp, n_dp, grad_out, routes, route_probs, dispatched, w_gate, w_up, w_down):
    micro, tok_dev, width = grad_out.shape
    cols = w_gate.shape[1]
    tokens = micro * tok_dev
    part = micro * CAPS
    rows = n_exp * part
    chips = n_dp // 2
    row_block = width // n_dp
    vmem = pl.BlockSpec(memory_space=pltpu.VMEM)
    hbm = pl.BlockSpec(memory_space=pl.ANY)
    grad = pltpu.VMEM((row_block, cols), F32)
    dma = pltpu.SemaphoreType.DMA
    others = max(chips - 1, 1)
    gather = row_block % 128 == 0
    return pl.pallas_call(
        functools.partial(kernel, micro, n_exp, n_dp),
        out_shape=(pltpu.VMEM((tokens, width), BF16), grad, grad, grad),
        in_specs=[vmem, vmem, hbm, hbm, hbm, hbm, hbm],
        out_specs=(vmem, vmem, vmem, vmem),
        scratch_shapes=[
            pltpu.VMEM((tokens, width), BF16),
            pltpu.VMEM((rows, width), BF16),
            pltpu.VMEM((width, cols), BF16),
            pltpu.VMEM((width, cols), BF16),
            pltpu.VMEM((cols, width), BF16),
            pltpu.VMEM((n_exp, part, width), BF16),
            pltpu.VMEM((n_exp, part, width), BF16),
            pltpu.VMEM((n_exp, part, width), BF16),
            pltpu.VMEM((n_exp, part, width), BF16),
            pltpu.VMEM((3, 2, chips, row_block, cols), F32),
            pltpu.VMEM((3, 2, chips, row_block, cols), BF16),
            pltpu.VMEM((3, chips, row_block, cols), BF16),
            pltpu.VMEM((3, chips, row_block, cols), BF16),
            pltpu.VMEM((3, others, row_block, cols), BF16),
            pltpu.VMEM((n_dp, n_exp, part, row_block) if gather else (8, 128), BF16),
            pltpu.VMEM((n_dp, rows, cols) if gather else (8, 128), BF16),
            dma((5,)),
            dma((n_exp - 1,)),
            dma((n_exp - 1,)),
            dma((n_exp - 1,)),
            dma((n_exp - 1,)),
            dma((3,)),
            dma((3,)),
            dma((3, others)),
            dma((3, others)),
            dma((n_dp - 1,)),
            dma((n_dp - 1,)),
            dma((n_dp - 1,)),
            dma((n_dp - 1,)),
        ],
        compiler_params=pltpu.CompilerParams(collective_id=0, has_side_effects=True),
    )(
        routes.transpose(0, 2, 1),
        route_probs.transpose(0, 2, 1),
        grad_out.reshape(tokens, width),
        dispatched.reshape(rows, width),
        w_gate,
        w_up,
        w_down,
    )


def per_device(n_exp, n_dp, grad_out, *rest):
    pooled = n_exp == 4 and n_dp == 8 and (grad_out.shape[2] // n_dp) % 128 == 0
    call = pooled_call if pooled else spread_call
    out = settled(call(n_exp, n_dp, grad_out, *rest))
    return (out[0].reshape(grad_out.shape),) + tuple(out[1:])


def solution(mesh):
    return jax.shard_map(
        functools.partial(per_device, mesh.shape["expert"], mesh.shape["dp"]),
        mesh=mesh,
        in_specs=(
            P(None, ("dp", "expert"), None),
            P(None, ("dp", "expert"), None),
            P(None, ("dp", "expert"), None),
            P(None, ("dp", "expert"), None),
            P(None, "expert"),
            P(None, "expert"),
            P("expert", None),
        ),
        out_specs=(
            P(None, ("dp", "expert"), None),
            P("dp", "expert"),
            P("dp", "expert"),
            P("dp", "expert"),
        ),
        check_vma=False,
    )
```

```python
import functools

import jax
import jax.numpy as jnp
from jax import lax
from jax.experimental import pallas as pl
from jax.experimental.pallas import tpu as pltpu
from jax.sharding import PartitionSpec as P

CAPS = 8
MESH = pl.DeviceIdType.MESH
BF16 = jnp.bfloat16
F32 = jnp.float32


def dot(left, right, lc, rc):
    return lax.dot_general(
        left, right, (((lc,), (rc,)), ((), ())), preferred_element_type=F32
    )


def flipped(index, bits):
    step = 1
    while step <= bits:
        if bits & step:
            index = index + step - 2 * step * lax.rem(lax.div(index, step), 2)
        step *= 2
    return index


def kernel(
    micro,
    n_exp,
    n_dp,
    routes_ref,
    probs_ref,
    go_hbm,
    x_hbm,
    wg_hbm,
    wu_hbm,
    wd_hbm,
    gin_ref,
    gg_ref,
    gu_ref,
    gd_ref,
    go_v,
    x_v,
    wg_v,
    wu_v,
    wd_v,
    a_send,
    a_buf,
    r_send,
    r_buf,
    acc,
    p1_send,
    p1_buf,
    p2_send,
    p2_buf,
    s_all,
    h_all,
    load_sem,
    a_ssem,
    a_rsem,
    r_ssem,
    r_rsem,
    p1_ssem,
    p1_rsem,
    p2_ssem,
    p2_rsem,
    s_ssem,
    s_rsem,
    h_ssem,
    h_rsem,
):
    member = lax.axis_index("expert")
    replica = lax.axis_index("dp")
    core = lax.rem(replica, 2)
    chip = lax.div(replica, 2)
    chips = n_dp // 2
    partner = {"dp": chip * 2 + 1 - core}
    window = n_exp // 2
    tokens = go_v.shape[0]
    width = go_v.shape[1]
    tok_dev = tokens // micro
    part = micro * CAPS
    rows = n_exp * part
    row_block = width // n_dp
    gather = row_block % 128 == 0

    def member_at(k):
        return flipped(member, k)

    def chip_at(k):
        return {"dp": flipped(chip, k) * 2 + core}

    loads = [
        pltpu.make_async_copy(src, dst, load_sem.at[i])
        for i, (src, dst) in enumerate(
            ((go_hbm, go_v), (x_hbm, x_v), (wg_hbm, wg_v), (wu_hbm, wu_v), (wd_hbm, wd_v))
        )
    ]
    for load in loads:
        load.start()

    barrier = pltpu.get_barrier_semaphore()
    for k in range(1, n_exp):
        pl.semaphore_signal(
            barrier, inc=1, device_id={"expert": member_at(k)}, device_id_type=MESH
        )
    for k in range(1, n_dp):
        pl.semaphore_signal(
            barrier, inc=1, device_id={"dp": flipped(replica, k)}, device_id_type=MESH
        )

    ids = jnp.concatenate([routes_ref[m] for m in range(micro)], axis=1)
    probs = jnp.concatenate([probs_ref[m].astype(F32) for m in range(micro)], axis=1)
    pad = max(window, 8)
    expert_row = lax.broadcasted_iota(jnp.int32, (pad, tokens), 0)
    hits, weights = [], []
    table = jnp.zeros((pad, tokens), F32)
    for e in range(window):
        named = ids == e
        hits.append(jnp.sum(jnp.where(named, 1.0, 0.0), axis=0, keepdims=True))
        weights.append(jnp.sum(jnp.where(named, probs, 0.0), axis=0, keepdims=True))
        table = jnp.where(expert_row == e, hits[e], table)
    ti = lax.broadcasted_iota(jnp.int32, (tokens, tokens), 0)
    tj = lax.broadcasted_iota(jnp.int32, (tokens, tokens), 1)
    earlier = jnp.where((ti < tj) & (lax.div(ti, tok_dev) == lax.div(tj, tok_dev)), 1.0, 0.0)
    ranking = dot(table.astype(BF16), earlier.astype(BF16), 1, 0)
    slot = lax.broadcasted_iota(jnp.int32, (CAPS, tokens), 0).astype(F32)
    batch = lax.div(lax.broadcasted_iota(jnp.int32, (CAPS, tokens), 1), tok_dev)
    ones, scales = [], []
    for h in range(n_exp):
        e = h // 2
        chosen = (hits[e] > 0.5) & (ranking[e : e + 1] == slot)
        for m in range(micro):
            here = chosen & (batch == m)
            ones.append(jnp.where(here, 1.0, 0.0))
            scales.append(jnp.where(here, weights[e], 0.0))
    mixing = jnp.concatenate(ones, axis=0).astype(BF16)
    picking = jnp.concatenate(scales, axis=0).astype(BF16)

    loads[0].wait()
    sending = dot(picking, go_v[...], 1, 0).astype(BF16)
    for h in range(n_exp):
        a_send[h] = sending[h * part : (h + 1) * part]
    pl.semaphore_wait(barrier, n_exp - 1 + n_dp - 1)
    def a_copy(k, src, slot, to):
        return pltpu.make_async_remote_copy(
            src_ref=src,
            dst_ref=a_buf.at[slot],
            send_sem=a_ssem.at[k - 1],
            recv_sem=a_rsem.at[k - 1],
            device_id={"expert": to},
            device_id_type=MESH,
        )

    a_copies = {}
    for k in range(1, n_exp):
        a_copies[k] = a_copy(k, a_send.at[member_at(k)], member, member_at(k))
        a_copies[k].start()
    a_buf[member] = a_send[member]

    loads[1].wait()
    ri = lax.broadcasted_iota(jnp.int32, (rows, rows), 0)
    rj = lax.broadcasted_iota(jnp.int32, (rows, rows), 1)
    wanted = (
        lax.rem(lax.div(ri, CAPS), micro) * (n_exp * CAPS)
        + lax.div(ri, part) * CAPS
        + lax.rem(ri, CAPS)
    )
    inputs = dot(jnp.where(rj == wanted, 1.0, 0.0).astype(BF16), x_v[...], 1, 0).astype(BF16)
    loads[2].wait()
    gate = dot(inputs, wg_v[...], 1, 0)
    loads[3].wait()
    up = dot(inputs, wu_v[...], 1, 0)
    sigmoid = jax.nn.sigmoid(gate)
    activated = gate * sigmoid
    hidden = (activated * up).astype(BF16)
    h_copies, s_copies = [], []
    if gather:
        h_all[replica] = hidden
        for k in range(n_dp - 1, 0, -1):
            copy = pltpu.make_async_remote_copy(
                src_ref=h_all.at[replica],
                dst_ref=h_all.at[replica],
                send_sem=h_ssem.at[k - 1],
                recv_sem=h_rsem.at[k - 1],
                device_id={"dp": flipped(replica, k)},
                device_id_type=MESH,
            )
            copy.start()
            h_copies.append(copy)
    slope = up * sigmoid * (1.0 + gate * (1.0 - sigmoid))
    loads[4].wait()

    def p1_copy(o):
        return pltpu.make_async_remote_copy(
            src_ref=p1_send.at[o, 1 - core],
            dst_ref=p1_buf.at[o],
            send_sem=p1_ssem.at[o],
            recv_sem=p1_rsem.at[o],
            device_id=partner,
            device_id_type=MESH,
        )

    def store_terms(o, value):
        for d in range(n_dp):
            block = value[d * row_block : (d + 1) * row_block]
            acc[o, d % 2, d // 2] = block
            p1_send[o, d % 2, d // 2] = block.astype(BF16)

    p1_copies, p2_copies = {}, {}

    def start_p1(o, value):
        store_terms(o, value)
        p1_copies[o] = p1_copy(o)
        p1_copies[o].start()

    def start_p2(o):
        p1_copies[o].wait_recv()
        for k in range(chips - 1, 0, -1):
            q = flipped(chip, k)
            p2_send[o, q] = (acc[o, core, q] + p1_buf[o, q].astype(F32)).astype(BF16)
            copy = pltpu.make_async_remote_copy(
                src_ref=p2_send.at[o, q],
                dst_ref=p2_buf.at[o, k - 1],
                send_sem=p2_ssem.at[o, k - 1],
                recv_sem=p2_rsem.at[o, k - 1],
                device_id=chip_at(k),
                device_id_type=MESH,
            )
            copy.start()
            p2_copies[o, k] = copy

    for k in range(1, n_exp):
        a_copies[k].wait_recv()
    scaled = a_buf[...].reshape(rows, width)
    if gather:
        for k in range(n_dp - 1, 0, -1):
            peer = flipped(replica, k)
            columns = pl.ds(pl.multiple_of(peer * row_block, row_block), row_block)
            copy = pltpu.make_async_remote_copy(
                src_ref=a_buf.at[:, :, columns],
                dst_ref=s_all.at[replica],
                send_sem=s_ssem.at[k - 1],
                recv_sem=s_rsem.at[k - 1],
                device_id={"dp": peer},
                device_id_type=MESH,
            )
            copy.start()
            s_copies.append(copy)
    else:
        start_p1(0, dot(scaled, hidden, 0, 0))
    dhidden = dot(scaled, wd_v[...], 1, 1)
    d_gate = (dhidden * slope).astype(BF16)
    d_up = (dhidden * activated).astype(BF16)
    returning = (dot(d_gate, wg_v[...], 1, 1) + dot(d_up, wu_v[...], 1, 1)).astype(BF16)
    for h in range(n_exp):
        r_send[h] = returning[h * part : (h + 1) * part]
    r_copies = []
    for k in range(n_exp - 1, 0, -1):
        copy = pltpu.make_async_remote_copy(
            src_ref=r_send.at[member_at(k)],
            dst_ref=r_buf.at[member],
            send_sem=r_ssem.at[k - 1],
            recv_sem=r_rsem.at[k - 1],
            device_id={"expert": member_at(k)},
            device_id_type=MESH,
        )
        copy.start()
        r_copies.append(copy)
    start_p1(1, dot(inputs, d_gate, 0, 0))
    start_p1(2, dot(inputs, d_up, 0, 0))
    if not gather:
        start_p2(0)
    r_buf[member] = r_send[member]
    start_p2(1)
    start_p2(2)

    if gather:
        own = pl.ds(pl.multiple_of(replica * row_block, row_block), row_block)
        s_all[replica] = a_buf[:, :, own]
        for copy in h_copies + s_copies:
            copy.wait_recv()
        slots = n_dp * rows
        down = dot(
            s_all[...].reshape(slots, row_block), h_all[...].reshape(slots, wg_v.shape[1]), 0, 0
        )
        gd_ref[...] = down * (1.0 / (micro * n_dp))
    for copy in r_copies:
        copy.wait_recv()
    gin_ref[...] = dot(mixing, r_buf[...].reshape(rows, width), 0, 0).astype(BF16)

    factor = 1.0 / (micro * n_dp)
    for o, out in enumerate((gd_ref, gg_ref, gu_ref)):
        if o not in p1_copies:
            continue
        total = acc[o, core, chip] + p1_buf[o, chip].astype(F32)
        for k in range(chips - 1, 0, -1):
            p2_copies[o, k].wait_recv()
            total = total + p2_buf[o, k - 1].astype(F32)
        out[...] = total * factor
    started = [*a_copies.values(), *p1_copies.values(), *p2_copies.values()]
    for copy in started + r_copies + h_copies + s_copies:
        copy.wait_send()


def pooled_kernel(
    micro,
    n_exp,
    n_dp,
    routes_hbm,
    probs_hbm,
    go_hbm,
    x_hbm,
    wg_hbm,
    wu_hbm,
    wd_hbm,
    gin_ref,
    gg_ref,
    gu_ref,
    gd_ref,
    routes_v,
    probs_v,
    go_v,
    x_v,
    x_par,
    xt_v,
    wg_v,
    wu_v,
    wd_v,
    a_send,
    a_buf,
    r_send,
    r_buf,
    mix_v,
    d_all,
    relay_send,
    relay_buf,
    last_send,
    last_buf,
    s_all,
    h_all,
    down_v,
    down_buf,
    load_sem,
    a_ssem,
    a_rsem,
    r_ssem,
    r_rsem,
    x_sem,
    d_sem,
    relay_ssem,
    relay_rsem,
    last_ssem,
    last_rsem,
    s_ssem,
    s_rsem,
    h_ssem,
    h_rsem,
    down_sem,
):
    member = lax.axis_index("expert")
    replica = lax.axis_index("dp")
    core = lax.rem(replica, 2)
    chip = lax.div(replica, 2)
    chips = n_dp // 2
    partner = {"dp": chip * 2 + 1 - core}
    window = n_exp // 2
    tokens, width = go_v.shape
    cols = wg_v.shape[1]
    tok_dev = tokens // micro
    part = micro * CAPS
    rows = n_exp * part
    row_block = width // n_dp
    pair_block = 2 * row_block
    hops = range(chips - 1, 0, -1)

    loads = [
        pltpu.make_async_copy(src, dst, load_sem.at[i])
        for i, (src, dst) in enumerate(
            (
                (routes_hbm, routes_v),
                (probs_hbm, probs_v),
                (go_hbm, go_v),
                *((x_hbm.at[m], x_v.at[:, pl.ds(m * CAPS, CAPS), :]) for m in range(micro)),
                (wg_hbm, wg_v),
                (wu_hbm, wu_v),
                (wd_hbm, wd_v),
            )
        )
    ]
    for load in loads:
        load.start()

    def chip_at(k):
        return flipped(chip, k)

    def peer_at(k):
        return {"dp": chip_at(k) * 2 + core}

    barrier = pltpu.get_barrier_semaphore()
    for k in range(1, n_exp):
        pl.semaphore_signal(
            barrier, inc=1, device_id={"expert": flipped(member, k)}, device_id_type=MESH
        )
    for k in hops:
        pl.semaphore_signal(barrier, inc=1, device_id=peer_at(k), device_id_type=MESH)
    pl.semaphore_signal(barrier, inc=1, device_id=partner, device_id_type=MESH)

    started = []

    def remote(src, dst, send_sem, recv_sem, device):
        copy = pltpu.make_async_remote_copy(
            src_ref=src,
            dst_ref=dst,
            send_sem=send_sem,
            recv_sem=recv_sem,
            device_id=device,
            device_id_type=MESH,
        )
        copy.start()
        started.append(copy)
        return copy

    pad = max(window, 8)
    expert_row = lax.broadcasted_iota(jnp.int32, (pad, tokens), 0)
    ti = lax.broadcasted_iota(jnp.int32, (tokens, tokens), 0)
    tj = lax.broadcasted_iota(jnp.int32, (tokens, tokens), 1)
    earlier = jnp.where((ti < tj) & (lax.div(ti, tok_dev) == lax.div(tj, tok_dev)), 1.0, 0.0)
    loads[0].wait()
    loads[1].wait()
    ids = jnp.concatenate([routes_v[m] for m in range(micro)], axis=1)
    probs = jnp.concatenate([probs_v[m].astype(F32) for m in range(micro)], axis=1)
    hits, weights = [], []
    table = jnp.zeros((pad, tokens), F32)
    for e in range(window):
        named = ids == e
        hits.append(jnp.sum(jnp.where(named, 1.0, 0.0), axis=0, keepdims=True))
        weights.append(jnp.sum(jnp.where(named, probs, 0.0), axis=0, keepdims=True))
        table = jnp.where(expert_row == e, hits[e], table)
    ranking = dot(table.astype(BF16), earlier.astype(BF16), 1, 0)
    slot = lax.broadcasted_iota(jnp.int32, (CAPS, tokens), 0).astype(F32)
    batch = lax.div(lax.broadcasted_iota(jnp.int32, (CAPS, tokens), 1), tok_dev)
    ones, scales = [], []
    for e in range(window):
        chosen = (hits[e] > 0.5) & (ranking[e : e + 1] == slot)
        for m in range(micro):
            here = chosen & (batch == m)
            ones.append(jnp.where(here, 1.0, 0.0))
            scales.append(jnp.where(here, weights[e], 0.0))
    picking = jnp.concatenate(scales, axis=0).astype(BF16)

    loads[2].wait()
    sending = dot(picking, go_v[...], 1, 0).astype(BF16)
    for e in range(window):
        a_send[e] = sending[e * part : (e + 1) * part]
    pl.semaphore_wait(barrier, n_exp - 1 + chips)

    inner = jnp.where((member == 0) | (member == n_exp - 1), 0, 1)
    order = [
        flipped(member, 1) * (1 - inner) + flipped(member, 2) * inner,
        flipped(member, 3),
        flipped(member, 2) * (1 - inner) + flipped(member, 1) * inner,
    ]
    nearest = [flipped(member, 1), flipped(member, 3) * inner + flipped(member, 2) * (1 - inner), flipped(member, 2) * inner + flipped(member, 3) * (1 - inner)]
    for j, to in enumerate(order):
        remote(
            a_send.at[lax.div(to, 2)],
            a_buf.at[member],
            a_ssem.at[j],
            a_rsem.at[member],
            {"expert": to},
        )
    a_buf[member] = a_send[lax.div(member, 2)]

    def a_arrival(source):
        return pltpu.make_async_remote_copy(
            src_ref=a_send.at[0],
            dst_ref=a_buf.at[source],
            send_sem=a_ssem.at[0],
            recv_sem=a_rsem.at[source],
            device_id={"expert": source},
            device_id_type=MESH,
        )

    for m in range(micro):
        loads[3 + m].wait()
    x_copy = remote(x_v, x_par, x_sem.at[0], x_sem.at[1], partner)

    inputs = x_v[...].reshape(rows, width)
    loads[3 + micro].wait()
    gate = dot(inputs, wg_v[...], 1, 0)
    loads[4 + micro].wait()
    up = dot(inputs, wu_v[...], 1, 0)
    sigmoid = jax.nn.sigmoid(gate)
    activated = gate * sigmoid
    h_all[chip] = (activated * up).astype(BF16)
    h_copies = {
        k: remote(
            h_all.at[chip], h_all.at[chip], h_ssem.at[k - 1], h_rsem.at[k - 1], peer_at(k)
        )
        for k in hops
    }
    slope = up * sigmoid * (1.0 + gate * (1.0 - sigmoid))

    def blocks(q):
        return pl.ds(pl.multiple_of(q * pair_block, pair_block), pair_block)

    def send_slices(source, j):
        for k in hops:
            remote(
                a_buf.at[source, :, blocks(chip_at(k))],
                s_all.at[chip, source],
                s_ssem.at[j, k - 1],
                s_rsem.at[k - 1],
                peer_at(k),
            )

    send_slices(member, 0)

    mix_v[...] = jnp.concatenate(
        [jnp.concatenate(ones[e * micro : (e + 1) * micro], axis=0) for e in range(window) for _ in range(2)],
        axis=0,
    ).astype(BF16)
    loads[5 + micro].wait()
    x_copy.wait_recv()
    for k in range(chips):
        q = chip_at(k) if k else chip
        own = pl.ds(pl.multiple_of((q * 2 + core) * row_block, row_block), row_block)
        mine = x_v[:, :, own].reshape(rows, row_block)
        other = x_par[:, :, own].reshape(rows, row_block)
        xt_v[k] = jnp.concatenate([mine, other], axis=0).T

    for j, source in enumerate(nearest):
        a_arrival(source).wait_recv()
        if j < n_exp - 2:
            send_slices(source, j + 1)
    scaled = a_buf[...].reshape(rows, width)
    dhidden = dot(scaled, wd_v[...], 1, 1)
    d_gate = (dhidden * slope).astype(BF16)
    d_up = (dhidden * activated).astype(BF16)
    d_all[0, :, :cols] = d_gate
    d_all[0, :, cols:] = d_up
    d_copy = remote(d_all.at[0], d_all.at[1], d_sem.at[0], d_sem.at[1], partner)
    send_slices(nearest[-1], n_exp - 1)

    pieces = 1
    piece = width // pieces

    def span(c):
        return pl.ds(c * piece, piece)

    r_copies = [
        [
            pltpu.make_async_remote_copy(
                src_ref=r_send.at[to, :, span(c)],
                dst_ref=r_buf.at[member, :, span(c)],
                send_sem=r_ssem.at[c, j],
                recv_sem=r_rsem.at[c, member],
                device_id={"expert": to},
                device_id_type=MESH,
            )
            for j, to in enumerate(order)
        ]
        for c in range(pieces)
    ]
    started.extend(copy for copies in r_copies for copy in copies)

    def send_back():
        for c in range(pieces):
            returning = dot(d_all[0, :, :cols], wg_v[span(c), :], 1, 1) + dot(
                d_all[0, :, cols:], wu_v[span(c), :], 1, 1
            )
            returning = returning.astype(BF16)
            for h in range(n_exp):
                r_send[h, :, span(c)] = returning[h * part : (h + 1) * part]
            for copy in r_copies[c]:
                copy.start()

    returns_first = core == 1

    @pl.when(returns_first)
    def _():
        send_back()

    d_copy.wait_recv()
    factors = d_all[...].reshape(2 * rows, 2 * cols)
    far = dot(xt_v[3], factors, 1, 0).astype(BF16)
    relays = []
    for i, k in enumerate((1, 2)):
        relay_send[i] = far[:, i * cols : (i + 1) * cols]
        relays.append(
            remote(
                relay_send.at[i],
                relay_buf.at[i],
                relay_ssem.at[i],
                relay_rsem.at[i],
                peer_at(k),
            )
        )

    def send_last(i, k, value):
        last_send[i] = value.astype(BF16)
        return remote(
            last_send.at[i], last_buf.at[i], last_ssem.at[i], last_rsem.at[i], peer_at(k)
        )

    near = [dot(xt_v[k], factors, 1, 0) for k in (1, 2)]
    last_copies = [
        send_last(0, 1, near[0][:, :cols]),
        send_last(1, 2, near[1][:, cols:]),
    ]
    total = dot(xt_v[0], factors, 1, 0)
    @pl.when(jnp.logical_not(returns_first))
    def _():
        send_back()

    r_buf[member] = r_send[member]
    s_all[chip] = a_buf[:, :, blocks(chip)]
    relays[0].wait_recv()
    last_copies.append(send_last(2, 2, near[1][:, :cols] + relay_buf[0].astype(F32)))
    relays[1].wait_recv()
    last_copies.append(send_last(3, 1, near[0][:, cols:] + relay_buf[1].astype(F32)))
    for k in hops:
        h_copies[k].wait_recv()
        pltpu.make_async_remote_copy(
            src_ref=s_all.at[chip],
            dst_ref=s_all.at[chip_at(k)],
            send_sem=s_ssem.at[0, k - 1],
            recv_sem=s_rsem.at[k - 1],
            device_id=peer_at(k),
            device_id_type=MESH,
        ).wait_recv()
    slots = chips * rows
    down = dot(s_all[...].reshape(slots, pair_block), h_all[...].reshape(slots, cols), 0, 0)
    down_v[0] = down[:row_block]
    down_v[1] = down[row_block:]
    down_copy = remote(down_v.at[1 - core], down_buf, down_sem.at[0], down_sem.at[1], partner)

    for c in range(pieces):
        for source in order:
            pltpu.make_async_remote_copy(
                src_ref=r_send.at[source, :, span(c)],
                dst_ref=r_buf.at[source, :, span(c)],
                send_sem=r_ssem.at[c, 0],
                recv_sem=r_rsem.at[c, source],
                device_id={"expert": source},
                device_id_type=MESH,
            ).wait_recv()
        gin_ref[:, span(c)] = dot(
            mix_v[...], r_buf[:, :, span(c)].reshape(rows, piece), 0, 0
        ).astype(BF16)

    factor = 1.0 / (micro * n_dp)
    down_copy.wait_recv()
    gd_ref[...] = (down_v[core] + down_buf[...]) * factor
    for copy in last_copies:
        copy.wait_recv()
    gates = total[:, :cols] + last_buf[0].astype(F32) + last_buf[2].astype(F32)
    ups = total[:, cols:] + last_buf[1].astype(F32) + last_buf[3].astype(F32)
    gg_ref[...] = gates * factor
    gu_ref[...] = ups * factor
    for copy in started:
        copy.wait_send()


def settle(*refs):
    count = len(refs) // 2
    sem = refs[-1]
    copies = [
        pltpu.make_async_copy(refs[i], refs[count + i], sem.at[i]) for i in range(count)
    ]
    for copy in copies:
        copy.start()
    for copy in copies:
        copy.wait()


def settled(arrays):
    anywhere = pl.BlockSpec(memory_space=pl.ANY)
    return pl.pallas_call(
        settle,
        out_shape=tuple(jax.ShapeDtypeStruct(a.shape, a.dtype) for a in arrays),
        in_specs=[pl.BlockSpec(memory_space=pltpu.VMEM)] * len(arrays),
        out_specs=(anywhere,) * len(arrays),
        scratch_shapes=[pltpu.SemaphoreType.DMA((len(arrays),))],
    )(*[pltpu.with_memory_space_constraint(a, pltpu.VMEM) for a in arrays])


def pooled_call(n_exp, n_dp, grad_out, routes, route_probs, dispatched, w_gate, w_up, w_down):
    micro, tok_dev, width = grad_out.shape
    cols = w_gate.shape[1]
    tokens = micro * tok_dev
    part = micro * CAPS
    rows = n_exp * part
    chips = n_dp // 2
    row_block = width // n_dp
    vmem = pl.BlockSpec(memory_space=pltpu.VMEM)
    hbm = pl.BlockSpec(memory_space=pl.ANY)
    grad = pltpu.VMEM((row_block, cols), F32)
    dma = pltpu.SemaphoreType.DMA
    return pl.pallas_call(
        functools.partial(pooled_kernel, micro, n_exp, n_dp),
        out_shape=(pltpu.VMEM((tokens, width), BF16), grad, grad, grad),
        in_specs=[hbm] * 7,
        out_specs=(vmem, vmem, vmem, vmem),
        scratch_shapes=[
            pltpu.VMEM((micro, routes.shape[2], tok_dev), jnp.int32),
            pltpu.VMEM((micro, routes.shape[2], tok_dev), BF16),
            pltpu.VMEM((tokens, width), BF16),
            pltpu.VMEM((n_exp, part, width), BF16),
            pltpu.VMEM((n_exp, part, width), BF16),
            pltpu.VMEM((chips, row_block, 2 * rows), BF16),
            pltpu.VMEM((width, cols), BF16),
            pltpu.VMEM((width, cols), BF16),
            pltpu.VMEM((cols, width), BF16),
            pltpu.VMEM((n_exp // 2, part, width), BF16),
            pltpu.VMEM((n_exp, part, width), BF16),
            pltpu.VMEM((n_exp, part, width), BF16),
            pltpu.VMEM((n_exp, part, width), BF16),
            pltpu.VMEM((rows, tokens), BF16),
            pltpu.VMEM((2, rows, 2 * cols), BF16),
            pltpu.VMEM((2, row_block, cols), BF16),
            pltpu.VMEM((2, row_block, cols), BF16),
            pltpu.VMEM((4, row_block, cols), BF16),
            pltpu.VMEM((4, row_block, cols), BF16),
            pltpu.VMEM((chips, n_exp, part, 2 * row_block), BF16),
            pltpu.VMEM((chips, rows, cols), BF16),
            pltpu.VMEM((2, row_block, cols), F32),
            pltpu.VMEM((row_block, cols), F32),
            dma((6 + micro,)),
            dma((n_exp - 1,)),
            dma((n_exp,)),
            dma((1, n_exp - 1)),
            dma((1, n_exp)),
            dma((2,)),
            dma((2,)),
            dma((2,)),
            dma((2,)),
            dma((4,)),
            dma((4,)),
            dma((n_exp, chips - 1)),
            dma((chips - 1,)),
            dma((chips - 1,)),
            dma((chips - 1,)),
            dma((2,)),
        ],
        compiler_params=pltpu.CompilerParams(collective_id=0, has_side_effects=True),
    )(
        routes.transpose(0, 2, 1),
        route_probs.transpose(0, 2, 1),
        grad_out.reshape(tokens, width),
        dispatched.reshape(micro, n_exp, CAPS, width),
        w_gate,
        w_up,
        w_down,
    )


def spread_call(n_exp, n_dp, grad_out, routes, route_probs, dispatched, w_gate, w_up, w_down):
    micro, tok_dev, width = grad_out.shape
    cols = w_gate.shape[1]
    tokens = micro * tok_dev
    part = micro * CAPS
    rows = n_exp * part
    chips = n_dp // 2
    row_block = width // n_dp
    vmem = pl.BlockSpec(memory_space=pltpu.VMEM)
    hbm = pl.BlockSpec(memory_space=pl.ANY)
    grad = pltpu.VMEM((row_block, cols), F32)
    dma = pltpu.SemaphoreType.DMA
    others = max(chips - 1, 1)
    gather = row_block % 128 == 0
    return pl.pallas_call(
        functools.partial(kernel, micro, n_exp, n_dp),
        out_shape=(pltpu.VMEM((tokens, width), BF16), grad, grad, grad),
        in_specs=[vmem, vmem, hbm, hbm, hbm, hbm, hbm],
        out_specs=(vmem, vmem, vmem, vmem),
        scratch_shapes=[
            pltpu.VMEM((tokens, width), BF16),
            pltpu.VMEM((rows, width), BF16),
            pltpu.VMEM((width, cols), BF16),
            pltpu.VMEM((width, cols), BF16),
            pltpu.VMEM((cols, width), BF16),
            pltpu.VMEM((n_exp, part, width), BF16),
            pltpu.VMEM((n_exp, part, width), BF16),
            pltpu.VMEM((n_exp, part, width), BF16),
            pltpu.VMEM((n_exp, part, width), BF16),
            pltpu.VMEM((3, 2, chips, row_block, cols), F32),
            pltpu.VMEM((3, 2, chips, row_block, cols), BF16),
            pltpu.VMEM((3, chips, row_block, cols), BF16),
            pltpu.VMEM((3, chips, row_block, cols), BF16),
            pltpu.VMEM((3, others, row_block, cols), BF16),
            pltpu.VMEM((n_dp, n_exp, part, row_block) if gather else (8, 128), BF16),
            pltpu.VMEM((n_dp, rows, cols) if gather else (8, 128), BF16),
            dma((5,)),
            dma((n_exp - 1,)),
            dma((n_exp - 1,)),
            dma((n_exp - 1,)),
            dma((n_exp - 1,)),
            dma((3,)),
            dma((3,)),
            dma((3, others)),
            dma((3, others)),
            dma((n_dp - 1,)),
            dma((n_dp - 1,)),
            dma((n_dp - 1,)),
            dma((n_dp - 1,)),
        ],
        compiler_params=pltpu.CompilerParams(collective_id=0, has_side_effects=True),
    )(
        routes.transpose(0, 2, 1),
        route_probs.transpose(0, 2, 1),
        grad_out.reshape(tokens, width),
        dispatched.reshape(rows, width),
        w_gate,
        w_up,
        w_down,
    )


def per_device(n_exp, n_dp, grad_out, *rest):
    pooled = n_exp == 4 and n_dp == 8 and (grad_out.shape[2] // n_dp) % 128 == 0
    call = pooled_call if pooled else spread_call
    out = settled(call(n_exp, n_dp, grad_out, *rest))
    return (out[0].reshape(grad_out.shape),) + tuple(out[1:])


def solution(mesh):
    return jax.shard_map(
        functools.partial(per_device, mesh.shape["expert"], mesh.shape["dp"]),
        mesh=mesh,
        in_specs=(
            P(None, ("dp", "expert"), None),
            P(None, ("dp", "expert"), None),
            P(None, ("dp", "expert"), None),
            P(None, ("dp", "expert"), None),
            P(None, "expert"),
            P(None, "expert"),
            P("expert", None),
        ),
        out_specs=(
            P(None, ("dp", "expert"), None),
            P("dp", "expert"),
            P("dp", "expert"),
            P("dp", "expert"),
        ),
        check_vma=False,
    )
```

```python
import functools

import jax
import jax.numpy as jnp
from jax import lax
from jax.experimental import pallas as pl
from jax.experimental.pallas import tpu as pltpu
from jax.sharding import PartitionSpec as P

CAPS = 8
MESH = pl.DeviceIdType.MESH
BF16 = jnp.bfloat16
F32 = jnp.float32


def dot(left, right, lc, rc):
    return lax.dot_general(
        left, right, (((lc,), (rc,)), ((), ())), preferred_element_type=F32
    )


def flipped(index, bits):
    step = 1
    while step <= bits:
        if bits & step:
            index = index + step - 2 * step * lax.rem(lax.div(index, step), 2)
        step *= 2
    return index


def kernel(
    micro,
    n_exp,
    n_dp,
    routes_ref,
    probs_ref,
    go_hbm,
    x_hbm,
    wg_hbm,
    wu_hbm,
    wd_hbm,
    gin_ref,
    gg_ref,
    gu_ref,
    gd_ref,
    go_v,
    x_v,
    wg_v,
    wu_v,
    wd_v,
    a_send,
    a_buf,
    r_send,
    r_buf,
    acc,
    p1_send,
    p1_buf,
    p2_send,
    p2_buf,
    s_all,
    h_all,
    load_sem,
    a_ssem,
    a_rsem,
    r_ssem,
    r_rsem,
    p1_ssem,
    p1_rsem,
    p2_ssem,
    p2_rsem,
    s_ssem,
    s_rsem,
    h_ssem,
    h_rsem,
):
    member = lax.axis_index("expert")
    replica = lax.axis_index("dp")
    core = lax.rem(replica, 2)
    chip = lax.div(replica, 2)
    chips = n_dp // 2
    partner = {"dp": chip * 2 + 1 - core}
    window = n_exp // 2
    tokens = go_v.shape[0]
    width = go_v.shape[1]
    tok_dev = tokens // micro
    part = micro * CAPS
    rows = n_exp * part
    row_block = width // n_dp
    gather = row_block % 128 == 0

    def member_at(k):
        return flipped(member, k)

    def chip_at(k):
        return {"dp": flipped(chip, k) * 2 + core}

    loads = [
        pltpu.make_async_copy(src, dst, load_sem.at[i])
        for i, (src, dst) in enumerate(
            ((go_hbm, go_v), (x_hbm, x_v), (wg_hbm, wg_v), (wu_hbm, wu_v), (wd_hbm, wd_v))
        )
    ]
    for load in loads:
        load.start()

    barrier = pltpu.get_barrier_semaphore()
    for k in range(1, n_exp):
        pl.semaphore_signal(
            barrier, inc=1, device_id={"expert": member_at(k)}, device_id_type=MESH
        )
    for k in range(1, n_dp):
        pl.semaphore_signal(
            barrier, inc=1, device_id={"dp": flipped(replica, k)}, device_id_type=MESH
        )

    ids = jnp.concatenate([routes_ref[m] for m in range(micro)], axis=1)
    probs = jnp.concatenate([probs_ref[m].astype(F32) for m in range(micro)], axis=1)
    pad = max(window, 8)
    expert_row = lax.broadcasted_iota(jnp.int32, (pad, tokens), 0)
    hits, weights = [], []
    table = jnp.zeros((pad, tokens), F32)
    for e in range(window):
        named = ids == e
        hits.append(jnp.sum(jnp.where(named, 1.0, 0.0), axis=0, keepdims=True))
        weights.append(jnp.sum(jnp.where(named, probs, 0.0), axis=0, keepdims=True))
        table = jnp.where(expert_row == e, hits[e], table)
    ti = lax.broadcasted_iota(jnp.int32, (tokens, tokens), 0)
    tj = lax.broadcasted_iota(jnp.int32, (tokens, tokens), 1)
    earlier = jnp.where((ti < tj) & (lax.div(ti, tok_dev) == lax.div(tj, tok_dev)), 1.0, 0.0)
    ranking = dot(table.astype(BF16), earlier.astype(BF16), 1, 0)
    slot = lax.broadcasted_iota(jnp.int32, (CAPS, tokens), 0).astype(F32)
    batch = lax.div(lax.broadcasted_iota(jnp.int32, (CAPS, tokens), 1), tok_dev)
    ones, scales = [], []
    for h in range(n_exp):
        e = h // 2
        chosen = (hits[e] > 0.5) & (ranking[e : e + 1] == slot)
        for m in range(micro):
            here = chosen & (batch == m)
            ones.append(jnp.where(here, 1.0, 0.0))
            scales.append(jnp.where(here, weights[e], 0.0))
    mixing = jnp.concatenate(ones, axis=0).astype(BF16)
    picking = jnp.concatenate(scales, axis=0).astype(BF16)

    loads[0].wait()
    sending = dot(picking, go_v[...], 1, 0).astype(BF16)
    for h in range(n_exp):
        a_send[h] = sending[h * part : (h + 1) * part]
    pl.semaphore_wait(barrier, n_exp - 1 + n_dp - 1)
    def a_copy(k, src, slot, to):
        return pltpu.make_async_remote_copy(
            src_ref=src,
            dst_ref=a_buf.at[slot],
            send_sem=a_ssem.at[k - 1],
            recv_sem=a_rsem.at[k - 1],
            device_id={"expert": to},
            device_id_type=MESH,
        )

    a_copies = {}
    for k in range(1, n_exp):
        a_copies[k] = a_copy(k, a_send.at[member_at(k)], member, member_at(k))
        a_copies[k].start()
    a_buf[member] = a_send[member]

    loads[1].wait()
    ri = lax.broadcasted_iota(jnp.int32, (rows, rows), 0)
    rj = lax.broadcasted_iota(jnp.int32, (rows, rows), 1)
    wanted = (
        lax.rem(lax.div(ri, CAPS), micro) * (n_exp * CAPS)
        + lax.div(ri, part) * CAPS
        + lax.rem(ri, CAPS)
    )
    inputs = dot(jnp.where(rj == wanted, 1.0, 0.0).astype(BF16), x_v[...], 1, 0).astype(BF16)
    loads[2].wait()
    gate = dot(inputs, wg_v[...], 1, 0)
    loads[3].wait()
    up = dot(inputs, wu_v[...], 1, 0)
    sigmoid = jax.nn.sigmoid(gate)
    activated = gate * sigmoid
    hidden = (activated * up).astype(BF16)
    h_copies, s_copies = [], []
    if gather:
        h_all[replica] = hidden
        for k in range(n_dp - 1, 0, -1):
            copy = pltpu.make_async_remote_copy(
                src_ref=h_all.at[replica],
                dst_ref=h_all.at[replica],
                send_sem=h_ssem.at[k - 1],
                recv_sem=h_rsem.at[k - 1],
                device_id={"dp": flipped(replica, k)},
                device_id_type=MESH,
            )
            copy.start()
            h_copies.append(copy)
    slope = up * sigmoid * (1.0 + gate * (1.0 - sigmoid))
    loads[4].wait()

    def p1_copy(o):
        return pltpu.make_async_remote_copy(
            src_ref=p1_send.at[o, 1 - core],
            dst_ref=p1_buf.at[o],
            send_sem=p1_ssem.at[o],
            recv_sem=p1_rsem.at[o],
            device_id=partner,
            device_id_type=MESH,
        )

    def store_terms(o, value):
        for d in range(n_dp):
            block = value[d * row_block : (d + 1) * row_block]
            acc[o, d % 2, d // 2] = block
            p1_send[o, d % 2, d // 2] = block.astype(BF16)

    p1_copies, p2_copies = {}, {}

    def start_p1(o, value):
        store_terms(o, value)
        p1_copies[o] = p1_copy(o)
        p1_copies[o].start()

    def start_p2(o):
        p1_copies[o].wait_recv()
        for k in range(chips - 1, 0, -1):
            q = flipped(chip, k)
            p2_send[o, q] = (acc[o, core, q] + p1_buf[o, q].astype(F32)).astype(BF16)
            copy = pltpu.make_async_remote_copy(
                src_ref=p2_send.at[o, q],
                dst_ref=p2_buf.at[o, k - 1],
                send_sem=p2_ssem.at[o, k - 1],
                recv_sem=p2_rsem.at[o, k - 1],
                device_id=chip_at(k),
                device_id_type=MESH,
            )
            copy.start()
            p2_copies[o, k] = copy

    for k in range(1, n_exp):
        a_copies[k].wait_recv()
    scaled = a_buf[...].reshape(rows, width)
    if gather:
        for k in range(n_dp - 1, 0, -1):
            peer = flipped(replica, k)
            columns = pl.ds(pl.multiple_of(peer * row_block, row_block), row_block)
            copy = pltpu.make_async_remote_copy(
                src_ref=a_buf.at[:, :, columns],
                dst_ref=s_all.at[replica],
                send_sem=s_ssem.at[k - 1],
                recv_sem=s_rsem.at[k - 1],
                device_id={"dp": peer},
                device_id_type=MESH,
            )
            copy.start()
            s_copies.append(copy)
    else:
        start_p1(0, dot(scaled, hidden, 0, 0))
    dhidden = dot(scaled, wd_v[...], 1, 1)
    d_gate = (dhidden * slope).astype(BF16)
    d_up = (dhidden * activated).astype(BF16)
    returning = (dot(d_gate, wg_v[...], 1, 1) + dot(d_up, wu_v[...], 1, 1)).astype(BF16)
    for h in range(n_exp):
        r_send[h] = returning[h * part : (h + 1) * part]
    r_copies = []
    for k in range(n_exp - 1, 0, -1):
        copy = pltpu.make_async_remote_copy(
            src_ref=r_send.at[member_at(k)],
            dst_ref=r_buf.at[member],
            send_sem=r_ssem.at[k - 1],
            recv_sem=r_rsem.at[k - 1],
            device_id={"expert": member_at(k)},
            device_id_type=MESH,
        )
        copy.start()
        r_copies.append(copy)
    start_p1(1, dot(inputs, d_gate, 0, 0))
    start_p1(2, dot(inputs, d_up, 0, 0))
    if not gather:
        start_p2(0)
    r_buf[member] = r_send[member]
    start_p2(1)
    start_p2(2)

    if gather:
        own = pl.ds(pl.multiple_of(replica * row_block, row_block), row_block)
        s_all[replica] = a_buf[:, :, own]
        for copy in h_copies + s_copies:
            copy.wait_recv()
        slots = n_dp * rows
        down = dot(
            s_all[...].reshape(slots, row_block), h_all[...].reshape(slots, wg_v.shape[1]), 0, 0
        )
        gd_ref[...] = down * (1.0 / (micro * n_dp))
    for copy in r_copies:
        copy.wait_recv()
    gin_ref[...] = dot(mixing, r_buf[...].reshape(rows, width), 0, 0).astype(BF16)

    factor = 1.0 / (micro * n_dp)
    for o, out in enumerate((gd_ref, gg_ref, gu_ref)):
        if o not in p1_copies:
            continue
        total = acc[o, core, chip] + p1_buf[o, chip].astype(F32)
        for k in range(chips - 1, 0, -1):
            p2_copies[o, k].wait_recv()
            total = total + p2_buf[o, k - 1].astype(F32)
        out[...] = total * factor
    started = [*a_copies.values(), *p1_copies.values(), *p2_copies.values()]
    for copy in started + r_copies + h_copies + s_copies:
        copy.wait_send()


def pooled_kernel(
    micro,
    n_exp,
    n_dp,
    routes_hbm,
    probs_hbm,
    go_hbm,
    x_hbm,
    wg_hbm,
    wu_hbm,
    wd_hbm,
    gin_ref,
    gg_ref,
    gu_ref,
    gd_ref,
    routes_v,
    probs_v,
    go_v,
    x_v,
    x_par,
    xt_v,
    wg_v,
    wu_v,
    wd_v,
    a_send,
    a_buf,
    r_send,
    r_buf,
    mix_v,
    d_all,
    relay_buf,
    last_send,
    last_buf,
    s_all,
    h_all,
    down_v,
    down_buf,
    sized,
    load_sem,
    sent_sem,
    a_sem,
    r_sem,
    x_sem,
    d_sem,
    relay_sem,
    last_sem,
    slot_sem,
    down_sem,
):
    member = lax.axis_index("expert")
    replica = lax.axis_index("dp")
    core = lax.rem(replica, 2)
    chip = lax.div(replica, 2)
    chips = n_dp // 2
    partner = {"dp": chip * 2 + 1 - core}
    window = n_exp // 2
    tokens, width = go_v.shape
    cols = wg_v.shape[1]
    tok_dev = tokens // micro
    part = micro * CAPS
    rows = n_exp * part
    row_block = width // n_dp
    pair_block = 2 * row_block
    hops = range(chips - 1, 0, -1)

    def chip_at(k):
        return flipped(chip, k)

    def peer_at(k):
        return {"dp": chip_at(k) * 2 + core}

    barrier = pltpu.get_barrier_semaphore()
    for k in range(n_exp - 1, 0, -1):
        pl.semaphore_signal(
            barrier, inc=1, device_id={"expert": flipped(member, k)}, device_id_type=MESH
        )
    for k in hops:
        pl.semaphore_signal(barrier, inc=1, device_id=peer_at(k), device_id_type=MESH)
    pl.semaphore_signal(barrier, inc=1, device_id=partner, device_id_type=MESH)

    loads = [
        pltpu.make_async_copy(src, dst, load_sem.at[min(i, 3)])
        for i, (src, dst) in enumerate(
            (
                (routes_hbm, routes_v),
                (probs_hbm, probs_v),
                (go_hbm, go_v),
                *((x_hbm.at[m], x_v.at[:, pl.ds(m * CAPS, CAPS), :]) for m in range(micro)),
                (wg_hbm, wg_v),
                (wu_hbm, wu_v),
                (wd_hbm, wd_v),
            )
        )
    ]
    for load in loads:
        load.start()

    def arrivals(size, sem):
        return pltpu.make_async_copy(sized.at[pl.ds(0, size)], sized.at[pl.ds(0, size)], sem)

    sent = []

    def remote(src, dst, sem, device, start=True):
        copy = pltpu.make_async_remote_copy(
            src_ref=src,
            dst_ref=dst,
            send_sem=sent_sem.at[0],
            recv_sem=sem,
            device_id=device,
            device_id_type=MESH,
        )
        if start:
            copy.start()
            bulk = 1
            for n in src.shape:
                bulk *= n
            sent.append(bulk * (2 if src.dtype == F32 else 1))
        return copy

    pad = max(window, 8)
    expert_row = lax.broadcasted_iota(jnp.int32, (pad, tokens), 0)
    ti = lax.broadcasted_iota(jnp.int32, (tokens, tokens), 0)
    tj = lax.broadcasted_iota(jnp.int32, (tokens, tokens), 1)
    earlier = jnp.where((ti < tj) & (lax.div(ti, tok_dev) == lax.div(tj, tok_dev)), 1.0, 0.0)
    loads[0].wait()
    loads[1].wait()
    ids = jnp.concatenate([routes_v[m] for m in range(micro)], axis=1)
    probs = jnp.concatenate([probs_v[m].astype(F32) for m in range(micro)], axis=1)
    hits, weights = [], []
    table = jnp.zeros((pad, tokens), F32)
    for e in range(window):
        named = ids == e
        hits.append(jnp.sum(jnp.where(named, 1.0, 0.0), axis=0, keepdims=True))
        weights.append(jnp.sum(jnp.where(named, probs, 0.0), axis=0, keepdims=True))
        table = jnp.where(expert_row == e, hits[e], table)
    ranking = dot(table.astype(BF16), earlier.astype(BF16), 1, 0)
    slot = lax.broadcasted_iota(jnp.int32, (CAPS, tokens), 0).astype(F32)
    batch = lax.div(lax.broadcasted_iota(jnp.int32, (CAPS, tokens), 1), tok_dev)
    ones, scales = [], []
    for e in range(window):
        chosen = (hits[e] > 0.5) & (ranking[e : e + 1] == slot)
        for m in range(micro):
            here = chosen & (batch == m)
            ones.append(jnp.where(here, 1.0, 0.0))
            scales.append(jnp.where(here, weights[e], 0.0))
    picking = jnp.concatenate(scales, axis=0).astype(BF16)

    loads[2].wait()
    sending = dot(picking, go_v[...], 1, 0).astype(BF16)
    for e in range(window):
        a_send[e] = sending[e * part : (e + 1) * part]
    pl.semaphore_wait(barrier, n_exp - 1 + chips)

    inner = jnp.where((member == 0) | (member == n_exp - 1), 0, 1)
    order = [1 + inner, 3, 2 - inner]
    arriving = [1, 2 + inner, 3 - inner]

    def member_at(k):
        low, high = lax.rem(k, 2), lax.div(k, 2)
        low = low * (1 - 2 * lax.rem(member, 2))
        high = high * (2 - 4 * lax.div(member, 2))
        return member + low + high

    for k in order:
        to = member_at(k)
        remote(a_send.at[lax.div(to, 2)], a_buf.at[member], a_sem.at[k - 1], {"expert": to})
    a_buf[member] = a_send[lax.div(member, 2)]

    weights_rows = width * cols // width
    arrivals(rows + 3 * weights_rows, load_sem.at[3]).wait()
    remote(x_v, x_par, x_sem.at[0], partner)
    inputs = x_v[...].reshape(rows, width)
    gate = dot(inputs, wg_v[...], 1, 0)
    up = dot(inputs, wu_v[...], 1, 0)
    sigmoid = jax.nn.sigmoid(gate)
    activated = gate * sigmoid
    h_all[chip] = (activated * up).astype(BF16)
    for k in hops:
        remote(h_all.at[chip], h_all.at[chip], slot_sem.at[0], peer_at(k))
    slope = up * sigmoid * (1.0 + gate * (1.0 - sigmoid))

    def blocks(q):
        return pl.ds(pl.multiple_of(q * pair_block, pair_block), pair_block)

    def send_slices(source):
        for k in hops:
            remote(
                a_buf.at[source, :, blocks(chip_at(k))],
                s_all.at[chip, source],
                slot_sem.at[0],
                peer_at(k),
            )

    send_slices(member)

    mix_v[...] = jnp.concatenate(
        [
            jnp.concatenate(ones[e * micro : (e + 1) * micro], axis=0)
            for e in range(window)
            for _ in range(2)
        ],
        axis=0,
    ).astype(BF16)
    pltpu.make_async_copy(x_par, x_par, x_sem.at[0]).wait()
    for k in range(chips):
        q = chip_at(k) if k else chip
        own = pl.ds(pl.multiple_of((q * 2 + core) * row_block, row_block), row_block)
        mine = x_v[:, :, own].reshape(rows, row_block)
        other = x_par[:, :, own].reshape(rows, row_block)
        xt_v[k] = jnp.concatenate([mine, other], axis=0).T

    for j, k in enumerate(arriving):
        source = member_at(k)
        pltpu.make_async_copy(a_buf.at[source], a_buf.at[source], a_sem.at[k - 1]).wait()
        if j < n_exp - 2:
            send_slices(source)
    scaled = a_buf[...].reshape(rows, width)
    dhidden = dot(scaled, wd_v[...], 1, 1)
    d_all[0, :, :cols] = (dhidden * slope).astype(BF16)
    d_all[0, :, cols:] = (dhidden * activated).astype(BF16)
    remote(d_all.at[0], d_all.at[1], d_sem.at[0], partner)
    send_slices(member_at(arriving[-1]))

    def send_back():
        returning = dot(d_all[0, :, :cols], wg_v[...], 1, 1) + dot(
            d_all[0, :, cols:], wu_v[...], 1, 1
        )
        returning = returning.astype(BF16)
        for h in range(n_exp):
            r_send[h] = returning[h * part : (h + 1) * part]
        for k in order:
            to = member_at(k)
            remote(r_send.at[to], r_buf.at[member], r_sem.at[0], {"expert": to}, False).start()

    sent.append((n_exp - 1) * part * width)
    returns_first = (core == 1) | (member != 0)

    @pl.when(returns_first)
    def _():
        send_back()

    pltpu.make_async_copy(d_all.at[1], d_all.at[1], d_sem.at[0]).wait()
    factors = d_all[...].reshape(2 * rows, 2 * cols)
    def send_half(i, k, value, dst, sem):
        last_send[i] = value.astype(BF16)
        remote(last_send.at[i], dst.at[i % 4], sem, peer_at(k))

    far = dot(xt_v[3], factors, 1, 0)
    send_half(4, 1, far[:, :cols], relay_buf, relay_sem.at[0])
    send_half(5, 2, far[:, cols:], relay_buf, relay_sem.at[1])
    near = [dot(xt_v[k], factors, 1, 0) for k in (1, 2)]
    send_half(0, 1, near[0][:, :cols], last_buf, last_sem.at[0])
    send_half(1, 2, near[1][:, cols:], last_buf, last_sem.at[0])
    total = dot(xt_v[0], factors, 1, 0)
    @pl.when(jnp.logical_not(returns_first))
    def _():
        send_back()

    r_buf[member] = r_send[member]
    s_all[chip] = a_buf[:, :, blocks(chip)]
    for i, (k, value) in enumerate(((2, near[1][:, :cols]), (1, near[0][:, cols:]))):
        pltpu.make_async_copy(relay_buf.at[i], relay_buf.at[i], relay_sem.at[i]).wait()
        send_half(
            2 + i, k, value + relay_buf[i].astype(F32), last_buf, last_sem.at[1]
        )
    others = (chips - 1) * (rows * cols + rows * pair_block)
    arrivals(others // width, slot_sem.at[0]).wait()
    slots = chips * rows
    down = dot(s_all[...].reshape(slots, pair_block), h_all[...].reshape(slots, cols), 0, 0)
    down_v[0] = down[:row_block]
    down_v[1] = down[row_block:]
    remote(down_v.at[1 - core], down_buf, down_sem.at[0], partner)

    arrivals((n_exp - 1) * part, r_sem.at[0]).wait()
    gin_ref[...] = dot(mix_v[...], r_buf[...].reshape(rows, width), 0, 0).astype(BF16)

    factor = 1.0 / (micro * n_dp)
    pltpu.make_async_copy(down_buf, down_buf, down_sem.at[0]).wait()
    gd_ref[...] = (down_v[core] + down_buf[...]) * factor
    halves = 2 * row_block * cols // width
    arrivals(halves, last_sem.at[0]).wait()
    gg_ref[...] = (total[:, :cols] + last_buf[0].astype(F32)) * factor
    gu_ref[...] = (total[:, cols:] + last_buf[1].astype(F32)) * factor
    arrivals(halves, last_sem.at[1]).wait()
    gg_ref[...] = gg_ref[...] + last_buf[2].astype(F32) * factor
    gu_ref[...] = gu_ref[...] + last_buf[3].astype(F32) * factor
    arrivals(sum(sent) // width, sent_sem.at[0]).wait()


def settle(*refs):
    count = len(refs) // 2
    sem = refs[-1]
    copies = [
        pltpu.make_async_copy(refs[i], refs[count + i], sem.at[i]) for i in range(count)
    ]
    for copy in copies:
        copy.start()
    for copy in copies:
        copy.wait()


def settled(arrays):
    anywhere = pl.BlockSpec(memory_space=pl.ANY)
    return pl.pallas_call(
        settle,
        out_shape=tuple(jax.ShapeDtypeStruct(a.shape, a.dtype) for a in arrays),
        in_specs=[pl.BlockSpec(memory_space=pltpu.VMEM)] * len(arrays),
        out_specs=(anywhere,) * len(arrays),
        scratch_shapes=[pltpu.SemaphoreType.DMA((len(arrays),))],
    )(*[pltpu.with_memory_space_constraint(a, pltpu.VMEM) for a in arrays])


def pooled_call(n_exp, n_dp, grad_out, routes, route_probs, dispatched, w_gate, w_up, w_down):
    micro, tok_dev, width = grad_out.shape
    cols = w_gate.shape[1]
    tokens = micro * tok_dev
    part = micro * CAPS
    rows = n_exp * part
    chips = n_dp // 2
    row_block = width // n_dp
    vmem = pl.BlockSpec(memory_space=pltpu.VMEM)
    hbm = pl.BlockSpec(memory_space=pl.ANY)
    grad = pltpu.VMEM((row_block, cols), F32)
    dma = pltpu.SemaphoreType.DMA
    return pl.pallas_call(
        functools.partial(pooled_kernel, micro, n_exp, n_dp),
        out_shape=(pltpu.VMEM((tokens, width), BF16), grad, grad, grad),
        in_specs=[hbm] * 7,
        out_specs=(vmem, vmem, vmem, vmem),
        scratch_shapes=[
            pltpu.VMEM((micro, routes.shape[2], tok_dev), jnp.int32),
            pltpu.VMEM((micro, routes.shape[2], tok_dev), BF16),
            pltpu.VMEM((tokens, width), BF16),
            pltpu.VMEM((n_exp, part, width), BF16),
            pltpu.VMEM((n_exp, part, width), BF16),
            pltpu.VMEM((chips, row_block, 2 * rows), BF16),
            pltpu.VMEM((width, cols), BF16),
            pltpu.VMEM((width, cols), BF16),
            pltpu.VMEM((cols, width), BF16),
            pltpu.VMEM((n_exp // 2, part, width), BF16),
            pltpu.VMEM((n_exp, part, width), BF16),
            pltpu.VMEM((n_exp, part, width), BF16),
            pltpu.VMEM((n_exp, part, width), BF16),
            pltpu.VMEM((rows, tokens), BF16),
            pltpu.VMEM((2, rows, 2 * cols), BF16),
            pltpu.VMEM((2, row_block, cols), BF16),
            pltpu.VMEM((6, row_block, cols), BF16),
            pltpu.VMEM((4, row_block, cols), BF16),
            pltpu.VMEM((chips, n_exp, part, 2 * row_block), BF16),
            pltpu.VMEM((chips, rows, cols), BF16),
            pltpu.VMEM((2, row_block, cols), F32),
            pltpu.VMEM((row_block, cols), F32),
            pltpu.VMEM((width, width), BF16),
            dma((4,)),
            dma((1,)),
            dma((n_exp - 1,)),
            dma((1,)),
            dma((1,)),
            dma((1,)),
            dma((2,)),
            dma((2,)),
            dma((1,)),
            dma((1,)),
        ],
        compiler_params=pltpu.CompilerParams(collective_id=0, has_side_effects=True),
    )(
        routes.transpose(0, 2, 1),
        route_probs.transpose(0, 2, 1),
        grad_out.reshape(tokens, width),
        dispatched.reshape(micro, n_exp, CAPS, width),
        w_gate,
        w_up,
        w_down,
    )


def spread_call(n_exp, n_dp, grad_out, routes, route_probs, dispatched, w_gate, w_up, w_down):
    micro, tok_dev, width = grad_out.shape
    cols = w_gate.shape[1]
    tokens = micro * tok_dev
    part = micro * CAPS
    rows = n_exp * part
    chips = n_dp // 2
    row_block = width // n_dp
    vmem = pl.BlockSpec(memory_space=pltpu.VMEM)
    hbm = pl.BlockSpec(memory_space=pl.ANY)
    grad = pltpu.VMEM((row_block, cols), F32)
    dma = pltpu.SemaphoreType.DMA
    others = max(chips - 1, 1)
    gather = row_block % 128 == 0
    return pl.pallas_call(
        functools.partial(kernel, micro, n_exp, n_dp),
        out_shape=(pltpu.VMEM((tokens, width), BF16), grad, grad, grad),
        in_specs=[vmem, vmem, hbm, hbm, hbm, hbm, hbm],
        out_specs=(vmem, vmem, vmem, vmem),
        scratch_shapes=[
            pltpu.VMEM((tokens, width), BF16),
            pltpu.VMEM((rows, width), BF16),
            pltpu.VMEM((width, cols), BF16),
            pltpu.VMEM((width, cols), BF16),
            pltpu.VMEM((cols, width), BF16),
            pltpu.VMEM((n_exp, part, width), BF16),
            pltpu.VMEM((n_exp, part, width), BF16),
            pltpu.VMEM((n_exp, part, width), BF16),
            pltpu.VMEM((n_exp, part, width), BF16),
            pltpu.VMEM((3, 2, chips, row_block, cols), F32),
            pltpu.VMEM((3, 2, chips, row_block, cols), BF16),
            pltpu.VMEM((3, chips, row_block, cols), BF16),
            pltpu.VMEM((3, chips, row_block, cols), BF16),
            pltpu.VMEM((3, others, row_block, cols), BF16),
            pltpu.VMEM((n_dp, n_exp, part, row_block) if gather else (8, 128), BF16),
            pltpu.VMEM((n_dp, rows, cols) if gather else (8, 128), BF16),
            dma((5,)),
            dma((n_exp - 1,)),
            dma((n_exp - 1,)),
            dma((n_exp - 1,)),
            dma((n_exp - 1,)),
            dma((3,)),
            dma((3,)),
            dma((3, others)),
            dma((3, others)),
            dma((n_dp - 1,)),
            dma((n_dp - 1,)),
            dma((n_dp - 1,)),
            dma((n_dp - 1,)),
        ],
        compiler_params=pltpu.CompilerParams(collective_id=0, has_side_effects=True),
    )(
        routes.transpose(0, 2, 1),
        route_probs.transpose(0, 2, 1),
        grad_out.reshape(tokens, width),
        dispatched.reshape(rows, width),
        w_gate,
        w_up,
        w_down,
    )


def per_device(n_exp, n_dp, grad_out, *rest):
    pooled = n_exp == 4 and n_dp == 8 and (grad_out.shape[2] // n_dp) % 128 == 0
    call = pooled_call if pooled else spread_call
    out = settled(call(n_exp, n_dp, grad_out, *rest))
    return (out[0].reshape(grad_out.shape),) + tuple(out[1:])


def solution(mesh):
    return jax.shard_map(
        functools.partial(per_device, mesh.shape["expert"], mesh.shape["dp"]),
        mesh=mesh,
        in_specs=(
            P(None, ("dp", "expert"), None),
            P(None, ("dp", "expert"), None),
            P(None, ("dp", "expert"), None),
            P(None, ("dp", "expert"), None),
            P(None, "expert"),
            P(None, "expert"),
            P("expert", None),
        ),
        out_specs=(
            P(None, ("dp", "expert"), None),
            P("dp", "expert"),
            P("dp", "expert"),
            P("dp", "expert"),
        ),
        check_vma=False,
    )
```

```python
import functools

import jax
import jax.numpy as jnp
from jax import lax
from jax.experimental import pallas as pl
from jax.experimental.pallas import tpu as pltpu
from jax.sharding import PartitionSpec as P

CAPS = 8
MESH = pl.DeviceIdType.MESH
BF16 = jnp.bfloat16
F32 = jnp.float32


def dot(left, right, lc, rc):
    return lax.dot_general(
        left, right, (((lc,), (rc,)), ((), ())), preferred_element_type=F32
    )


def flipped(index, bits):
    step = 1
    while step <= bits:
        if bits & step:
            index = index + step - 2 * step * lax.rem(lax.div(index, step), 2)
        step *= 2
    return index


def kernel(
    micro,
    n_exp,
    n_dp,
    routes_ref,
    probs_ref,
    go_hbm,
    x_hbm,
    wg_hbm,
    wu_hbm,
    wd_hbm,
    gin_ref,
    gg_ref,
    gu_ref,
    gd_ref,
    go_v,
    x_v,
    wg_v,
    wu_v,
    wd_v,
    a_send,
    a_buf,
    r_send,
    r_buf,
    acc,
    p1_send,
    p1_buf,
    p2_send,
    p2_buf,
    s_all,
    h_all,
    load_sem,
    a_ssem,
    a_rsem,
    r_ssem,
    r_rsem,
    p1_ssem,
    p1_rsem,
    p2_ssem,
    p2_rsem,
    s_ssem,
    s_rsem,
    h_ssem,
    h_rsem,
):
    member = lax.axis_index("expert")
    replica = lax.axis_index("dp")
    core = lax.rem(replica, 2)
    chip = lax.div(replica, 2)
    chips = n_dp // 2
    partner = {"dp": chip * 2 + 1 - core}
    window = n_exp // 2
    tokens = go_v.shape[0]
    width = go_v.shape[1]
    tok_dev = tokens // micro
    part = micro * CAPS
    rows = n_exp * part
    row_block = width // n_dp
    gather = row_block % 128 == 0

    def member_at(k):
        return flipped(member, k)

    def chip_at(k):
        return {"dp": flipped(chip, k) * 2 + core}

    loads = [
        pltpu.make_async_copy(src, dst, load_sem.at[i])
        for i, (src, dst) in enumerate(
            ((go_hbm, go_v), (x_hbm, x_v), (wg_hbm, wg_v), (wu_hbm, wu_v), (wd_hbm, wd_v))
        )
    ]
    for load in loads:
        load.start()

    barrier = pltpu.get_barrier_semaphore()
    for k in range(1, n_exp):
        pl.semaphore_signal(
            barrier, inc=1, device_id={"expert": member_at(k)}, device_id_type=MESH
        )
    for k in range(1, n_dp):
        pl.semaphore_signal(
            barrier, inc=1, device_id={"dp": flipped(replica, k)}, device_id_type=MESH
        )

    ids = jnp.concatenate([routes_ref[m] for m in range(micro)], axis=1)
    probs = jnp.concatenate([probs_ref[m].astype(F32) for m in range(micro)], axis=1)
    pad = max(window, 8)
    expert_row = lax.broadcasted_iota(jnp.int32, (pad, tokens), 0)
    hits, weights = [], []
    table = jnp.zeros((pad, tokens), F32)
    for e in range(window):
        named = ids == e
        hits.append(jnp.sum(jnp.where(named, 1.0, 0.0), axis=0, keepdims=True))
        weights.append(jnp.sum(jnp.where(named, probs, 0.0), axis=0, keepdims=True))
        table = jnp.where(expert_row == e, hits[e], table)
    ti = lax.broadcasted_iota(jnp.int32, (tokens, tokens), 0)
    tj = lax.broadcasted_iota(jnp.int32, (tokens, tokens), 1)
    earlier = jnp.where((ti < tj) & (lax.div(ti, tok_dev) == lax.div(tj, tok_dev)), 1.0, 0.0)
    ranking = dot(table.astype(BF16), earlier.astype(BF16), 1, 0)
    slot = lax.broadcasted_iota(jnp.int32, (CAPS, tokens), 0).astype(F32)
    batch = lax.div(lax.broadcasted_iota(jnp.int32, (CAPS, tokens), 1), tok_dev)
    ones, scales = [], []
    for h in range(n_exp):
        e = h // 2
        chosen = (hits[e] > 0.5) & (ranking[e : e + 1] == slot)
        for m in range(micro):
            here = chosen & (batch == m)
            ones.append(jnp.where(here, 1.0, 0.0))
            scales.append(jnp.where(here, weights[e], 0.0))
    mixing = jnp.concatenate(ones, axis=0).astype(BF16)
    picking = jnp.concatenate(scales, axis=0).astype(BF16)

    loads[0].wait()
    sending = dot(picking, go_v[...], 1, 0).astype(BF16)
    for h in range(n_exp):
        a_send[h] = sending[h * part : (h + 1) * part]
    pl.semaphore_wait(barrier, n_exp - 1 + n_dp - 1)
    def a_copy(k, src, slot, to):
        return pltpu.make_async_remote_copy(
            src_ref=src,
            dst_ref=a_buf.at[slot],
            send_sem=a_ssem.at[k - 1],
            recv_sem=a_rsem.at[k - 1],
            device_id={"expert": to},
            device_id_type=MESH,
        )

    a_copies = {}
    for k in range(1, n_exp):
        a_copies[k] = a_copy(k, a_send.at[member_at(k)], member, member_at(k))
        a_copies[k].start()
    a_buf[member] = a_send[member]

    loads[1].wait()
    ri = lax.broadcasted_iota(jnp.int32, (rows, rows), 0)
    rj = lax.broadcasted_iota(jnp.int32, (rows, rows), 1)
    wanted = (
        lax.rem(lax.div(ri, CAPS), micro) * (n_exp * CAPS)
        + lax.div(ri, part) * CAPS
        + lax.rem(ri, CAPS)
    )
    inputs = dot(jnp.where(rj == wanted, 1.0, 0.0).astype(BF16), x_v[...], 1, 0).astype(BF16)
    loads[2].wait()
    gate = dot(inputs, wg_v[...], 1, 0)
    loads[3].wait()
    up = dot(inputs, wu_v[...], 1, 0)
    sigmoid = jax.nn.sigmoid(gate)
    activated = gate * sigmoid
    hidden = (activated * up).astype(BF16)
    h_copies, s_copies = [], []
    if gather:
        h_all[replica] = hidden
        for k in range(n_dp - 1, 0, -1):
            copy = pltpu.make_async_remote_copy(
                src_ref=h_all.at[replica],
                dst_ref=h_all.at[replica],
                send_sem=h_ssem.at[k - 1],
                recv_sem=h_rsem.at[k - 1],
                device_id={"dp": flipped(replica, k)},
                device_id_type=MESH,
            )
            copy.start()
            h_copies.append(copy)
    slope = up * sigmoid * (1.0 + gate * (1.0 - sigmoid))
    loads[4].wait()

    def p1_copy(o):
        return pltpu.make_async_remote_copy(
            src_ref=p1_send.at[o, 1 - core],
            dst_ref=p1_buf.at[o],
            send_sem=p1_ssem.at[o],
            recv_sem=p1_rsem.at[o],
            device_id=partner,
            device_id_type=MESH,
        )

    def store_terms(o, value):
        for d in range(n_dp):
            block = value[d * row_block : (d + 1) * row_block]
            acc[o, d % 2, d // 2] = block
            p1_send[o, d % 2, d // 2] = block.astype(BF16)

    p1_copies, p2_copies = {}, {}

    def start_p1(o, value):
        store_terms(o, value)
        p1_copies[o] = p1_copy(o)
        p1_copies[o].start()

    def start_p2(o):
        p1_copies[o].wait_recv()
        for k in range(chips - 1, 0, -1):
            q = flipped(chip, k)
            p2_send[o, q] = (acc[o, core, q] + p1_buf[o, q].astype(F32)).astype(BF16)
            copy = pltpu.make_async_remote_copy(
                src_ref=p2_send.at[o, q],
                dst_ref=p2_buf.at[o, k - 1],
                send_sem=p2_ssem.at[o, k - 1],
                recv_sem=p2_rsem.at[o, k - 1],
                device_id=chip_at(k),
                device_id_type=MESH,
            )
            copy.start()
            p2_copies[o, k] = copy

    for k in range(1, n_exp):
        a_copies[k].wait_recv()
    scaled = a_buf[...].reshape(rows, width)
    if gather:
        for k in range(n_dp - 1, 0, -1):
            peer = flipped(replica, k)
            columns = pl.ds(pl.multiple_of(peer * row_block, row_block), row_block)
            copy = pltpu.make_async_remote_copy(
                src_ref=a_buf.at[:, :, columns],
                dst_ref=s_all.at[replica],
                send_sem=s_ssem.at[k - 1],
                recv_sem=s_rsem.at[k - 1],
                device_id={"dp": peer},
                device_id_type=MESH,
            )
            copy.start()
            s_copies.append(copy)
    else:
        start_p1(0, dot(scaled, hidden, 0, 0))
    dhidden = dot(scaled, wd_v[...], 1, 1)
    d_gate = (dhidden * slope).astype(BF16)
    d_up = (dhidden * activated).astype(BF16)
    returning = (dot(d_gate, wg_v[...], 1, 1) + dot(d_up, wu_v[...], 1, 1)).astype(BF16)
    for h in range(n_exp):
        r_send[h] = returning[h * part : (h + 1) * part]
    r_copies = []
    for k in range(n_exp - 1, 0, -1):
        copy = pltpu.make_async_remote_copy(
            src_ref=r_send.at[member_at(k)],
            dst_ref=r_buf.at[member],
            send_sem=r_ssem.at[k - 1],
            recv_sem=r_rsem.at[k - 1],
            device_id={"expert": member_at(k)},
            device_id_type=MESH,
        )
        copy.start()
        r_copies.append(copy)
    start_p1(1, dot(inputs, d_gate, 0, 0))
    start_p1(2, dot(inputs, d_up, 0, 0))
    if not gather:
        start_p2(0)
    r_buf[member] = r_send[member]
    start_p2(1)
    start_p2(2)

    if gather:
        own = pl.ds(pl.multiple_of(replica * row_block, row_block), row_block)
        s_all[replica] = a_buf[:, :, own]
        for copy in h_copies + s_copies:
            copy.wait_recv()
        slots = n_dp * rows
        down = dot(
            s_all[...].reshape(slots, row_block), h_all[...].reshape(slots, wg_v.shape[1]), 0, 0
        )
        gd_ref[...] = down * (1.0 / (micro * n_dp))
    for copy in r_copies:
        copy.wait_recv()
    gin_ref[...] = dot(mixing, r_buf[...].reshape(rows, width), 0, 0).astype(BF16)

    factor = 1.0 / (micro * n_dp)
    for o, out in enumerate((gd_ref, gg_ref, gu_ref)):
        if o not in p1_copies:
            continue
        total = acc[o, core, chip] + p1_buf[o, chip].astype(F32)
        for k in range(chips - 1, 0, -1):
            p2_copies[o, k].wait_recv()
            total = total + p2_buf[o, k - 1].astype(F32)
        out[...] = total * factor
    started = [*a_copies.values(), *p1_copies.values(), *p2_copies.values()]
    for copy in started + r_copies + h_copies + s_copies:
        copy.wait_send()


def pooled_kernel(
    micro,
    n_exp,
    n_dp,
    routes_hbm,
    probs_hbm,
    go_hbm,
    x_hbm,
    wg_hbm,
    wu_hbm,
    wd_hbm,
    gin_ref,
    gg_ref,
    gu_ref,
    gd_ref,
    routes_v,
    probs_v,
    go_v,
    x_v,
    x_par,
    xt_v,
    wg_v,
    wu_v,
    wd_v,
    a_send,
    a_buf,
    r_send,
    r_buf,
    mix_v,
    d_all,
    relay_buf,
    last_send,
    last_buf,
    s_all,
    h_all,
    down_v,
    down_buf,
    sized,
    load_sem,
    sent_sem,
    a_sem,
    r_sem,
    x_sem,
    d_sem,
    relay_sem,
    last_sem,
    slot_sem,
    down_sem,
):
    member = lax.axis_index("expert")
    replica = lax.axis_index("dp")
    core = lax.rem(replica, 2)
    chip = lax.div(replica, 2)
    chips = n_dp // 2
    partner = {"dp": chip * 2 + 1 - core}
    window = n_exp // 2
    tokens, width = go_v.shape
    cols = wg_v.shape[1]
    tok_dev = tokens // micro
    part = micro * CAPS
    rows = n_exp * part
    row_block = width // n_dp
    pair_block = 2 * row_block
    hops = range(chips - 1, 0, -1)

    def chip_at(k):
        return flipped(chip, k)

    def peer_at(k):
        return {"dp": chip_at(k) * 2 + core}

    loads = [
        pltpu.make_async_copy(src, dst, load_sem.at[min(i, 3)])
        for i, (src, dst) in enumerate(
            (
                (routes_hbm, routes_v),
                (probs_hbm, probs_v),
                (go_hbm, go_v),
                *((x_hbm.at[m], x_v.at[:, pl.ds(m * CAPS, CAPS), :]) for m in range(micro)),
                (wg_hbm, wg_v),
                (wu_hbm, wu_v),
                (wd_hbm, wd_v),
            )
        )
    ]
    for load in loads[:3]:
        load.start()

    barrier = pltpu.get_barrier_semaphore()
    for k in range(n_exp - 1, 0, -1):
        pl.semaphore_signal(
            barrier, inc=1, device_id={"expert": flipped(member, k)}, device_id_type=MESH
        )
    for k in hops:
        pl.semaphore_signal(barrier, inc=1, device_id=peer_at(k), device_id_type=MESH)
    pl.semaphore_signal(barrier, inc=1, device_id=partner, device_id_type=MESH)

    def arrivals(size, sem):
        return pltpu.make_async_copy(sized.at[pl.ds(0, size)], sized.at[pl.ds(0, size)], sem)

    sent = []

    def remote(src, dst, sem, device, counted=True):
        copy = pltpu.make_async_remote_copy(
            src_ref=src,
            dst_ref=dst,
            send_sem=sent_sem.at[0],
            recv_sem=sem,
            device_id=device,
            device_id_type=MESH,
        )
        copy.start()
        if counted:
            bulk = 1
            for n in src.shape:
                bulk *= n
            sent.append(bulk * (2 if src.dtype == F32 else 1))

    pad = max(window, 8)
    expert_row = lax.broadcasted_iota(jnp.int32, (pad, tokens), 0)
    ti = lax.broadcasted_iota(jnp.int32, (tokens, tokens), 0)
    tj = lax.broadcasted_iota(jnp.int32, (tokens, tokens), 1)
    earlier = jnp.where((ti < tj) & (lax.div(ti, tok_dev) == lax.div(tj, tok_dev)), 1.0, 0.0)
    loads[0].wait()
    loads[1].wait()
    ids = jnp.concatenate([routes_v[m] for m in range(micro)], axis=1)
    probs = jnp.concatenate([probs_v[m].astype(F32) for m in range(micro)], axis=1)
    hits, weights = [], []
    table = jnp.zeros((pad, tokens), F32)
    for e in range(window):
        named = ids == e
        hits.append(jnp.sum(jnp.where(named, 1.0, 0.0), axis=0, keepdims=True))
        weights.append(jnp.sum(jnp.where(named, probs, 0.0), axis=0, keepdims=True))
        table = jnp.where(expert_row == e, hits[e], table)
    ranking = dot(table.astype(BF16), earlier.astype(BF16), 1, 0)
    slot = lax.broadcasted_iota(jnp.int32, (CAPS, tokens), 0).astype(F32)
    batch = lax.div(lax.broadcasted_iota(jnp.int32, (CAPS, tokens), 1), tok_dev)
    ones, scales = [], []
    for e in range(window):
        chosen = (hits[e] > 0.5) & (ranking[e : e + 1] == slot)
        for m in range(micro):
            here = chosen & (batch == m)
            ones.append(jnp.where(here, 1.0, 0.0))
            scales.append(jnp.where(here, weights[e], 0.0))
    picking = jnp.concatenate(scales, axis=0).astype(BF16)

    loads[2].wait()
    for load in loads[3:]:
        load.start()
    sending = dot(picking, go_v[...], 1, 0).astype(BF16)
    for e in range(window):
        a_send[e] = sending[e * part : (e + 1) * part]
    pl.semaphore_wait(barrier, n_exp - 1 + chips)

    inner = jnp.where((member == 0) | (member == n_exp - 1), 0, 1)
    order = [1 + inner, 3, 2 - inner]
    arriving = [1, 2 + inner, 3 - inner]

    def member_at(k):
        low, high = lax.rem(k, 2), lax.div(k, 2)
        low = low * (1 - 2 * lax.rem(member, 2))
        high = high * (2 - 4 * lax.div(member, 2))
        return member + low + high

    for k in order:
        to = member_at(k)
        remote(a_send.at[lax.div(to, 2)], a_buf.at[member], a_sem.at[k - 1], {"expert": to})
    a_buf[member] = a_send[lax.div(member, 2)]

    weights_rows = width * cols // width
    arrivals(rows + 3 * weights_rows, load_sem.at[3]).wait()
    remote(x_v, x_par, x_sem.at[0], partner)
    inputs = x_v[...].reshape(rows, width)
    gate = dot(inputs, wg_v[...], 1, 0)
    up = dot(inputs, wu_v[...], 1, 0)
    sigmoid = jax.nn.sigmoid(gate)
    activated = gate * sigmoid
    h_all[chip] = (activated * up).astype(BF16)
    for k in hops:
        remote(h_all.at[chip], h_all.at[chip], slot_sem.at[0], peer_at(k))
    slope = up * sigmoid * (1.0 + gate * (1.0 - sigmoid))

    def blocks(q):
        return pl.ds(pl.multiple_of(q * pair_block, pair_block), pair_block)

    def send_slices(source, counted=True):
        for k in hops:
            remote(
                a_buf.at[source, :, blocks(chip_at(k))],
                s_all.at[chip, source],
                slot_sem.at[0],
                peer_at(k),
                counted,
            )

    send_slices(member)

    mix_v[...] = jnp.concatenate(
        [
            jnp.concatenate(ones[e * micro : (e + 1) * micro], axis=0)
            for e in range(window)
            for _ in range(2)
        ],
        axis=0,
    ).astype(BF16)
    pltpu.make_async_copy(x_par, x_par, x_sem.at[0]).wait()
    for k in range(chips):
        q = chip_at(k) if k else chip
        own = pl.ds(pl.multiple_of((q * 2 + core) * row_block, row_block), row_block)
        mine = x_v[:, :, own].reshape(rows, row_block)
        other = x_par[:, :, own].reshape(rows, row_block)
        xt_v[k] = jnp.concatenate([mine, other], axis=0).T

    for j, k in enumerate(arriving):
        source = member_at(k)
        pltpu.make_async_copy(a_buf.at[source], a_buf.at[source], a_sem.at[k - 1]).wait()
        if j < n_exp - 2:
            send_slices(source)
    scaled = a_buf[...].reshape(rows, width)
    dhidden = dot(scaled, wd_v[...], 1, 1)
    d_all[0, :, :cols] = (dhidden * slope).astype(BF16)
    d_all[0, :, cols:] = (dhidden * activated).astype(BF16)
    remote(d_all.at[0], d_all.at[1], d_sem.at[0], partner)

    @pl.when(core == 1)
    def _():
        send_slices(member_at(arriving[-1]), False)

    sent.append((chips - 1) * part * pair_block)

    def send_back():
        returning = dot(d_all[0, :, :cols], wg_v[...], 1, 1) + dot(
            d_all[0, :, cols:], wu_v[...], 1, 1
        )
        returning = returning.astype(BF16)
        for h in range(n_exp):
            r_send[h] = returning[h * part : (h + 1) * part]
        for k in (3 - inner, 2 + inner, 1):
            to = member_at(k)
            remote(r_send.at[to], r_buf.at[member], r_sem.at[0], {"expert": to}, False)

    sent.append((n_exp - 1) * part * width)
    returns_first = (core == 1) | (member != 0)

    @pl.when(returns_first)
    def _():
        send_back()

    pltpu.make_async_copy(d_all.at[1], d_all.at[1], d_sem.at[0]).wait()
    factors = d_all[...].reshape(2 * rows, 2 * cols)
    def send_half(i, k, value, dst, sem):
        last_send[i] = value.astype(BF16)
        remote(last_send.at[i], dst.at[i % 4], sem, peer_at(k))

    far = dot(xt_v[3], factors, 1, 0)
    last_send[4] = far[:, :cols].astype(BF16)
    last_send[5] = far[:, cols:].astype(BF16)
    strips = [pl.ds(c * row_block // 2, row_block // 2) for c in range(2)]
    for c, strip in enumerate(strips):
        for i in range(2):
            remote(
                last_send.at[4 + i, strip],
                relay_buf.at[i, strip],
                relay_sem.at[i, c],
                peer_at(1 + i),
            )

    @pl.when(core == 0)
    def _():
        send_slices(member_at(arriving[-1]), False)

    near = [dot(xt_v[k], factors, 1, 0) for k in (1, 2)]
    send_half(0, 1, near[0][:, :cols], last_buf, last_sem.at[0])
    send_half(1, 2, near[1][:, cols:], last_buf, last_sem.at[0])
    total = dot(xt_v[0], factors, 1, 0)
    @pl.when(jnp.logical_not(returns_first))
    def _():
        send_back()

    r_buf[member] = r_send[member]
    s_all[chip] = a_buf[:, :, blocks(chip)]
    own_term = (near[1][:, :cols], near[0][:, cols:])
    for c, strip in enumerate(strips):
        for i in range(2):
            piece = relay_buf.at[i, strip]
            pltpu.make_async_copy(piece, piece, relay_sem.at[i, c]).wait()
            value = own_term[i][c * row_block // 2 : (c + 1) * row_block // 2]
            last_send[2 + i, strip] = (value + piece[...].astype(F32)).astype(BF16)
            remote(
                last_send.at[2 + i, strip],
                last_buf.at[2 + i, strip],
                last_sem.at[1],
                peer_at(2 - i),
            )
    others = (chips - 1) * (rows * cols + rows * pair_block)
    arrivals(others // width, slot_sem.at[0]).wait()
    slots = chips * rows
    down = dot(s_all[...].reshape(slots, pair_block), h_all[...].reshape(slots, cols), 0, 0)
    down_v[0] = down[:row_block]
    down_v[1] = down[row_block:]
    remote(down_v.at[1 - core], down_buf, down_sem.at[0], partner)

    arrivals((n_exp - 1) * part, r_sem.at[0]).wait()
    gin_ref[...] = dot(mix_v[...], r_buf[...].reshape(rows, width), 0, 0).astype(BF16)

    factor = 1.0 / (micro * n_dp)
    pltpu.make_async_copy(down_buf, down_buf, down_sem.at[0]).wait()
    gd_ref[...] = (down_v[core] + down_buf[...]) * factor
    halves = 2 * row_block * cols // width
    arrivals(halves, last_sem.at[0]).wait()
    gg_ref[...] = (total[:, :cols] + last_buf[0].astype(F32)) * factor
    gu_ref[...] = (total[:, cols:] + last_buf[1].astype(F32)) * factor
    arrivals(halves, last_sem.at[1]).wait()
    gg_ref[...] = gg_ref[...] + last_buf[2].astype(F32) * factor
    gu_ref[...] = gu_ref[...] + last_buf[3].astype(F32) * factor
    arrivals(sum(sent) // width, sent_sem.at[0]).wait()


def settle(*refs):
    count = len(refs) // 2
    sem = refs[-1]
    copies = [
        pltpu.make_async_copy(refs[i], refs[count + i], sem.at[i]) for i in range(count)
    ]
    for copy in copies:
        copy.start()
    for copy in copies:
        copy.wait()


def settled(arrays):
    anywhere = pl.BlockSpec(memory_space=pl.ANY)
    return pl.pallas_call(
        settle,
        out_shape=tuple(jax.ShapeDtypeStruct(a.shape, a.dtype) for a in arrays),
        in_specs=[pl.BlockSpec(memory_space=pltpu.VMEM)] * len(arrays),
        out_specs=(anywhere,) * len(arrays),
        scratch_shapes=[pltpu.SemaphoreType.DMA((len(arrays),))],
    )(*[pltpu.with_memory_space_constraint(a, pltpu.VMEM) for a in arrays])


def pooled_call(n_exp, n_dp, grad_out, routes, route_probs, dispatched, w_gate, w_up, w_down):
    micro, tok_dev, width = grad_out.shape
    cols = w_gate.shape[1]
    tokens = micro * tok_dev
    part = micro * CAPS
    rows = n_exp * part
    chips = n_dp // 2
    row_block = width // n_dp
    vmem = pl.BlockSpec(memory_space=pltpu.VMEM)
    hbm = pl.BlockSpec(memory_space=pl.ANY)
    grad = pltpu.VMEM((row_block, cols), F32)
    dma = pltpu.SemaphoreType.DMA
    return pl.pallas_call(
        functools.partial(pooled_kernel, micro, n_exp, n_dp),
        out_shape=(pltpu.VMEM((tokens, width), BF16), grad, grad, grad),
        in_specs=[hbm] * 7,
        out_specs=(vmem, vmem, vmem, vmem),
        scratch_shapes=[
            pltpu.VMEM((micro, routes.shape[2], tok_dev), jnp.int32),
            pltpu.VMEM((micro, routes.shape[2], tok_dev), BF16),
            pltpu.VMEM((tokens, width), BF16),
            pltpu.VMEM((n_exp, part, width), BF16),
            pltpu.VMEM((n_exp, part, width), BF16),
            pltpu.VMEM((chips, row_block, 2 * rows), BF16),
            pltpu.VMEM((width, cols), BF16),
            pltpu.VMEM((width, cols), BF16),
            pltpu.VMEM((cols, width), BF16),
            pltpu.VMEM((n_exp // 2, part, width), BF16),
            pltpu.VMEM((n_exp, part, width), BF16),
            pltpu.VMEM((n_exp, part, width), BF16),
            pltpu.VMEM((n_exp, part, width), BF16),
            pltpu.VMEM((rows, tokens), BF16),
            pltpu.VMEM((2, rows, 2 * cols), BF16),
            pltpu.VMEM((2, row_block, cols), BF16),
            pltpu.VMEM((6, row_block, cols), BF16),
            pltpu.VMEM((4, row_block, cols), BF16),
            pltpu.VMEM((chips, n_exp, part, 2 * row_block), BF16),
            pltpu.VMEM((chips, rows, cols), BF16),
            pltpu.VMEM((2, row_block, cols), F32),
            pltpu.VMEM((row_block, cols), F32),
            pltpu.VMEM((width, width), BF16),
            dma((4,)),
            dma((1,)),
            dma((n_exp - 1,)),
            dma((1,)),
            dma((1,)),
            dma((1,)),
            dma((2, 2)),
            dma((2,)),
            dma((1,)),
            dma((1,)),
        ],
        compiler_params=pltpu.CompilerParams(collective_id=0, has_side_effects=True),
    )(
        routes.transpose(0, 2, 1),
        route_probs.transpose(0, 2, 1),
        grad_out.reshape(tokens, width),
        dispatched.reshape(micro, n_exp, CAPS, width),
        w_gate,
        w_up,
        w_down,
    )


def spread_call(n_exp, n_dp, grad_out, routes, route_probs, dispatched, w_gate, w_up, w_down):
    micro, tok_dev, width = grad_out.shape
    cols = w_gate.shape[1]
    tokens = micro * tok_dev
    part = micro * CAPS
    rows = n_exp * part
    chips = n_dp // 2
    row_block = width // n_dp
    vmem = pl.BlockSpec(memory_space=pltpu.VMEM)
    hbm = pl.BlockSpec(memory_space=pl.ANY)
    grad = pltpu.VMEM((row_block, cols), F32)
    dma = pltpu.SemaphoreType.DMA
    others = max(chips - 1, 1)
    gather = row_block % 128 == 0
    return pl.pallas_call(
        functools.partial(kernel, micro, n_exp, n_dp),
        out_shape=(pltpu.VMEM((tokens, width), BF16), grad, grad, grad),
        in_specs=[vmem, vmem, hbm, hbm, hbm, hbm, hbm],
        out_specs=(vmem, vmem, vmem, vmem),
        scratch_shapes=[
            pltpu.VMEM((tokens, width), BF16),
            pltpu.VMEM((rows, width), BF16),
            pltpu.VMEM((width, cols), BF16),
            pltpu.VMEM((width, cols), BF16),
            pltpu.VMEM((cols, width), BF16),
            pltpu.VMEM((n_exp, part, width), BF16),
            pltpu.VMEM((n_exp, part, width), BF16),
            pltpu.VMEM((n_exp, part, width), BF16),
            pltpu.VMEM((n_exp, part, width), BF16),
            pltpu.VMEM((3, 2, chips, row_block, cols), F32),
            pltpu.VMEM((3, 2, chips, row_block, cols), BF16),
            pltpu.VMEM((3, chips, row_block, cols), BF16),
            pltpu.VMEM((3, chips, row_block, cols), BF16),
            pltpu.VMEM((3, others, row_block, cols), BF16),
            pltpu.VMEM((n_dp, n_exp, part, row_block) if gather else (8, 128), BF16),
            pltpu.VMEM((n_dp, rows, cols) if gather else (8, 128), BF16),
            dma((5,)),
            dma((n_exp - 1,)),
            dma((n_exp - 1,)),
            dma((n_exp - 1,)),
            dma((n_exp - 1,)),
            dma((3,)),
            dma((3,)),
            dma((3, others)),
            dma((3, others)),
            dma((n_dp - 1,)),
            dma((n_dp - 1,)),
            dma((n_dp - 1,)),
            dma((n_dp - 1,)),
        ],
        compiler_params=pltpu.CompilerParams(collective_id=0, has_side_effects=True),
    )(
        routes.transpose(0, 2, 1),
        route_probs.transpose(0, 2, 1),
        grad_out.reshape(tokens, width),
        dispatched.reshape(rows, width),
        w_gate,
        w_up,
        w_down,
    )


def per_device(n_exp, n_dp, grad_out, *rest):
    pooled = n_exp == 4 and n_dp == 8 and (grad_out.shape[2] // n_dp) % 128 == 0
    call = pooled_call if pooled else spread_call
    out = settled(call(n_exp, n_dp, grad_out, *rest))
    return (out[0].reshape(grad_out.shape),) + tuple(out[1:])


def solution(mesh):
    return jax.shard_map(
        functools.partial(per_device, mesh.shape["expert"], mesh.shape["dp"]),
        mesh=mesh,
        in_specs=(
            P(None, ("dp", "expert"), None),
            P(None, ("dp", "expert"), None),
            P(None, ("dp", "expert"), None),
            P(None, ("dp", "expert"), None),
            P(None, "expert"),
            P(None, "expert"),
            P("expert", None),
        ),
        out_specs=(
            P(None, ("dp", "expert"), None),
            P("dp", "expert"),
            P("dp", "expert"),
            P("dp", "expert"),
        ),
        check_vma=False,
    )
```

```python
import functools

import jax
import jax.numpy as jnp
from jax import lax
from jax.experimental import pallas as pl
from jax.experimental.pallas import tpu as pltpu
from jax.sharding import PartitionSpec as P

CAPS = 8
MESH = pl.DeviceIdType.MESH
BF16 = jnp.bfloat16
F32 = jnp.float32


def dot(left, right, lc, rc):
    return lax.dot_general(
        left, right, (((lc,), (rc,)), ((), ())), preferred_element_type=F32
    )


def flipped(index, bits):
    step = 1
    while step <= bits:
        if bits & step:
            index = index + step - 2 * step * lax.rem(lax.div(index, step), 2)
        step *= 2
    return index


def kernel(
    micro,
    n_exp,
    n_dp,
    routes_ref,
    probs_ref,
    go_hbm,
    x_hbm,
    wg_hbm,
    wu_hbm,
    wd_hbm,
    gin_ref,
    gg_ref,
    gu_ref,
    gd_ref,
    go_v,
    x_v,
    wg_v,
    wu_v,
    wd_v,
    a_send,
    a_buf,
    r_send,
    r_buf,
    acc,
    p1_send,
    p1_buf,
    p2_send,
    p2_buf,
    s_all,
    h_all,
    load_sem,
    a_ssem,
    a_rsem,
    r_ssem,
    r_rsem,
    p1_ssem,
    p1_rsem,
    p2_ssem,
    p2_rsem,
    s_ssem,
    s_rsem,
    h_ssem,
    h_rsem,
):
    member = lax.axis_index("expert")
    replica = lax.axis_index("dp")
    core = lax.rem(replica, 2)
    chip = lax.div(replica, 2)
    chips = n_dp // 2
    partner = {"dp": chip * 2 + 1 - core}
    window = n_exp // 2
    tokens = go_v.shape[0]
    width = go_v.shape[1]
    tok_dev = tokens // micro
    part = micro * CAPS
    rows = n_exp * part
    row_block = width // n_dp
    gather = row_block % 128 == 0

    def member_at(k):
        return flipped(member, k)

    def chip_at(k):
        return {"dp": flipped(chip, k) * 2 + core}

    loads = [
        pltpu.make_async_copy(src, dst, load_sem.at[i])
        for i, (src, dst) in enumerate(
            ((go_hbm, go_v), (x_hbm, x_v), (wg_hbm, wg_v), (wu_hbm, wu_v), (wd_hbm, wd_v))
        )
    ]
    for load in loads:
        load.start()

    barrier = pltpu.get_barrier_semaphore()
    for k in range(1, n_exp):
        pl.semaphore_signal(
            barrier, inc=1, device_id={"expert": member_at(k)}, device_id_type=MESH
        )
    for k in range(1, n_dp):
        pl.semaphore_signal(
            barrier, inc=1, device_id={"dp": flipped(replica, k)}, device_id_type=MESH
        )

    ids = jnp.concatenate([routes_ref[m] for m in range(micro)], axis=1)
    probs = jnp.concatenate([probs_ref[m].astype(F32) for m in range(micro)], axis=1)
    pad = max(window, 8)
    expert_row = lax.broadcasted_iota(jnp.int32, (pad, tokens), 0)
    hits, weights = [], []
    table = jnp.zeros((pad, tokens), F32)
    for e in range(window):
        named = ids == e
        hits.append(jnp.sum(jnp.where(named, 1.0, 0.0), axis=0, keepdims=True))
        weights.append(jnp.sum(jnp.where(named, probs, 0.0), axis=0, keepdims=True))
        table = jnp.where(expert_row == e, hits[e], table)
    ti = lax.broadcasted_iota(jnp.int32, (tokens, tokens), 0)
    tj = lax.broadcasted_iota(jnp.int32, (tokens, tokens), 1)
    earlier = jnp.where((ti < tj) & (lax.div(ti, tok_dev) == lax.div(tj, tok_dev)), 1.0, 0.0)
    ranking = dot(table.astype(BF16), earlier.astype(BF16), 1, 0)
    slot = lax.broadcasted_iota(jnp.int32, (CAPS, tokens), 0).astype(F32)
    batch = lax.div(lax.broadcasted_iota(jnp.int32, (CAPS, tokens), 1), tok_dev)
    ones, scales = [], []
    for h in range(n_exp):
        e = h // 2
        chosen = (hits[e] > 0.5) & (ranking[e : e + 1] == slot)
        for m in range(micro):
            here = chosen & (batch == m)
            ones.append(jnp.where(here, 1.0, 0.0))
            scales.append(jnp.where(here, weights[e], 0.0))
    mixing = jnp.concatenate(ones, axis=0).astype(BF16)
    picking = jnp.concatenate(scales, axis=0).astype(BF16)

    loads[0].wait()
    sending = dot(picking, go_v[...], 1, 0).astype(BF16)
    for h in range(n_exp):
        a_send[h] = sending[h * part : (h + 1) * part]
    pl.semaphore_wait(barrier, n_exp - 1 + n_dp - 1)
    def a_copy(k, src, slot, to):
        return pltpu.make_async_remote_copy(
            src_ref=src,
            dst_ref=a_buf.at[slot],
            send_sem=a_ssem.at[k - 1],
            recv_sem=a_rsem.at[k - 1],
            device_id={"expert": to},
            device_id_type=MESH,
        )

    a_copies = {}
    for k in range(1, n_exp):
        a_copies[k] = a_copy(k, a_send.at[member_at(k)], member, member_at(k))
        a_copies[k].start()
    a_buf[member] = a_send[member]

    loads[1].wait()
    ri = lax.broadcasted_iota(jnp.int32, (rows, rows), 0)
    rj = lax.broadcasted_iota(jnp.int32, (rows, rows), 1)
    wanted = (
        lax.rem(lax.div(ri, CAPS), micro) * (n_exp * CAPS)
        + lax.div(ri, part) * CAPS
        + lax.rem(ri, CAPS)
    )
    inputs = dot(jnp.where(rj == wanted, 1.0, 0.0).astype(BF16), x_v[...], 1, 0).astype(BF16)
    loads[2].wait()
    gate = dot(inputs, wg_v[...], 1, 0)
    loads[3].wait()
    up = dot(inputs, wu_v[...], 1, 0)
    sigmoid = jax.nn.sigmoid(gate)
    activated = gate * sigmoid
    hidden = (activated * up).astype(BF16)
    h_copies, s_copies = [], []
    if gather:
        h_all[replica] = hidden
        for k in range(n_dp - 1, 0, -1):
            copy = pltpu.make_async_remote_copy(
                src_ref=h_all.at[replica],
                dst_ref=h_all.at[replica],
                send_sem=h_ssem.at[k - 1],
                recv_sem=h_rsem.at[k - 1],
                device_id={"dp": flipped(replica, k)},
                device_id_type=MESH,
            )
            copy.start()
            h_copies.append(copy)
    slope = up * sigmoid * (1.0 + gate * (1.0 - sigmoid))
    loads[4].wait()

    def p1_copy(o):
        return pltpu.make_async_remote_copy(
            src_ref=p1_send.at[o, 1 - core],
            dst_ref=p1_buf.at[o],
            send_sem=p1_ssem.at[o],
            recv_sem=p1_rsem.at[o],
            device_id=partner,
            device_id_type=MESH,
        )

    def store_terms(o, value):
        for d in range(n_dp):
            block = value[d * row_block : (d + 1) * row_block]
            acc[o, d % 2, d // 2] = block
            p1_send[o, d % 2, d // 2] = block.astype(BF16)

    p1_copies, p2_copies = {}, {}

    def start_p1(o, value):
        store_terms(o, value)
        p1_copies[o] = p1_copy(o)
        p1_copies[o].start()

    def start_p2(o):
        p1_copies[o].wait_recv()
        for k in range(chips - 1, 0, -1):
            q = flipped(chip, k)
            p2_send[o, q] = (acc[o, core, q] + p1_buf[o, q].astype(F32)).astype(BF16)
            copy = pltpu.make_async_remote_copy(
                src_ref=p2_send.at[o, q],
                dst_ref=p2_buf.at[o, k - 1],
                send_sem=p2_ssem.at[o, k - 1],
                recv_sem=p2_rsem.at[o, k - 1],
                device_id=chip_at(k),
                device_id_type=MESH,
            )
            copy.start()
            p2_copies[o, k] = copy

    for k in range(1, n_exp):
        a_copies[k].wait_recv()
    scaled = a_buf[...].reshape(rows, width)
    if gather:
        for k in range(n_dp - 1, 0, -1):
            peer = flipped(replica, k)
            columns = pl.ds(pl.multiple_of(peer * row_block, row_block), row_block)
            copy = pltpu.make_async_remote_copy(
                src_ref=a_buf.at[:, :, columns],
                dst_ref=s_all.at[replica],
                send_sem=s_ssem.at[k - 1],
                recv_sem=s_rsem.at[k - 1],
                device_id={"dp": peer},
                device_id_type=MESH,
            )
            copy.start()
            s_copies.append(copy)
    else:
        start_p1(0, dot(scaled, hidden, 0, 0))
    dhidden = dot(scaled, wd_v[...], 1, 1)
    d_gate = (dhidden * slope).astype(BF16)
    d_up = (dhidden * activated).astype(BF16)
    returning = (dot(d_gate, wg_v[...], 1, 1) + dot(d_up, wu_v[...], 1, 1)).astype(BF16)
    for h in range(n_exp):
        r_send[h] = returning[h * part : (h + 1) * part]
    r_copies = []
    for k in range(n_exp - 1, 0, -1):
        copy = pltpu.make_async_remote_copy(
            src_ref=r_send.at[member_at(k)],
            dst_ref=r_buf.at[member],
            send_sem=r_ssem.at[k - 1],
            recv_sem=r_rsem.at[k - 1],
            device_id={"expert": member_at(k)},
            device_id_type=MESH,
        )
        copy.start()
        r_copies.append(copy)
    start_p1(1, dot(inputs, d_gate, 0, 0))
    start_p1(2, dot(inputs, d_up, 0, 0))
    if not gather:
        start_p2(0)
    r_buf[member] = r_send[member]
    start_p2(1)
    start_p2(2)

    if gather:
        own = pl.ds(pl.multiple_of(replica * row_block, row_block), row_block)
        s_all[replica] = a_buf[:, :, own]
        for copy in h_copies + s_copies:
            copy.wait_recv()
        slots = n_dp * rows
        down = dot(
            s_all[...].reshape(slots, row_block), h_all[...].reshape(slots, wg_v.shape[1]), 0, 0
        )
        gd_ref[...] = down * (1.0 / (micro * n_dp))
    for copy in r_copies:
        copy.wait_recv()
    gin_ref[...] = dot(mixing, r_buf[...].reshape(rows, width), 0, 0).astype(BF16)

    factor = 1.0 / (micro * n_dp)
    for o, out in enumerate((gd_ref, gg_ref, gu_ref)):
        if o not in p1_copies:
            continue
        total = acc[o, core, chip] + p1_buf[o, chip].astype(F32)
        for k in range(chips - 1, 0, -1):
            p2_copies[o, k].wait_recv()
            total = total + p2_buf[o, k - 1].astype(F32)
        out[...] = total * factor
    started = [*a_copies.values(), *p1_copies.values(), *p2_copies.values()]
    for copy in started + r_copies + h_copies + s_copies:
        copy.wait_send()


def pooled_kernel(
    micro,
    n_exp,
    n_dp,
    routes_hbm,
    probs_hbm,
    go_hbm,
    x_hbm,
    wg_hbm,
    wu_hbm,
    wd_hbm,
    gin_ref,
    gg_ref,
    gu_ref,
    gd_ref,
    routes_v,
    probs_v,
    go_v,
    x_v,
    x_par,
    xt_v,
    wg_v,
    wu_v,
    wd_v,
    a_send,
    a_buf,
    r_send,
    r_buf,
    mix_v,
    d_all,
    relay_buf,
    last_send,
    last_buf,
    sums_send,
    s_all,
    h_all,
    down_v,
    down_buf,
    sized,
    load_sem,
    sent_sem,
    a_sem,
    r_sem,
    x_sem,
    d_sem,
    relay_sem,
    last_sem,
    slot_sem,
    down_sem,
    turn_sem,
):
    member = lax.axis_index("expert")
    replica = lax.axis_index("dp")
    core = lax.rem(replica, 2)
    chip = lax.div(replica, 2)
    chips = n_dp // 2
    partner = {"dp": chip * 2 + 1 - core}
    window = n_exp // 2
    tokens, width = go_v.shape
    cols = wg_v.shape[1]
    tok_dev = tokens // micro
    part = micro * CAPS
    rows = n_exp * part
    row_block = width // n_dp
    pair_block = 2 * row_block
    hops = range(chips - 1, 0, -1)

    def chip_at(k):
        return flipped(chip, k)

    def peer_at(k, side=core):
        return {"dp": chip_at(k) * 2 + side}

    loads = [
        pltpu.make_async_copy(src, dst, load_sem.at[min(i, 3)])
        for i, (src, dst) in enumerate(
            (
                (routes_hbm, routes_v),
                (probs_hbm, probs_v),
                (go_hbm, go_v),
                *((x_hbm.at[m], x_v.at[:, pl.ds(m * CAPS, CAPS), :]) for m in range(micro)),
                (wg_hbm, wg_v),
                (wu_hbm, wu_v),
                (wd_hbm, wd_v),
            )
        )
    ]
    for load in loads[:3]:
        load.start()

    barrier = pltpu.get_barrier_semaphore()
    for k in range(n_exp - 1, 0, -1):
        pl.semaphore_signal(
            barrier, inc=1, device_id={"expert": flipped(member, k)}, device_id_type=MESH
        )
    for k in hops:
        pl.semaphore_signal(barrier, inc=1, device_id=peer_at(k), device_id_type=MESH)
    pl.semaphore_signal(barrier, inc=1, device_id=partner, device_id_type=MESH)
    for k in (1, 2):
        pl.semaphore_signal(barrier, inc=1, device_id=peer_at(k, 1 - core), device_id_type=MESH)

    def arrivals(size, sem):
        return pltpu.make_async_copy(sized.at[pl.ds(0, size)], sized.at[pl.ds(0, size)], sem)

    sent = []

    def remote(src, dst, sem, device, counted=True, group=0):
        copy = pltpu.make_async_remote_copy(
            src_ref=src,
            dst_ref=dst,
            send_sem=sent_sem.at[group],
            recv_sem=sem,
            device_id=device,
            device_id_type=MESH,
        )
        copy.start()
        if counted:
            bulk = 1
            for n in src.shape:
                bulk *= n
            sent.append(bulk * (2 if src.dtype == F32 else 1))

    pad = max(window, 8)
    expert_row = lax.broadcasted_iota(jnp.int32, (pad, tokens), 0)
    ti = lax.broadcasted_iota(jnp.int32, (tokens, tokens), 0)
    tj = lax.broadcasted_iota(jnp.int32, (tokens, tokens), 1)
    earlier = jnp.where((ti < tj) & (lax.div(ti, tok_dev) == lax.div(tj, tok_dev)), 1.0, 0.0)
    loads[0].wait()
    loads[1].wait()
    ids = jnp.concatenate([routes_v[m] for m in range(micro)], axis=1)
    probs = jnp.concatenate([probs_v[m].astype(F32) for m in range(micro)], axis=1)
    hits, weights = [], []
    table = jnp.zeros((pad, tokens), F32)
    for e in range(window):
        named = ids == e
        hits.append(jnp.sum(jnp.where(named, 1.0, 0.0), axis=0, keepdims=True))
        weights.append(jnp.sum(jnp.where(named, probs, 0.0), axis=0, keepdims=True))
        table = jnp.where(expert_row == e, hits[e], table)
    ranking = dot(table.astype(BF16), earlier.astype(BF16), 1, 0)
    slot = lax.broadcasted_iota(jnp.int32, (CAPS, tokens), 0).astype(F32)
    batch = lax.div(lax.broadcasted_iota(jnp.int32, (CAPS, tokens), 1), tok_dev)
    ones, scales = [], []
    for e in range(window):
        chosen = (hits[e] > 0.5) & (ranking[e : e + 1] == slot)
        for m in range(micro):
            here = chosen & (batch == m)
            ones.append(jnp.where(here, 1.0, 0.0))
            scales.append(jnp.where(here, weights[e], 0.0))
    picking = jnp.concatenate(scales, axis=0).astype(BF16)

    loads[2].wait()
    for load in loads[3:]:
        load.start()
    sending = dot(picking, go_v[...], 1, 0).astype(BF16)
    for e in range(window):
        a_send[e] = sending[e * part : (e + 1) * part]
    pl.semaphore_wait(barrier, n_exp - 1 + chips + 2)

    inner = jnp.where((member == 0) | (member == n_exp - 1), 0, 1)
    outer = (1 - inner) * (1 - core)
    order = [1 + inner + 2 * outer, 3 - 2 * outer, 2 - inner]
    arriving = [1, 3, 2]

    def member_at(k):
        low, high = lax.rem(k, 2), lax.div(k, 2)
        low = low * (1 - 2 * lax.rem(member, 2))
        high = high * (2 - 4 * lax.div(member, 2))
        return member + low + high

    for k in order:
        to = member_at(k)
        remote(a_send.at[lax.div(to, 2)], a_buf.at[member], a_sem.at[k - 1], {"expert": to})
    a_buf[member] = a_send[lax.div(member, 2)]

    weights_rows = width * cols // width
    arrivals(rows + 3 * weights_rows, load_sem.at[3]).wait()
    remote(x_v, x_par, x_sem.at[0], partner)
    inputs = x_v[...].reshape(rows, width)
    gate = dot(inputs, wg_v[...], 1, 0)
    up = dot(inputs, wu_v[...], 1, 0)
    sigmoid = jax.nn.sigmoid(gate)
    activated = gate * sigmoid
    h_all[chip] = (activated * up).astype(BF16)
    for k in hops:
        remote(h_all.at[chip], h_all.at[chip], slot_sem.at[0], peer_at(k))
    slope = up * sigmoid * (1.0 + gate * (1.0 - sigmoid))

    def blocks(q):
        return pl.ds(pl.multiple_of(q * pair_block, pair_block), pair_block)

    def send_slices(source, counted=True):
        for k in hops:
            remote(
                a_buf.at[source, :, blocks(chip_at(k))],
                s_all.at[chip, source],
                slot_sem.at[0],
                peer_at(k),
                counted,
            )

    send_slices(member)

    mix_v[...] = jnp.concatenate(
        [
            jnp.concatenate(ones[e * micro : (e + 1) * micro], axis=0)
            for e in range(window)
            for _ in range(2)
        ],
        axis=0,
    ).astype(BF16)
    pltpu.make_async_copy(x_par, x_par, x_sem.at[0]).wait()
    for j in range(chips + 2):
        k, side = (j, core) if j < chips else (j - chips + 1, 0)
        q = chip_at(k) if k else chip
        own = pl.ds(pl.multiple_of((q * 2 + side) * row_block, row_block), row_block)
        mine = x_v[:, :, own].reshape(rows, row_block)
        other = x_par[:, :, own].reshape(rows, row_block)
        xt_v[j] = jnp.concatenate([mine, other], axis=0).T

    for j, k in enumerate(arriving):
        source = member_at(k)
        pltpu.make_async_copy(a_buf.at[source], a_buf.at[source], a_sem.at[k - 1]).wait()
        if j < n_exp - 2:
            send_slices(source)
    scaled = a_buf[...].reshape(rows, width)
    dhidden = dot(scaled, wd_v[...], 1, 1)
    d_all[0, :, :cols] = (dhidden * slope).astype(BF16)
    d_all[0, :, cols:] = (dhidden * activated).astype(BF16)
    remote(d_all.at[0], d_all.at[1], d_sem.at[0], partner)

    @pl.when(core == 1)
    def _():
        send_slices(member_at(arriving[-1]), False)

    sent.append((chips - 1) * part * pair_block)

    def send_rows(to):
        remote(r_send.at[to], r_buf.at[member], r_sem.at[0], {"expert": to}, False)

    def send_back():
        returning = dot(d_all[0, :, :cols], wg_v[...], 1, 1) + dot(
            d_all[0, :, cols:], wu_v[...], 1, 1
        )
        returning = returning.astype(BF16)
        for h in range(n_exp):
            r_send[h] = returning[h * part : (h + 1) * part]
        for k in (3 - inner, 1):
            send_rows(member_at(k))

        @pl.when(core == 0)
        def _():
            send_rows(member_at(2 + inner))


    sent.append((n_exp - 1) * part * width)
    returns_first = (core == 1) | (member != 0)

    @pl.when(returns_first)
    def _():
        send_back()

    pltpu.make_async_copy(d_all.at[1], d_all.at[1], d_sem.at[0]).wait()
    factors = d_all[...].reshape(2 * rows, 2 * cols)
    half = row_block // 2
    strips = [pl.ds(c * half, half) for c in range(2)]
    far = dot(xt_v[3], factors, 1, 0)
    for i in range(2):
        last_send[4 + i] = far[:, i * cols : (i + 1) * cols].astype(BF16)
    for c, strip in enumerate(strips):
        for i in range(2):
            remote(
                last_send.at[4 + i, strip],
                relay_buf.at[1 - core, i, strip],
                relay_sem.at[1 - core, c],
                peer_at(1 + i, 1),
            )

    @pl.when(core == 1)
    def _():
        pl.semaphore_signal(turn_sem, inc=1, device_id=partner, device_id_type=MESH)

    near = [dot(xt_v[k], factors, 1, 0) for k in (1, 2)]
    last_send[0] = near[0][:, :cols].astype(BF16)
    last_send[1] = near[1][:, cols:].astype(BF16)
    total = dot(xt_v[0], factors, 1, 0)
    @pl.when(jnp.logical_not(returns_first))
    def _():
        send_back()

    r_buf[member] = r_send[member]
    s_all[chip] = a_buf[:, :, blocks(chip)]

    @pl.when(core == 0)
    def _():
        pl.semaphore_wait(turn_sem, 1)


    @pl.when(core == 0)
    def _():
        send_slices(member_at(arriving[-1]), False)

    for i in range(2):
        remote(last_send.at[i], last_buf.at[i], last_sem.at[0], peer_at(1 + i))
    @pl.when(core == 1)
    def _():
        extra = [
            dot(xt_v[chips + 1], factors[:, :cols], 1, 0),
            dot(xt_v[chips], factors[:, cols:], 1, 0),
        ]
        terms = [[near[1][:, :cols], near[0][:, cols:]], extra]
        for side in (1, 0):
            for c, strip in enumerate(strips):
                arrivals(2 * half * cols // width, relay_sem.at[side, c]).wait()
                if side == 1 and c == 0:
                    send_rows(member_at(2 + inner))
                for i in range(2):
                    value = terms[side][i][c * half : (c + 1) * half]
                    value = value + relay_buf[side, i, strip].astype(F32)
                    sums_send[side, i, strip] = value.astype(BF16)
                    remote(
                        sums_send.at[side, i, strip],
                        last_buf.at[2 + i, strip],
                        last_sem.at[1],
                        peer_at(2 - i, 1 - side),
                        False,
                        1,
                    )
    others = (chips - 1) * (rows * cols + rows * pair_block)
    arrivals(others // width, slot_sem.at[0]).wait()
    slots = chips * rows
    down = dot(s_all[...].reshape(slots, pair_block), h_all[...].reshape(slots, cols), 0, 0)
    down_v[0] = down[:row_block]
    down_v[1] = down[row_block:]
    remote(down_v.at[1 - core], down_buf, down_sem.at[0], partner)

    arrivals((n_exp - 1) * part, r_sem.at[0]).wait()
    gin_ref[...] = dot(mix_v[...], r_buf[...].reshape(rows, width), 0, 0).astype(BF16)

    factor = 1.0 / (micro * n_dp)
    pltpu.make_async_copy(down_buf, down_buf, down_sem.at[0]).wait()
    gd_ref[...] = (down_v[core] + down_buf[...]) * factor
    halves = 2 * row_block * cols // width
    arrivals(halves, last_sem.at[0]).wait()
    gg_ref[...] = (total[:, :cols] + last_buf[0].astype(F32)) * factor
    gu_ref[...] = (total[:, cols:] + last_buf[1].astype(F32)) * factor
    arrivals(halves, last_sem.at[1]).wait()
    gg_ref[...] = gg_ref[...] + last_buf[2].astype(F32) * factor
    gu_ref[...] = gu_ref[...] + last_buf[3].astype(F32) * factor

    @pl.when(core == 1)
    def _():
        arrivals(4 * row_block * cols // width, sent_sem.at[1]).wait()

    arrivals(sum(sent) // width, sent_sem.at[0]).wait()


def settle(*refs):
    count = len(refs) // 2 - 1
    sized, sem = refs[-2:]
    for i in range(count):
        pltpu.make_async_copy(refs[i], refs[count + i], sem.at[0]).start()
    pltpu.make_async_copy(sized, sized, sem.at[0]).wait()


def settled(arrays):
    anywhere = pl.BlockSpec(memory_space=pl.ANY)
    words = sum(a.size * a.dtype.itemsize // 2 for a in arrays)
    return pl.pallas_call(
        settle,
        out_shape=tuple(jax.ShapeDtypeStruct(a.shape, a.dtype) for a in arrays),
        in_specs=[pl.BlockSpec(memory_space=pltpu.VMEM)] * len(arrays),
        out_specs=(anywhere,) * len(arrays),
        scratch_shapes=[
            pltpu.VMEM((words // arrays[0].shape[1], arrays[0].shape[1]), BF16),
            pltpu.SemaphoreType.DMA((1,)),
        ],
    )(*[pltpu.with_memory_space_constraint(a, pltpu.VMEM) for a in arrays])


def pooled_call(n_exp, n_dp, grad_out, routes, route_probs, dispatched, w_gate, w_up, w_down):
    micro, tok_dev, width = grad_out.shape
    cols = w_gate.shape[1]
    tokens = micro * tok_dev
    part = micro * CAPS
    rows = n_exp * part
    chips = n_dp // 2
    row_block = width // n_dp
    vmem = pl.BlockSpec(memory_space=pltpu.VMEM)
    hbm = pl.BlockSpec(memory_space=pl.ANY)
    grad = pltpu.VMEM((row_block, cols), F32)
    dma = pltpu.SemaphoreType.DMA
    return pl.pallas_call(
        functools.partial(pooled_kernel, micro, n_exp, n_dp),
        out_shape=(pltpu.VMEM((tokens, width), BF16), grad, grad, grad),
        in_specs=[hbm] * 7,
        out_specs=(vmem, vmem, vmem, vmem),
        scratch_shapes=[
            pltpu.VMEM((micro, routes.shape[2], tok_dev), jnp.int32),
            pltpu.VMEM((micro, routes.shape[2], tok_dev), BF16),
            pltpu.VMEM((tokens, width), BF16),
            pltpu.VMEM((n_exp, part, width), BF16),
            pltpu.VMEM((n_exp, part, width), BF16),
            pltpu.VMEM((chips + 2, row_block, 2 * rows), BF16),
            pltpu.VMEM((width, cols), BF16),
            pltpu.VMEM((width, cols), BF16),
            pltpu.VMEM((cols, width), BF16),
            pltpu.VMEM((n_exp // 2, part, width), BF16),
            pltpu.VMEM((n_exp, part, width), BF16),
            pltpu.VMEM((n_exp, part, width), BF16),
            pltpu.VMEM((n_exp, part, width), BF16),
            pltpu.VMEM((rows, tokens), BF16),
            pltpu.VMEM((2, rows, 2 * cols), BF16),
            pltpu.VMEM((2, 2, row_block, cols), BF16),
            pltpu.VMEM((6, row_block, cols), BF16),
            pltpu.VMEM((4, row_block, cols), BF16),
            pltpu.VMEM((2, 2, row_block, cols), BF16),
            pltpu.VMEM((chips, n_exp, part, 2 * row_block), BF16),
            pltpu.VMEM((chips, rows, cols), BF16),
            pltpu.VMEM((2, row_block, cols), F32),
            pltpu.VMEM((row_block, cols), F32),
            pltpu.VMEM((width, width), BF16),
            dma((4,)),
            dma((2,)),
            dma((n_exp - 1,)),
            dma((1,)),
            dma((1,)),
            dma((1,)),
            dma((2, 2)),
            dma((2,)),
            dma((1,)),
            dma((1,)),
            pltpu.SemaphoreType.REGULAR,
        ],
        compiler_params=pltpu.CompilerParams(collective_id=0, has_side_effects=True),
    )(
        routes.transpose(0, 2, 1),
        route_probs.transpose(0, 2, 1),
        grad_out.reshape(tokens, width),
        dispatched.reshape(micro, n_exp, CAPS, width),
        w_gate,
        w_up,
        w_down,
    )


def spread_call(n_exp, n_dp, grad_out, routes, route_probs, dispatched, w_gate, w_up, w_down):
    micro, tok_dev, width = grad_out.shape
    cols = w_gate.shape[1]
    tokens = micro * tok_dev
    part = micro * CAPS
    rows = n_exp * part
    chips = n_dp // 2
    row_block = width // n_dp
    vmem = pl.BlockSpec(memory_space=pltpu.VMEM)
    hbm = pl.BlockSpec(memory_space=pl.ANY)
    grad = pltpu.VMEM((row_block, cols), F32)
    dma = pltpu.SemaphoreType.DMA
    others = max(chips - 1, 1)
    gather = row_block % 128 == 0
    return pl.pallas_call(
        functools.partial(kernel, micro, n_exp, n_dp),
        out_shape=(pltpu.VMEM((tokens, width), BF16), grad, grad, grad),
        in_specs=[vmem, vmem, hbm, hbm, hbm, hbm, hbm],
        out_specs=(vmem, vmem, vmem, vmem),
        scratch_shapes=[
            pltpu.VMEM((tokens, width), BF16),
            pltpu.VMEM((rows, width), BF16),
            pltpu.VMEM((width, cols), BF16),
            pltpu.VMEM((width, cols), BF16),
            pltpu.VMEM((cols, width), BF16),
            pltpu.VMEM((n_exp, part, width), BF16),
            pltpu.VMEM((n_exp, part, width), BF16),
            pltpu.VMEM((n_exp, part, width), BF16),
            pltpu.VMEM((n_exp, part, width), BF16),
            pltpu.VMEM((3, 2, chips, row_block, cols), F32),
            pltpu.VMEM((3, 2, chips, row_block, cols), BF16),
            pltpu.VMEM((3, chips, row_block, cols), BF16),
            pltpu.VMEM((3, chips, row_block, cols), BF16),
            pltpu.VMEM((3, others, row_block, cols), BF16),
            pltpu.VMEM((n_dp, n_exp, part, row_block) if gather else (8, 128), BF16),
            pltpu.VMEM((n_dp, rows, cols) if gather else (8, 128), BF16),
            dma((5,)),
            dma((n_exp - 1,)),
            dma((n_exp - 1,)),
            dma((n_exp - 1,)),
            dma((n_exp - 1,)),
            dma((3,)),
            dma((3,)),
            dma((3, others)),
            dma((3, others)),
            dma((n_dp - 1,)),
            dma((n_dp - 1,)),
            dma((n_dp - 1,)),
            dma((n_dp - 1,)),
        ],
        compiler_params=pltpu.CompilerParams(collective_id=0, has_side_effects=True),
    )(
        routes.transpose(0, 2, 1),
        route_probs.transpose(0, 2, 1),
        grad_out.reshape(tokens, width),
        dispatched.reshape(rows, width),
        w_gate,
        w_up,
        w_down,
    )


def per_device(n_exp, n_dp, grad_out, *rest):
    pooled = n_exp == 4 and n_dp == 8 and (grad_out.shape[2] // n_dp) % 128 == 0
    call = pooled_call if pooled else spread_call
    out = settled(call(n_exp, n_dp, grad_out, *rest))
    return (out[0].reshape(grad_out.shape),) + tuple(out[1:])


def solution(mesh):
    return jax.shard_map(
        functools.partial(per_device, mesh.shape["expert"], mesh.shape["dp"]),
        mesh=mesh,
        in_specs=(
            P(None, ("dp", "expert"), None),
            P(None, ("dp", "expert"), None),
            P(None, ("dp", "expert"), None),
            P(None, ("dp", "expert"), None),
            P(None, "expert"),
            P(None, "expert"),
            P("expert", None),
        ),
        out_specs=(
            P(None, ("dp", "expert"), None),
            P("dp", "expert"),
            P("dp", "expert"),
            P("dp", "expert"),
        ),
        check_vma=False,
    )
```

```python
import functools

import jax
import jax.numpy as jnp
from jax import lax
from jax.experimental import pallas as pl
from jax.experimental.pallas import tpu as pltpu
from jax.sharding import PartitionSpec as P

CAPS = 8
MESH = pl.DeviceIdType.MESH
BF16 = jnp.bfloat16
F32 = jnp.float32


def dot(left, right, lc, rc):
    return lax.dot_general(
        left, right, (((lc,), (rc,)), ((), ())), preferred_element_type=F32
    )


def flipped(index, bits):
    step = 1
    while step <= bits:
        if bits & step:
            index = index + step - 2 * step * lax.rem(lax.div(index, step), 2)
        step *= 2
    return index


def kernel(
    micro,
    n_exp,
    n_dp,
    routes_ref,
    probs_ref,
    go_hbm,
    x_hbm,
    wg_hbm,
    wu_hbm,
    wd_hbm,
    gin_ref,
    gg_ref,
    gu_ref,
    gd_ref,
    go_v,
    x_v,
    wg_v,
    wu_v,
    wd_v,
    a_send,
    a_buf,
    r_send,
    r_buf,
    acc,
    p1_send,
    p1_buf,
    p2_send,
    p2_buf,
    s_all,
    h_all,
    load_sem,
    a_ssem,
    a_rsem,
    r_ssem,
    r_rsem,
    p1_ssem,
    p1_rsem,
    p2_ssem,
    p2_rsem,
    s_ssem,
    s_rsem,
    h_ssem,
    h_rsem,
):
    member = lax.axis_index("expert")
    replica = lax.axis_index("dp")
    core = lax.rem(replica, 2)
    chip = lax.div(replica, 2)
    chips = n_dp // 2
    partner = {"dp": chip * 2 + 1 - core}
    window = n_exp // 2
    tokens = go_v.shape[0]
    width = go_v.shape[1]
    tok_dev = tokens // micro
    part = micro * CAPS
    rows = n_exp * part
    row_block = width // n_dp
    gather = row_block % 128 == 0

    def member_at(k):
        return flipped(member, k)

    def chip_at(k):
        return {"dp": flipped(chip, k) * 2 + core}

    loads = [
        pltpu.make_async_copy(src, dst, load_sem.at[i])
        for i, (src, dst) in enumerate(
            ((go_hbm, go_v), (x_hbm, x_v), (wg_hbm, wg_v), (wu_hbm, wu_v), (wd_hbm, wd_v))
        )
    ]
    for load in loads:
        load.start()

    barrier = pltpu.get_barrier_semaphore()
    for k in range(1, n_exp):
        pl.semaphore_signal(
            barrier, inc=1, device_id={"expert": member_at(k)}, device_id_type=MESH
        )
    for k in range(1, n_dp):
        pl.semaphore_signal(
            barrier, inc=1, device_id={"dp": flipped(replica, k)}, device_id_type=MESH
        )

    ids = jnp.concatenate([routes_ref[m] for m in range(micro)], axis=1)
    probs = jnp.concatenate([probs_ref[m].astype(F32) for m in range(micro)], axis=1)
    pad = max(window, 8)
    expert_row = lax.broadcasted_iota(jnp.int32, (pad, tokens), 0)
    hits, weights = [], []
    table = jnp.zeros((pad, tokens), F32)
    for e in range(window):
        named = ids == e
        hits.append(jnp.sum(jnp.where(named, 1.0, 0.0), axis=0, keepdims=True))
        weights.append(jnp.sum(jnp.where(named, probs, 0.0), axis=0, keepdims=True))
        table = jnp.where(expert_row == e, hits[e], table)
    ti = lax.broadcasted_iota(jnp.int32, (tokens, tokens), 0)
    tj = lax.broadcasted_iota(jnp.int32, (tokens, tokens), 1)
    earlier = jnp.where((ti < tj) & (lax.div(ti, tok_dev) == lax.div(tj, tok_dev)), 1.0, 0.0)
    ranking = dot(table.astype(BF16), earlier.astype(BF16), 1, 0)
    slot = lax.broadcasted_iota(jnp.int32, (CAPS, tokens), 0).astype(F32)
    batch = lax.div(lax.broadcasted_iota(jnp.int32, (CAPS, tokens), 1), tok_dev)
    ones, scales = [], []
    for h in range(n_exp):
        e = h // 2
        chosen = (hits[e] > 0.5) & (ranking[e : e + 1] == slot)
        for m in range(micro):
            here = chosen & (batch == m)
            ones.append(jnp.where(here, 1.0, 0.0))
            scales.append(jnp.where(here, weights[e], 0.0))
    mixing = jnp.concatenate(ones, axis=0).astype(BF16)
    picking = jnp.concatenate(scales, axis=0).astype(BF16)

    loads[0].wait()
    sending = dot(picking, go_v[...], 1, 0).astype(BF16)
    for h in range(n_exp):
        a_send[h] = sending[h * part : (h + 1) * part]
    pl.semaphore_wait(barrier, n_exp - 1 + n_dp - 1)
    def a_copy(k, src, slot, to):
        return pltpu.make_async_remote_copy(
            src_ref=src,
            dst_ref=a_buf.at[slot],
            send_sem=a_ssem.at[k - 1],
            recv_sem=a_rsem.at[k - 1],
            device_id={"expert": to},
            device_id_type=MESH,
        )

    a_copies = {}
    for k in range(1, n_exp):
        a_copies[k] = a_copy(k, a_send.at[member_at(k)], member, member_at(k))
        a_copies[k].start()
    a_buf[member] = a_send[member]

    loads[1].wait()
    ri = lax.broadcasted_iota(jnp.int32, (rows, rows), 0)
    rj = lax.broadcasted_iota(jnp.int32, (rows, rows), 1)
    wanted = (
        lax.rem(lax.div(ri, CAPS), micro) * (n_exp * CAPS)
        + lax.div(ri, part) * CAPS
        + lax.rem(ri, CAPS)
    )
    inputs = dot(jnp.where(rj == wanted, 1.0, 0.0).astype(BF16), x_v[...], 1, 0).astype(BF16)
    loads[2].wait()
    gate = dot(inputs, wg_v[...], 1, 0)
    loads[3].wait()
    up = dot(inputs, wu_v[...], 1, 0)
    sigmoid = jax.nn.sigmoid(gate)
    activated = gate * sigmoid
    hidden = (activated * up).astype(BF16)
    h_copies, s_copies = [], []
    if gather:
        h_all[replica] = hidden
        for k in range(n_dp - 1, 0, -1):
            copy = pltpu.make_async_remote_copy(
                src_ref=h_all.at[replica],
                dst_ref=h_all.at[replica],
                send_sem=h_ssem.at[k - 1],
                recv_sem=h_rsem.at[k - 1],
                device_id={"dp": flipped(replica, k)},
                device_id_type=MESH,
            )
            copy.start()
            h_copies.append(copy)
    slope = up * sigmoid * (1.0 + gate * (1.0 - sigmoid))
    loads[4].wait()

    def p1_copy(o):
        return pltpu.make_async_remote_copy(
            src_ref=p1_send.at[o, 1 - core],
            dst_ref=p1_buf.at[o],
            send_sem=p1_ssem.at[o],
            recv_sem=p1_rsem.at[o],
            device_id=partner,
            device_id_type=MESH,
        )

    def store_terms(o, value):
        for d in range(n_dp):
            block = value[d * row_block : (d + 1) * row_block]
            acc[o, d % 2, d // 2] = block
            p1_send[o, d % 2, d // 2] = block.astype(BF16)

    p1_copies, p2_copies = {}, {}

    def start_p1(o, value):
        store_terms(o, value)
        p1_copies[o] = p1_copy(o)
        p1_copies[o].start()

    def start_p2(o):
        p1_copies[o].wait_recv()
        for k in range(chips - 1, 0, -1):
            q = flipped(chip, k)
            p2_send[o, q] = (acc[o, core, q] + p1_buf[o, q].astype(F32)).astype(BF16)
            copy = pltpu.make_async_remote_copy(
                src_ref=p2_send.at[o, q],
                dst_ref=p2_buf.at[o, k - 1],
                send_sem=p2_ssem.at[o, k - 1],
                recv_sem=p2_rsem.at[o, k - 1],
                device_id=chip_at(k),
                device_id_type=MESH,
            )
            copy.start()
            p2_copies[o, k] = copy

    for k in range(1, n_exp):
        a_copies[k].wait_recv()
    scaled = a_buf[...].reshape(rows, width)
    if gather:
        for k in range(n_dp - 1, 0, -1):
            peer = flipped(replica, k)
            columns = pl.ds(pl.multiple_of(peer * row_block, row_block), row_block)
            copy = pltpu.make_async_remote_copy(
                src_ref=a_buf.at[:, :, columns],
                dst_ref=s_all.at[replica],
                send_sem=s_ssem.at[k - 1],
                recv_sem=s_rsem.at[k - 1],
                device_id={"dp": peer},
                device_id_type=MESH,
            )
            copy.start()
            s_copies.append(copy)
    else:
        start_p1(0, dot(scaled, hidden, 0, 0))
    dhidden = dot(scaled, wd_v[...], 1, 1)
    d_gate = (dhidden * slope).astype(BF16)
    d_up = (dhidden * activated).astype(BF16)
    returning = (dot(d_gate, wg_v[...], 1, 1) + dot(d_up, wu_v[...], 1, 1)).astype(BF16)
    for h in range(n_exp):
        r_send[h] = returning[h * part : (h + 1) * part]
    r_copies = []
    for k in range(n_exp - 1, 0, -1):
        copy = pltpu.make_async_remote_copy(
            src_ref=r_send.at[member_at(k)],
            dst_ref=r_buf.at[member],
            send_sem=r_ssem.at[k - 1],
            recv_sem=r_rsem.at[k - 1],
            device_id={"expert": member_at(k)},
            device_id_type=MESH,
        )
        copy.start()
        r_copies.append(copy)
    start_p1(1, dot(inputs, d_gate, 0, 0))
    start_p1(2, dot(inputs, d_up, 0, 0))
    if not gather:
        start_p2(0)
    r_buf[member] = r_send[member]
    start_p2(1)
    start_p2(2)

    if gather:
        own = pl.ds(pl.multiple_of(replica * row_block, row_block), row_block)
        s_all[replica] = a_buf[:, :, own]
        for copy in h_copies + s_copies:
            copy.wait_recv()
        slots = n_dp * rows
        down = dot(
            s_all[...].reshape(slots, row_block), h_all[...].reshape(slots, wg_v.shape[1]), 0, 0
        )
        gd_ref[...] = down * (1.0 / (micro * n_dp))
    for copy in r_copies:
        copy.wait_recv()
    gin_ref[...] = dot(mixing, r_buf[...].reshape(rows, width), 0, 0).astype(BF16)

    factor = 1.0 / (micro * n_dp)
    for o, out in enumerate((gd_ref, gg_ref, gu_ref)):
        if o not in p1_copies:
            continue
        total = acc[o, core, chip] + p1_buf[o, chip].astype(F32)
        for k in range(chips - 1, 0, -1):
            p2_copies[o, k].wait_recv()
            total = total + p2_buf[o, k - 1].astype(F32)
        out[...] = total * factor
    started = [*a_copies.values(), *p1_copies.values(), *p2_copies.values()]
    for copy in started + r_copies + h_copies + s_copies:
        copy.wait_send()


def pooled_kernel(
    micro,
    n_exp,
    n_dp,
    routes_hbm,
    probs_hbm,
    go_hbm,
    x_hbm,
    wg_hbm,
    wu_hbm,
    wd_hbm,
    gin_ref,
    gg_ref,
    gu_ref,
    gd_ref,
    routes_v,
    probs_v,
    go_v,
    x_v,
    x_par,
    xt_v,
    wg_v,
    wu_v,
    wd_v,
    wdt_v,
    wgt_v,
    a_send,
    a_buf,
    r_send,
    r_buf,
    mix_v,
    d_all,
    relay_buf,
    last_send,
    last_buf,
    sums_send,
    s_all,
    h_all,
    down_v,
    down_buf,
    sized,
    load_sem,
    sent_sem,
    a_sem,
    r_sem,
    x_sem,
    d_sem,
    relay_sem,
    last_sem,
    slot_sem,
    down_sem,
    turn_sem,
):
    member = lax.axis_index("expert")
    replica = lax.axis_index("dp")
    core = lax.rem(replica, 2)
    chip = lax.div(replica, 2)
    chips = n_dp // 2
    partner = {"dp": chip * 2 + 1 - core}
    window = n_exp // 2
    tokens, width = go_v.shape
    cols = wg_v.shape[1]
    tok_dev = tokens // micro
    part = micro * CAPS
    rows = n_exp * part
    row_block = width // n_dp
    pair_block = 2 * row_block
    hops = range(chips - 1, 0, -1)

    def chip_at(k):
        return flipped(chip, k)

    def peer_at(k, side=core):
        return {"dp": chip_at(k) * 2 + side}

    loads = [
        pltpu.make_async_copy(src, dst, load_sem.at[min(i, 3)])
        for i, (src, dst) in enumerate(
            (
                (routes_hbm, routes_v),
                (probs_hbm, probs_v),
                (go_hbm, go_v),
                *((x_hbm.at[m], x_v.at[:, pl.ds(m * CAPS, CAPS), :]) for m in range(micro)),
                (wg_hbm, wg_v),
                (wu_hbm, wu_v),
                (wd_hbm, wd_v),
            )
        )
    ]
    for load in loads[:3]:
        load.start()

    barrier = pltpu.get_barrier_semaphore()
    for k in range(n_exp - 1, 0, -1):
        pl.semaphore_signal(
            barrier, inc=1, device_id={"expert": flipped(member, k)}, device_id_type=MESH
        )
    for k in hops:
        pl.semaphore_signal(barrier, inc=1, device_id=peer_at(k), device_id_type=MESH)
    pl.semaphore_signal(barrier, inc=1, device_id=partner, device_id_type=MESH)
    for k in (1, 2):
        pl.semaphore_signal(barrier, inc=1, device_id=peer_at(k, 1 - core), device_id_type=MESH)

    def arrivals(size, sem):
        return pltpu.make_async_copy(sized.at[pl.ds(0, size)], sized.at[pl.ds(0, size)], sem)

    sent = []

    def remote(src, dst, sem, device, counted=True, group=0):
        copy = pltpu.make_async_remote_copy(
            src_ref=src,
            dst_ref=dst,
            send_sem=sent_sem.at[group],
            recv_sem=sem,
            device_id=device,
            device_id_type=MESH,
        )
        copy.start()
        if counted:
            bulk = 1
            for n in src.shape:
                bulk *= n
            sent.append(bulk * (2 if src.dtype == F32 else 1))

    pad = max(window, 8)
    expert_row = lax.broadcasted_iota(jnp.int32, (pad, tokens), 0)
    ti = lax.broadcasted_iota(jnp.int32, (tokens, tokens), 0)
    tj = lax.broadcasted_iota(jnp.int32, (tokens, tokens), 1)
    earlier = jnp.where((ti < tj) & (lax.div(ti, tok_dev) == lax.div(tj, tok_dev)), 1.0, 0.0)
    loads[0].wait()
    loads[1].wait()
    ids = jnp.concatenate([routes_v[m] for m in range(micro)], axis=1)
    probs = jnp.concatenate([probs_v[m].astype(F32) for m in range(micro)], axis=1)
    hits, weights = [], []
    table = jnp.zeros((pad, tokens), F32)
    for e in range(window):
        named = ids == e
        hits.append(jnp.sum(jnp.where(named, 1.0, 0.0), axis=0, keepdims=True))
        weights.append(jnp.sum(jnp.where(named, probs, 0.0), axis=0, keepdims=True))
        table = jnp.where(expert_row == e, hits[e], table)
    ranking = dot(table.astype(BF16), earlier.astype(BF16), 1, 0)
    slot = lax.broadcasted_iota(jnp.int32, (CAPS, tokens), 0).astype(F32)
    batch = lax.div(lax.broadcasted_iota(jnp.int32, (CAPS, tokens), 1), tok_dev)
    ones, scales = [], []
    for e in range(window):
        chosen = (hits[e] > 0.5) & (ranking[e : e + 1] == slot)
        for m in range(micro):
            here = chosen & (batch == m)
            ones.append(jnp.where(here, 1.0, 0.0))
            scales.append(jnp.where(here, weights[e], 0.0))
    picking = jnp.concatenate(scales, axis=0).astype(BF16)

    loads[2].wait()
    for load in loads[3:]:
        load.start()
    sending = dot(picking, go_v[...], 1, 0).astype(BF16)
    for e in range(window):
        a_send[e] = sending[e * part : (e + 1) * part]
    pl.semaphore_wait(barrier, n_exp - 1 + chips + 2)

    inner = jnp.where((member == 0) | (member == n_exp - 1), 0, 1)
    outer = (1 - inner) * (1 - core)
    order = [1 + inner + 2 * outer, 3 - 2 * outer, 2 - inner]
    arriving = [1, 3, 2]

    def member_at(k):
        low, high = lax.rem(k, 2), lax.div(k, 2)
        low = low * (1 - 2 * lax.rem(member, 2))
        high = high * (2 - 4 * lax.div(member, 2))
        return member + low + high

    for k in order:
        to = member_at(k)
        remote(a_send.at[lax.div(to, 2)], a_buf.at[member], a_sem.at[k - 1], {"expert": to})
    a_buf[member] = a_send[lax.div(member, 2)]

    weights_rows = width * cols // width
    arrivals(rows + 3 * weights_rows, load_sem.at[3]).wait()
    remote(x_v, x_par, x_sem.at[0], partner)
    inputs = x_v[...].reshape(rows, width)
    gate = dot(inputs, wg_v[...], 1, 0)
    up = dot(inputs, wu_v[...], 1, 0)
    sigmoid = jax.nn.sigmoid(gate)
    activated = gate * sigmoid
    h_all[chip] = (activated * up).astype(BF16)
    for k in hops:
        remote(h_all.at[chip], h_all.at[chip], slot_sem.at[0], peer_at(k))
    slope = up * sigmoid * (1.0 + gate * (1.0 - sigmoid))

    def blocks(q):
        return pl.ds(pl.multiple_of(q * pair_block, pair_block), pair_block)

    def send_slices(source, counted=True):
        for k in hops:
            remote(
                a_buf.at[source, :, blocks(chip_at(k))],
                s_all.at[chip, source],
                slot_sem.at[0],
                peer_at(k),
                counted,
            )

    send_slices(member)

    mix_v[...] = jnp.concatenate(
        [
            jnp.concatenate(ones[e * micro : (e + 1) * micro], axis=0)
            for e in range(window)
            for _ in range(2)
        ],
        axis=0,
    ).astype(BF16)
    wdt_v[...] = wd_v[...].T
    wgt_v[:cols] = wg_v[...].T
    wgt_v[cols:] = wu_v[...].T
    pltpu.make_async_copy(x_par, x_par, x_sem.at[0]).wait()
    for j in range(chips + 2):
        k, side = (j, core) if j < chips else (j - chips + 1, 0)
        q = chip_at(k) if k else chip
        own = pl.ds(pl.multiple_of((q * 2 + side) * row_block, row_block), row_block)
        mine = x_v[:, :, own].reshape(rows, row_block)
        other = x_par[:, :, own].reshape(rows, row_block)
        xt_v[j] = jnp.concatenate([mine, other], axis=0).T

    for j, k in enumerate(arriving):
        source = member_at(k)
        pltpu.make_async_copy(a_buf.at[source], a_buf.at[source], a_sem.at[k - 1]).wait()
        if j < n_exp - 2:
            send_slices(source)
    scaled = a_buf[...].reshape(rows, width)
    dhidden = dot(scaled, wdt_v[...], 1, 0)
    d_all[0, :, :cols] = (dhidden * slope).astype(BF16)
    d_all[0, :, cols:] = (dhidden * activated).astype(BF16)
    remote(d_all.at[0], d_all.at[1], d_sem.at[0], partner)

    @pl.when(core == 1)
    def _():
        send_slices(member_at(arriving[-1]), False)

    sent.append((chips - 1) * part * pair_block)

    def send_rows(to):
        remote(r_send.at[to], r_buf.at[member], r_sem.at[0], {"expert": to}, False)

    def send_back():
        returning = dot(d_all[0], wgt_v[...], 1, 0)
        returning = returning.astype(BF16)
        for h in range(n_exp):
            r_send[h] = returning[h * part : (h + 1) * part]
        for k in (3 - inner, 1):
            send_rows(member_at(k))

        @pl.when(core == 0)
        def _():
            send_rows(member_at(2 + inner))


    sent.append((n_exp - 1) * part * width)
    returns_first = (core == 1) | (member != 0)

    @pl.when(returns_first)
    def _():
        send_back()

    pltpu.make_async_copy(d_all.at[1], d_all.at[1], d_sem.at[0]).wait()
    factors = d_all[...].reshape(2 * rows, 2 * cols)
    half = row_block // 2
    strips = [pl.ds(c * half, half) for c in range(2)]
    far = dot(xt_v[3], factors, 1, 0)
    for i in range(2):
        last_send[4 + i] = far[:, i * cols : (i + 1) * cols].astype(BF16)
    for c, strip in enumerate(strips):
        for i in range(2):
            remote(
                last_send.at[4 + i, strip],
                relay_buf.at[1 - core, i, strip],
                relay_sem.at[1 - core, c],
                peer_at(1 + i, 1),
            )

    @pl.when(core == 1)
    def _():
        pl.semaphore_signal(turn_sem, inc=1, device_id=partner, device_id_type=MESH)

    near = [dot(xt_v[k], factors, 1, 0) for k in (1, 2)]
    last_send[0] = near[0][:, :cols].astype(BF16)
    last_send[1] = near[1][:, cols:].astype(BF16)
    total = dot(xt_v[0], factors, 1, 0)
    @pl.when(jnp.logical_not(returns_first))
    def _():
        send_back()

    r_buf[member] = r_send[member]
    s_all[chip] = a_buf[:, :, blocks(chip)]

    @pl.when(core == 0)
    def _():
        pl.semaphore_wait(turn_sem, 1)


    @pl.when(core == 0)
    def _():
        send_slices(member_at(arriving[-1]), False)

    for i in range(2):
        remote(last_send.at[i], last_buf.at[i], last_sem.at[0], peer_at(1 + i))
    @pl.when(core == 1)
    def _():
        extra = [
            dot(xt_v[chips + 1], factors[:, :cols], 1, 0),
            dot(xt_v[chips], factors[:, cols:], 1, 0),
        ]
        terms = [[near[1][:, :cols], near[0][:, cols:]], extra]
        for side in (1, 0):
            for c, strip in enumerate(strips):
                arrivals(2 * half * cols // width, relay_sem.at[side, c]).wait()
                if side == 1 and c == 0:
                    send_rows(member_at(2 + inner))
                for i in range(2):
                    value = terms[side][i][c * half : (c + 1) * half]
                    value = value + relay_buf[side, i, strip].astype(F32)
                    sums_send[side, i, strip] = value.astype(BF16)
                    remote(
                        sums_send.at[side, i, strip],
                        last_buf.at[2 + i, strip],
                        last_sem.at[1 + c],
                        peer_at(2 - i, 1 - side),
                        False,
                        1,
                    )
    others = (chips - 1) * (rows * cols + rows * pair_block)
    arrivals(others // width, slot_sem.at[0]).wait()
    slots = chips * rows
    down = dot(s_all[...].reshape(slots, pair_block), h_all[...].reshape(slots, cols), 0, 0)
    down_v[0] = down[:row_block]
    down_v[1] = down[row_block:]
    remote(down_v.at[1 - core], down_buf, down_sem.at[0], partner)

    arrivals((n_exp - 1) * part, r_sem.at[0]).wait()
    gin_ref[...] = dot(mix_v[...], r_buf[...].reshape(rows, width), 0, 0).astype(BF16)

    factor = 1.0 / (micro * n_dp)
    pltpu.make_async_copy(down_buf, down_buf, down_sem.at[0]).wait()
    gd_ref[...] = (down_v[core] + down_buf[...]) * factor
    halves = 2 * row_block * cols // width
    arrivals(halves, last_sem.at[0]).wait()
    gg_ref[...] = (total[:, :cols] + last_buf[0].astype(F32)) * factor
    gu_ref[...] = (total[:, cols:] + last_buf[1].astype(F32)) * factor
    for c, strip in enumerate(strips):
        arrivals(halves // 2, last_sem.at[1 + c]).wait()
        gg_ref[strip] = gg_ref[strip] + last_buf[2, strip].astype(F32) * factor
        gu_ref[strip] = gu_ref[strip] + last_buf[3, strip].astype(F32) * factor

    @pl.when(core == 1)
    def _():
        arrivals(4 * row_block * cols // width, sent_sem.at[1]).wait()

    arrivals(sum(sent) // width, sent_sem.at[0]).wait()


def settle(*refs):
    count = len(refs) // 2 - 1
    sized, sem = refs[-2:]
    for i in range(count):
        strip = refs[i].shape[0] // 4
        for c in range(4):
            span = pl.ds(c * strip, strip)
            pltpu.make_async_copy(refs[i].at[span], refs[count + i].at[span], sem.at[0]).start()
    pltpu.make_async_copy(sized, sized, sem.at[0]).wait()


def settled(arrays):
    anywhere = pl.BlockSpec(memory_space=pl.ANY)
    words = sum(a.size * a.dtype.itemsize // 2 for a in arrays)
    return pl.pallas_call(
        settle,
        out_shape=tuple(jax.ShapeDtypeStruct(a.shape, a.dtype) for a in arrays),
        in_specs=[pl.BlockSpec(memory_space=pltpu.VMEM)] * len(arrays),
        out_specs=(anywhere,) * len(arrays),
        scratch_shapes=[
            pltpu.VMEM((words // arrays[0].shape[1], arrays[0].shape[1]), BF16),
            pltpu.SemaphoreType.DMA((1,)),
        ],
    )(*[pltpu.with_memory_space_constraint(a, pltpu.VMEM) for a in arrays])


def pooled_call(n_exp, n_dp, grad_out, routes, route_probs, dispatched, w_gate, w_up, w_down):
    micro, tok_dev, width = grad_out.shape
    cols = w_gate.shape[1]
    tokens = micro * tok_dev
    part = micro * CAPS
    rows = n_exp * part
    chips = n_dp // 2
    row_block = width // n_dp
    vmem = pl.BlockSpec(memory_space=pltpu.VMEM)
    hbm = pl.BlockSpec(memory_space=pl.ANY)
    grad = pltpu.VMEM((row_block, cols), F32)
    dma = pltpu.SemaphoreType.DMA
    return pl.pallas_call(
        functools.partial(pooled_kernel, micro, n_exp, n_dp),
        out_shape=(pltpu.VMEM((tokens, width), BF16), grad, grad, grad),
        in_specs=[hbm] * 7,
        out_specs=(vmem, vmem, vmem, vmem),
        scratch_shapes=[
            pltpu.VMEM((micro, routes.shape[2], tok_dev), jnp.int32),
            pltpu.VMEM((micro, routes.shape[2], tok_dev), BF16),
            pltpu.VMEM((tokens, width), BF16),
            pltpu.VMEM((n_exp, part, width), BF16),
            pltpu.VMEM((n_exp, part, width), BF16),
            pltpu.VMEM((chips + 2, row_block, 2 * rows), BF16),
            pltpu.VMEM((width, cols), BF16),
            pltpu.VMEM((width, cols), BF16),
            pltpu.VMEM((cols, width), BF16),
            pltpu.VMEM((width, cols), BF16),
            pltpu.VMEM((2 * cols, width), BF16),
            pltpu.VMEM((n_exp // 2, part, width), BF16),
            pltpu.VMEM((n_exp, part, width), BF16),
            pltpu.VMEM((n_exp, part, width), BF16),
            pltpu.VMEM((n_exp, part, width), BF16),
            pltpu.VMEM((rows, tokens), BF16),
            pltpu.VMEM((2, rows, 2 * cols), BF16),
            pltpu.VMEM((2, 2, row_block, cols), BF16),
            pltpu.VMEM((6, row_block, cols), BF16),
            pltpu.VMEM((4, row_block, cols), BF16),
            pltpu.VMEM((2, 2, row_block, cols), BF16),
            pltpu.VMEM((chips, n_exp, part, 2 * row_block), BF16),
            pltpu.VMEM((chips, rows, cols), BF16),
            pltpu.VMEM((2, row_block, cols), F32),
            pltpu.VMEM((row_block, cols), F32),
            pltpu.VMEM((width, width), BF16),
            dma((4,)),
            dma((2,)),
            dma((n_exp - 1,)),
            dma((1,)),
            dma((1,)),
            dma((1,)),
            dma((2, 2)),
            dma((3,)),
            dma((1,)),
            dma((1,)),
            pltpu.SemaphoreType.REGULAR,
        ],
        compiler_params=pltpu.CompilerParams(collective_id=0, has_side_effects=True),
    )(
        routes.transpose(0, 2, 1),
        route_probs.transpose(0, 2, 1),
        grad_out.reshape(tokens, width),
        dispatched.reshape(micro, n_exp, CAPS, width),
        w_gate,
        w_up,
        w_down,
    )


def spread_call(n_exp, n_dp, grad_out, routes, route_probs, dispatched, w_gate, w_up, w_down):
    micro, tok_dev, width = grad_out.shape
    cols = w_gate.shape[1]
    tokens = micro * tok_dev
    part = micro * CAPS
    rows = n_exp * part
    chips = n_dp // 2
    row_block = width // n_dp
    vmem = pl.BlockSpec(memory_space=pltpu.VMEM)
    hbm = pl.BlockSpec(memory_space=pl.ANY)
    grad = pltpu.VMEM((row_block, cols), F32)
    dma = pltpu.SemaphoreType.DMA
    others = max(chips - 1, 1)
    gather = row_block % 128 == 0
    return pl.pallas_call(
        functools.partial(kernel, micro, n_exp, n_dp),
        out_shape=(pltpu.VMEM((tokens, width), BF16), grad, grad, grad),
        in_specs=[vmem, vmem, hbm, hbm, hbm, hbm, hbm],
        out_specs=(vmem, vmem, vmem, vmem),
        scratch_shapes=[
            pltpu.VMEM((tokens, width), BF16),
            pltpu.VMEM((rows, width), BF16),
            pltpu.VMEM((width, cols), BF16),
            pltpu.VMEM((width, cols), BF16),
            pltpu.VMEM((cols, width), BF16),
            pltpu.VMEM((n_exp, part, width), BF16),
            pltpu.VMEM((n_exp, part, width), BF16),
            pltpu.VMEM((n_exp, part, width), BF16),
            pltpu.VMEM((n_exp, part, width), BF16),
            pltpu.VMEM((3, 2, chips, row_block, cols), F32),
            pltpu.VMEM((3, 2, chips, row_block, cols), BF16),
            pltpu.VMEM((3, chips, row_block, cols), BF16),
            pltpu.VMEM((3, chips, row_block, cols), BF16),
            pltpu.VMEM((3, others, row_block, cols), BF16),
            pltpu.VMEM((n_dp, n_exp, part, row_block) if gather else (8, 128), BF16),
            pltpu.VMEM((n_dp, rows, cols) if gather else (8, 128), BF16),
            dma((5,)),
            dma((n_exp - 1,)),
            dma((n_exp - 1,)),
            dma((n_exp - 1,)),
            dma((n_exp - 1,)),
            dma((3,)),
            dma((3,)),
            dma((3, others)),
            dma((3, others)),
            dma((n_dp - 1,)),
            dma((n_dp - 1,)),
            dma((n_dp - 1,)),
            dma((n_dp - 1,)),
        ],
        compiler_params=pltpu.CompilerParams(collective_id=0, has_side_effects=True),
    )(
        routes.transpose(0, 2, 1),
        route_probs.transpose(0, 2, 1),
        grad_out.reshape(tokens, width),
        dispatched.reshape(rows, width),
        w_gate,
        w_up,
        w_down,
    )


def per_device(n_exp, n_dp, grad_out, *rest):
    pooled = n_exp == 4 and n_dp == 8 and (grad_out.shape[2] // n_dp) % 128 == 0
    call = pooled_call if pooled else spread_call
    out = settled(call(n_exp, n_dp, grad_out, *rest))
    return (out[0].reshape(grad_out.shape),) + tuple(out[1:])


def solution(mesh):
    return jax.shard_map(
        functools.partial(per_device, mesh.shape["expert"], mesh.shape["dp"]),
        mesh=mesh,
        in_specs=(
            P(None, ("dp", "expert"), None),
            P(None, ("dp", "expert"), None),
            P(None, ("dp", "expert"), None),
            P(None, ("dp", "expert"), None),
            P(None, "expert"),
            P(None, "expert"),
            P("expert", None),
        ),
        out_specs=(
            P(None, ("dp", "expert"), None),
            P("dp", "expert"),
            P("dp", "expert"),
            P("dp", "expert"),
        ),
        check_vma=False,
    )
```

```python
import functools

import jax
import jax.numpy as jnp
from jax import lax
from jax.experimental import pallas as pl
from jax.experimental.pallas import tpu as pltpu
from jax.sharding import PartitionSpec as P

CAPS = 8
MESH = pl.DeviceIdType.MESH
BF16 = jnp.bfloat16
F32 = jnp.float32


def dot(left, right, lc, rc):
    return lax.dot_general(
        left, right, (((lc,), (rc,)), ((), ())), preferred_element_type=F32
    )


def flipped(index, bits):
    step = 1
    while step <= bits:
        if bits & step:
            index = index + step - 2 * step * lax.rem(lax.div(index, step), 2)
        step *= 2
    return index


def kernel(
    micro,
    n_exp,
    n_dp,
    routes_ref,
    probs_ref,
    go_hbm,
    x_hbm,
    wg_hbm,
    wu_hbm,
    wd_hbm,
    gin_ref,
    gg_ref,
    gu_ref,
    gd_ref,
    go_v,
    x_v,
    wg_v,
    wu_v,
    wd_v,
    a_send,
    a_buf,
    r_send,
    r_buf,
    acc,
    p1_send,
    p1_buf,
    p2_send,
    p2_buf,
    s_all,
    h_all,
    load_sem,
    a_ssem,
    a_rsem,
    r_ssem,
    r_rsem,
    p1_ssem,
    p1_rsem,
    p2_ssem,
    p2_rsem,
    s_ssem,
    s_rsem,
    h_ssem,
    h_rsem,
):
    member = lax.axis_index("expert")
    replica = lax.axis_index("dp")
    core = lax.rem(replica, 2)
    chip = lax.div(replica, 2)
    chips = n_dp // 2
    partner = {"dp": chip * 2 + 1 - core}
    window = n_exp // 2
    tokens = go_v.shape[0]
    width = go_v.shape[1]
    tok_dev = tokens // micro
    part = micro * CAPS
    rows = n_exp * part
    row_block = width // n_dp
    gather = row_block % 128 == 0

    def member_at(k):
        return flipped(member, k)

    def chip_at(k):
        return {"dp": flipped(chip, k) * 2 + core}

    loads = [
        pltpu.make_async_copy(src, dst, load_sem.at[i])
        for i, (src, dst) in enumerate(
            ((go_hbm, go_v), (x_hbm, x_v), (wg_hbm, wg_v), (wu_hbm, wu_v), (wd_hbm, wd_v))
        )
    ]
    for load in loads:
        load.start()

    barrier = pltpu.get_barrier_semaphore()
    for k in range(1, n_exp):
        pl.semaphore_signal(
            barrier, inc=1, device_id={"expert": member_at(k)}, device_id_type=MESH
        )
    for k in range(1, n_dp):
        pl.semaphore_signal(
            barrier, inc=1, device_id={"dp": flipped(replica, k)}, device_id_type=MESH
        )

    ids = jnp.concatenate([routes_ref[m] for m in range(micro)], axis=1)
    probs = jnp.concatenate([probs_ref[m].astype(F32) for m in range(micro)], axis=1)
    pad = max(window, 8)
    expert_row = lax.broadcasted_iota(jnp.int32, (pad, tokens), 0)
    hits, weights = [], []
    table = jnp.zeros((pad, tokens), F32)
    for e in range(window):
        named = ids == e
        hits.append(jnp.sum(jnp.where(named, 1.0, 0.0), axis=0, keepdims=True))
        weights.append(jnp.sum(jnp.where(named, probs, 0.0), axis=0, keepdims=True))
        table = jnp.where(expert_row == e, hits[e], table)
    ti = lax.broadcasted_iota(jnp.int32, (tokens, tokens), 0)
    tj = lax.broadcasted_iota(jnp.int32, (tokens, tokens), 1)
    earlier = jnp.where((ti < tj) & (lax.div(ti, tok_dev) == lax.div(tj, tok_dev)), 1.0, 0.0)
    ranking = dot(table.astype(BF16), earlier.astype(BF16), 1, 0)
    slot = lax.broadcasted_iota(jnp.int32, (CAPS, tokens), 0).astype(F32)
    batch = lax.div(lax.broadcasted_iota(jnp.int32, (CAPS, tokens), 1), tok_dev)
    ones, scales = [], []
    for h in range(n_exp):
        e = h // 2
        chosen = (hits[e] > 0.5) & (ranking[e : e + 1] == slot)
        for m in range(micro):
            here = chosen & (batch == m)
            ones.append(jnp.where(here, 1.0, 0.0))
            scales.append(jnp.where(here, weights[e], 0.0))
    mixing = jnp.concatenate(ones, axis=0).astype(BF16)
    picking = jnp.concatenate(scales, axis=0).astype(BF16)

    loads[0].wait()
    sending = dot(picking, go_v[...], 1, 0).astype(BF16)
    for h in range(n_exp):
        a_send[h] = sending[h * part : (h + 1) * part]
    pl.semaphore_wait(barrier, n_exp - 1 + n_dp - 1)
    def a_copy(k, src, slot, to):
        return pltpu.make_async_remote_copy(
            src_ref=src,
            dst_ref=a_buf.at[slot],
            send_sem=a_ssem.at[k - 1],
            recv_sem=a_rsem.at[k - 1],
            device_id={"expert": to},
            device_id_type=MESH,
        )

    a_copies = {}
    for k in range(1, n_exp):
        a_copies[k] = a_copy(k, a_send.at[member_at(k)], member, member_at(k))
        a_copies[k].start()
    a_buf[member] = a_send[member]

    loads[1].wait()
    ri = lax.broadcasted_iota(jnp.int32, (rows, rows), 0)
    rj = lax.broadcasted_iota(jnp.int32, (rows, rows), 1)
    wanted = (
        lax.rem(lax.div(ri, CAPS), micro) * (n_exp * CAPS)
        + lax.div(ri, part) * CAPS
        + lax.rem(ri, CAPS)
    )
    inputs = dot(jnp.where(rj == wanted, 1.0, 0.0).astype(BF16), x_v[...], 1, 0).astype(BF16)
    loads[2].wait()
    gate = dot(inputs, wg_v[...], 1, 0)
    loads[3].wait()
    up = dot(inputs, wu_v[...], 1, 0)
    sigmoid = jax.nn.sigmoid(gate)
    activated = gate * sigmoid
    hidden = (activated * up).astype(BF16)
    h_copies, s_copies = [], []
    if gather:
        h_all[replica] = hidden
        for k in range(n_dp - 1, 0, -1):
            copy = pltpu.make_async_remote_copy(
                src_ref=h_all.at[replica],
                dst_ref=h_all.at[replica],
                send_sem=h_ssem.at[k - 1],
                recv_sem=h_rsem.at[k - 1],
                device_id={"dp": flipped(replica, k)},
                device_id_type=MESH,
            )
            copy.start()
            h_copies.append(copy)
    slope = up * sigmoid * (1.0 + gate * (1.0 - sigmoid))
    loads[4].wait()

    def p1_copy(o):
        return pltpu.make_async_remote_copy(
            src_ref=p1_send.at[o, 1 - core],
            dst_ref=p1_buf.at[o],
            send_sem=p1_ssem.at[o],
            recv_sem=p1_rsem.at[o],
            device_id=partner,
            device_id_type=MESH,
        )

    def store_terms(o, value):
        for d in range(n_dp):
            block = value[d * row_block : (d + 1) * row_block]
            acc[o, d % 2, d // 2] = block
            p1_send[o, d % 2, d // 2] = block.astype(BF16)

    p1_copies, p2_copies = {}, {}

    def start_p1(o, value):
        store_terms(o, value)
        p1_copies[o] = p1_copy(o)
        p1_copies[o].start()

    def start_p2(o):
        p1_copies[o].wait_recv()
        for k in range(chips - 1, 0, -1):
            q = flipped(chip, k)
            p2_send[o, q] = (acc[o, core, q] + p1_buf[o, q].astype(F32)).astype(BF16)
            copy = pltpu.make_async_remote_copy(
                src_ref=p2_send.at[o, q],
                dst_ref=p2_buf.at[o, k - 1],
                send_sem=p2_ssem.at[o, k - 1],
                recv_sem=p2_rsem.at[o, k - 1],
                device_id=chip_at(k),
                device_id_type=MESH,
            )
            copy.start()
            p2_copies[o, k] = copy

    for k in range(1, n_exp):
        a_copies[k].wait_recv()
    scaled = a_buf[...].reshape(rows, width)
    if gather:
        for k in range(n_dp - 1, 0, -1):
            peer = flipped(replica, k)
            columns = pl.ds(pl.multiple_of(peer * row_block, row_block), row_block)
            copy = pltpu.make_async_remote_copy(
                src_ref=a_buf.at[:, :, columns],
                dst_ref=s_all.at[replica],
                send_sem=s_ssem.at[k - 1],
                recv_sem=s_rsem.at[k - 1],
                device_id={"dp": peer},
                device_id_type=MESH,
            )
            copy.start()
            s_copies.append(copy)
    else:
        start_p1(0, dot(scaled, hidden, 0, 0))
    dhidden = dot(scaled, wd_v[...], 1, 1)
    d_gate = (dhidden * slope).astype(BF16)
    d_up = (dhidden * activated).astype(BF16)
    returning = (dot(d_gate, wg_v[...], 1, 1) + dot(d_up, wu_v[...], 1, 1)).astype(BF16)
    for h in range(n_exp):
        r_send[h] = returning[h * part : (h + 1) * part]
    r_copies = []
    for k in range(n_exp - 1, 0, -1):
        copy = pltpu.make_async_remote_copy(
            src_ref=r_send.at[member_at(k)],
            dst_ref=r_buf.at[member],
            send_sem=r_ssem.at[k - 1],
            recv_sem=r_rsem.at[k - 1],
            device_id={"expert": member_at(k)},
            device_id_type=MESH,
        )
        copy.start()
        r_copies.append(copy)
    start_p1(1, dot(inputs, d_gate, 0, 0))
    start_p1(2, dot(inputs, d_up, 0, 0))
    if not gather:
        start_p2(0)
    r_buf[member] = r_send[member]
    start_p2(1)
    start_p2(2)

    if gather:
        own = pl.ds(pl.multiple_of(replica * row_block, row_block), row_block)
        s_all[replica] = a_buf[:, :, own]
        for copy in h_copies + s_copies:
            copy.wait_recv()
        slots = n_dp * rows
        down = dot(
            s_all[...].reshape(slots, row_block), h_all[...].reshape(slots, wg_v.shape[1]), 0, 0
        )
        gd_ref[...] = down * (1.0 / (micro * n_dp))
    for copy in r_copies:
        copy.wait_recv()
    gin_ref[...] = dot(mixing, r_buf[...].reshape(rows, width), 0, 0).astype(BF16)

    factor = 1.0 / (micro * n_dp)
    for o, out in enumerate((gd_ref, gg_ref, gu_ref)):
        if o not in p1_copies:
            continue
        total = acc[o, core, chip] + p1_buf[o, chip].astype(F32)
        for k in range(chips - 1, 0, -1):
            p2_copies[o, k].wait_recv()
            total = total + p2_buf[o, k - 1].astype(F32)
        out[...] = total * factor
    started = [*a_copies.values(), *p1_copies.values(), *p2_copies.values()]
    for copy in started + r_copies + h_copies + s_copies:
        copy.wait_send()


def pooled_kernel(
    micro,
    n_exp,
    n_dp,
    routes_hbm,
    probs_hbm,
    go_hbm,
    x_hbm,
    wg_hbm,
    wu_hbm,
    wd_hbm,
    gin_ref,
    gg_ref,
    gu_ref,
    gd_ref,
    routes_v,
    probs_v,
    go_v,
    x_v,
    x_par,
    xt_v,
    wg_v,
    wu_v,
    wd_v,
    wdt_v,
    wgt_v,
    a_send,
    a_buf,
    r_send,
    r_buf,
    mix_v,
    d_all,
    relay_buf,
    last_send,
    last_buf,
    sums_send,
    s_all,
    h_all,
    down_v,
    down_buf,
    sized,
    load_sem,
    sent_sem,
    a_sem,
    r_sem,
    x_sem,
    d_sem,
    relay_sem,
    last_sem,
    slot_sem,
    down_sem,
    turn_sem,
):
    member = lax.axis_index("expert")
    replica = lax.axis_index("dp")
    core = lax.rem(replica, 2)
    chip = lax.div(replica, 2)
    chips = n_dp // 2
    partner = {"dp": chip * 2 + 1 - core}
    window = n_exp // 2
    tokens, width = go_v.shape
    cols = wg_v.shape[1]
    tok_dev = tokens // micro
    part = micro * CAPS
    rows = n_exp * part
    row_block = width // n_dp
    pair_block = 2 * row_block
    hops = range(chips - 1, 0, -1)

    def chip_at(k):
        return flipped(chip, k)

    def peer_at(k, side=core):
        return {"dp": chip_at(k) * 2 + side}

    loads = [
        pltpu.make_async_copy(src, dst, load_sem.at[min(i, 3)])
        for i, (src, dst) in enumerate(
            (
                (routes_hbm, routes_v),
                (probs_hbm, probs_v),
                (go_hbm, go_v),
                *((x_hbm.at[m], x_v.at[:, pl.ds(m * CAPS, CAPS), :]) for m in range(micro)),
                (wg_hbm, wg_v),
                (wu_hbm, wu_v),
                (wd_hbm, wd_v),
            )
        )
    ]
    for load in loads[:3]:
        load.start()

    barrier = pltpu.get_barrier_semaphore()
    for k in range(n_exp - 1, 0, -1):
        pl.semaphore_signal(
            barrier, inc=1, device_id={"expert": flipped(member, k)}, device_id_type=MESH
        )
    for k in hops:
        pl.semaphore_signal(barrier, inc=1, device_id=peer_at(k), device_id_type=MESH)
    pl.semaphore_signal(barrier, inc=1, device_id=partner, device_id_type=MESH)
    for k in (1, 2):
        pl.semaphore_signal(barrier, inc=1, device_id=peer_at(k, 1 - core), device_id_type=MESH)

    def arrivals(size, sem):
        return pltpu.make_async_copy(sized.at[pl.ds(0, size)], sized.at[pl.ds(0, size)], sem)

    sent = []

    def remote(src, dst, sem, device, counted=True, group=0):
        copy = pltpu.make_async_remote_copy(
            src_ref=src,
            dst_ref=dst,
            send_sem=sent_sem.at[group],
            recv_sem=sem,
            device_id=device,
            device_id_type=MESH,
        )
        copy.start()
        if counted:
            bulk = 1
            for n in src.shape:
                bulk *= n
            sent.append(bulk * (2 if src.dtype == F32 else 1))

    pad = max(window, 8)
    expert_row = lax.broadcasted_iota(jnp.int32, (pad, tokens), 0)
    ti = lax.broadcasted_iota(jnp.int32, (tokens, tokens), 0)
    tj = lax.broadcasted_iota(jnp.int32, (tokens, tokens), 1)
    earlier = jnp.where((ti < tj) & (lax.div(ti, tok_dev) == lax.div(tj, tok_dev)), 1.0, 0.0)
    loads[0].wait()
    loads[1].wait()
    ids = jnp.concatenate([routes_v[m] for m in range(micro)], axis=1)
    probs = jnp.concatenate([probs_v[m].astype(F32) for m in range(micro)], axis=1)
    hits, weights = [], []
    table = jnp.zeros((pad, tokens), F32)
    for e in range(window):
        named = ids == e
        hits.append(jnp.sum(jnp.where(named, 1.0, 0.0), axis=0, keepdims=True))
        weights.append(jnp.sum(jnp.where(named, probs, 0.0), axis=0, keepdims=True))
        table = jnp.where(expert_row == e, hits[e], table)
    ranking = dot(table.astype(BF16), earlier.astype(BF16), 1, 0)
    slot = lax.broadcasted_iota(jnp.int32, (CAPS, tokens), 0).astype(F32)
    batch = lax.div(lax.broadcasted_iota(jnp.int32, (CAPS, tokens), 1), tok_dev)
    ones, scales = [], []
    for e in range(window):
        chosen = (hits[e] > 0.5) & (ranking[e : e + 1] == slot)
        for m in range(micro):
            here = chosen & (batch == m)
            ones.append(jnp.where(here, 1.0, 0.0))
            scales.append(jnp.where(here, weights[e], 0.0))
    picking = jnp.concatenate(scales, axis=0).astype(BF16)

    loads[2].wait()
    for load in loads[3:]:
        load.start()
    sending = dot(picking, go_v[...], 1, 0).astype(BF16)
    for e in range(window):
        a_send[e] = sending[e * part : (e + 1) * part]
    pl.semaphore_wait(barrier, n_exp - 1 + chips + 2)

    inner = jnp.where((member == 0) | (member == n_exp - 1), 0, 1)
    outer = (1 - inner) * (1 - core)
    order = [1 + inner + 2 * outer, 3 - 2 * outer, 2 - inner]
    arriving = [1, 3, 2]

    def member_at(k):
        low, high = lax.rem(k, 2), lax.div(k, 2)
        low = low * (1 - 2 * lax.rem(member, 2))
        high = high * (2 - 4 * lax.div(member, 2))
        return member + low + high

    for k in order:
        to = member_at(k)
        remote(a_send.at[lax.div(to, 2)], a_buf.at[member], a_sem.at[k - 1], {"expert": to})
    a_buf[member] = a_send[lax.div(member, 2)]

    weights_rows = width * cols // width
    arrivals(rows + 3 * weights_rows, load_sem.at[3]).wait()
    remote(x_v, x_par, x_sem.at[0], partner)
    inputs = x_v[...].reshape(rows, width)
    gate = dot(inputs, wg_v[...], 1, 0)
    up = dot(inputs, wu_v[...], 1, 0)
    sigmoid = jax.nn.sigmoid(gate)
    activated = gate * sigmoid
    h_all[chip] = (activated * up).astype(BF16)
    for k in hops:
        remote(h_all.at[chip], h_all.at[chip], slot_sem.at[0], peer_at(k))
    slope = up * sigmoid * (1.0 + gate * (1.0 - sigmoid))

    def blocks(q):
        return pl.ds(pl.multiple_of(q * pair_block, pair_block), pair_block)

    def send_slices(source, counted=True):
        for k in hops:
            remote(
                a_buf.at[source, :, blocks(chip_at(k))],
                s_all.at[chip, source],
                slot_sem.at[0],
                peer_at(k),
                counted,
            )

    send_slices(member)

    mix_v[...] = jnp.concatenate(
        [
            jnp.concatenate(ones[e * micro : (e + 1) * micro], axis=0)
            for e in range(window)
            for _ in range(2)
        ],
        axis=0,
    ).astype(BF16)
    wdt_v[...] = wd_v[...].T
    wgt_v[:cols] = wg_v[...].T
    wgt_v[cols:] = wu_v[...].T
    pltpu.make_async_copy(x_par, x_par, x_sem.at[0]).wait()
    for j in range(chips + 2):
        k, side = (j, core) if j < chips else (j - chips + 1, 0)
        q = chip_at(k) if k else chip
        own = pl.ds(pl.multiple_of((q * 2 + side) * row_block, row_block), row_block)
        mine = x_v[:, :, own].reshape(rows, row_block)
        other = x_par[:, :, own].reshape(rows, row_block)
        xt_v[j] = jnp.concatenate([mine, other], axis=0).T

    for j, k in enumerate(arriving):
        source = member_at(k)
        pltpu.make_async_copy(a_buf.at[source], a_buf.at[source], a_sem.at[k - 1]).wait()
        if j < n_exp - 2:
            send_slices(source)
    scaled = a_buf[...].reshape(rows, width)
    dhidden = dot(scaled, wdt_v[...], 1, 0)
    d_all[0, :, :cols] = (dhidden * slope).astype(BF16)
    d_all[0, :, cols:] = (dhidden * activated).astype(BF16)
    remote(d_all.at[0], d_all.at[1], d_sem.at[0], partner)

    @pl.when(core == 1)
    def _():
        send_slices(member_at(arriving[-1]), False)

    sent.append((chips - 1) * part * pair_block)

    def send_rows(to):
        remote(r_send.at[to], r_buf.at[member], r_sem.at[0], {"expert": to}, False)

    def send_back():
        returning = dot(d_all[0], wgt_v[...], 1, 0)
        returning = returning.astype(BF16)
        for h in range(n_exp):
            r_send[h] = returning[h * part : (h + 1) * part]
        for k in (3 - inner, 1):
            send_rows(member_at(k))

        @pl.when(core == 0)
        def _():
            send_rows(member_at(2 + inner))


    sent.append((n_exp - 1) * part * width)
    returns_first = (core == 1) | (member != 0)

    @pl.when(returns_first)
    def _():
        send_back()

    pltpu.make_async_copy(d_all.at[1], d_all.at[1], d_sem.at[0]).wait()
    factors = d_all[...].reshape(2 * rows, 2 * cols)
    half = row_block // 2
    strips = [pl.ds(c * half, half) for c in range(2)]
    far = dot(xt_v[3], factors, 1, 0)
    for i in range(2):
        last_send[4 + i] = far[:, i * cols : (i + 1) * cols].astype(BF16)
    for c, strip in enumerate(strips):
        for i in range(2):
            remote(
                last_send.at[4 + i, strip],
                relay_buf.at[1 - core, i, strip],
                relay_sem.at[1 - core, c],
                peer_at(1 + i, 1),
            )

    @pl.when(core == 1)
    def _():
        pl.semaphore_signal(turn_sem, inc=1, device_id=partner, device_id_type=MESH)

    near = [dot(xt_v[k], factors, 1, 0) for k in (1, 2)]
    last_send[0] = near[0][:, :cols].astype(BF16)
    last_send[1] = near[1][:, cols:].astype(BF16)
    total = dot(xt_v[0], factors, 1, 0)
    @pl.when(jnp.logical_not(returns_first))
    def _():
        send_back()

    r_buf[member] = r_send[member]
    s_all[chip] = a_buf[:, :, blocks(chip)]

    @pl.when(core == 0)
    def _():
        pl.semaphore_wait(turn_sem, 1)


    @pl.when(core == 0)
    def _():
        send_slices(member_at(arriving[-1]), False)

    @pl.when(core == 0)
    def _():
        for i in range(2):
            remote(last_send.at[i], last_buf.at[i], last_sem.at[0], peer_at(1 + i), False)

    sent.append(2 * row_block * cols)
    @pl.when(core == 1)
    def _():
        extra = [
            dot(xt_v[chips + 1], factors[:, :cols], 1, 0),
            dot(xt_v[chips], factors[:, cols:], 1, 0),
        ]
        terms = [[near[1][:, :cols], near[0][:, cols:]], extra]
        for side in (1, 0):
            for c, strip in enumerate(strips):
                arrivals(2 * half * cols // width, relay_sem.at[side, c]).wait()
                if side == 1 and c == 0:
                    send_rows(member_at(2 + inner))
                    for i in range(2):
                        remote(
                            last_send.at[i], last_buf.at[i], last_sem.at[0], peer_at(1 + i), False
                        )
                for i in range(2):
                    value = terms[side][i][c * half : (c + 1) * half]
                    value = value + relay_buf[side, i, strip].astype(F32)
                    sums_send[side, i, strip] = value.astype(BF16)
                    remote(
                        sums_send.at[side, i, strip],
                        last_buf.at[2 + i, strip],
                        last_sem.at[1 + c],
                        peer_at(2 - i, 1 - side),
                        False,
                        1,
                    )
    others = (chips - 1) * (rows * cols + rows * pair_block)
    arrivals(others // width, slot_sem.at[0]).wait()
    slots = chips * rows
    down = dot(s_all[...].reshape(slots, pair_block), h_all[...].reshape(slots, cols), 0, 0)
    down_v[0] = down[:row_block]
    down_v[1] = down[row_block:]
    remote(down_v.at[1 - core], down_buf, down_sem.at[0], partner)

    arrivals((n_exp - 1) * part, r_sem.at[0]).wait()
    gin_ref[...] = dot(mix_v[...], r_buf[...].reshape(rows, width), 0, 0).astype(BF16)

    factor = 1.0 / (micro * n_dp)
    pltpu.make_async_copy(down_buf, down_buf, down_sem.at[0]).wait()
    gd_ref[...] = (down_v[core] + down_buf[...]) * factor
    halves = 2 * row_block * cols // width
    arrivals(halves, last_sem.at[0]).wait()
    gg_ref[...] = (total[:, :cols] + last_buf[0].astype(F32)) * factor
    gu_ref[...] = (total[:, cols:] + last_buf[1].astype(F32)) * factor
    for c, strip in enumerate(strips):
        arrivals(halves // 2, last_sem.at[1 + c]).wait()
        gg_ref[strip] = gg_ref[strip] + last_buf[2, strip].astype(F32) * factor
        gu_ref[strip] = gu_ref[strip] + last_buf[3, strip].astype(F32) * factor

    @pl.when(core == 1)
    def _():
        arrivals(4 * row_block * cols // width, sent_sem.at[1]).wait()

    arrivals(sum(sent) // width, sent_sem.at[0]).wait()


def settle(*refs):
    count = len(refs) // 2 - 1
    sized, sem = refs[-2:]
    for i in range(count):
        strip = refs[i].shape[0] // 4
        for c in range(4):
            span = pl.ds(c * strip, strip)
            pltpu.make_async_copy(refs[i].at[span], refs[count + i].at[span], sem.at[0]).start()
    pltpu.make_async_copy(sized, sized, sem.at[0]).wait()


def settled(arrays):
    anywhere = pl.BlockSpec(memory_space=pl.ANY)
    words = sum(a.size * a.dtype.itemsize // 2 for a in arrays)
    return pl.pallas_call(
        settle,
        out_shape=tuple(jax.ShapeDtypeStruct(a.shape, a.dtype) for a in arrays),
        in_specs=[pl.BlockSpec(memory_space=pltpu.VMEM)] * len(arrays),
        out_specs=(anywhere,) * len(arrays),
        scratch_shapes=[
            pltpu.VMEM((words // arrays[0].shape[1], arrays[0].shape[1]), BF16),
            pltpu.SemaphoreType.DMA((1,)),
        ],
    )(*[pltpu.with_memory_space_constraint(a, pltpu.VMEM) for a in arrays])


def pooled_call(n_exp, n_dp, grad_out, routes, route_probs, dispatched, w_gate, w_up, w_down):
    micro, tok_dev, width = grad_out.shape
    cols = w_gate.shape[1]
    tokens = micro * tok_dev
    part = micro * CAPS
    rows = n_exp * part
    chips = n_dp // 2
    row_block = width // n_dp
    vmem = pl.BlockSpec(memory_space=pltpu.VMEM)
    hbm = pl.BlockSpec(memory_space=pl.ANY)
    grad = pltpu.VMEM((row_block, cols), F32)
    dma = pltpu.SemaphoreType.DMA
    return pl.pallas_call(
        functools.partial(pooled_kernel, micro, n_exp, n_dp),
        out_shape=(pltpu.VMEM((tokens, width), BF16), grad, grad, grad),
        in_specs=[hbm] * 7,
        out_specs=(vmem, vmem, vmem, vmem),
        scratch_shapes=[
            pltpu.VMEM((micro, routes.shape[2], tok_dev), jnp.int32),
            pltpu.VMEM((micro, routes.shape[2], tok_dev), BF16),
            pltpu.VMEM((tokens, width), BF16),
            pltpu.VMEM((n_exp, part, width), BF16),
            pltpu.VMEM((n_exp, part, width), BF16),
            pltpu.VMEM((chips + 2, row_block, 2 * rows), BF16),
            pltpu.VMEM((width, cols), BF16),
            pltpu.VMEM((width, cols), BF16),
            pltpu.VMEM((cols, width), BF16),
            pltpu.VMEM((width, cols), BF16),
            pltpu.VMEM((2 * cols, width), BF16),
            pltpu.VMEM((n_exp // 2, part, width), BF16),
            pltpu.VMEM((n_exp, part, width), BF16),
            pltpu.VMEM((n_exp, part, width), BF16),
            pltpu.VMEM((n_exp, part, width), BF16),
            pltpu.VMEM((rows, tokens), BF16),
            pltpu.VMEM((2, rows, 2 * cols), BF16),
            pltpu.VMEM((2, 2, row_block, cols), BF16),
            pltpu.VMEM((6, row_block, cols), BF16),
            pltpu.VMEM((4, row_block, cols), BF16),
            pltpu.VMEM((2, 2, row_block, cols), BF16),
            pltpu.VMEM((chips, n_exp, part, 2 * row_block), BF16),
            pltpu.VMEM((chips, rows, cols), BF16),
            pltpu.VMEM((2, row_block, cols), F32),
            pltpu.VMEM((row_block, cols), F32),
            pltpu.VMEM((width, width), BF16),
            dma((4,)),
            dma((2,)),
            dma((n_exp - 1,)),
            dma((1,)),
            dma((1,)),
            dma((1,)),
            dma((2, 2)),
            dma((3,)),
            dma((1,)),
            dma((1,)),
            pltpu.SemaphoreType.REGULAR,
        ],
        compiler_params=pltpu.CompilerParams(collective_id=0, has_side_effects=True),
    )(
        routes.transpose(0, 2, 1),
        route_probs.transpose(0, 2, 1),
        grad_out.reshape(tokens, width),
        dispatched.reshape(micro, n_exp, CAPS, width),
        w_gate,
        w_up,
        w_down,
    )


def spread_call(n_exp, n_dp, grad_out, routes, route_probs, dispatched, w_gate, w_up, w_down):
    micro, tok_dev, width = grad_out.shape
    cols = w_gate.shape[1]
    tokens = micro * tok_dev
    part = micro * CAPS
    rows = n_exp * part
    chips = n_dp // 2
    row_block = width // n_dp
    vmem = pl.BlockSpec(memory_space=pltpu.VMEM)
    hbm = pl.BlockSpec(memory_space=pl.ANY)
    grad = pltpu.VMEM((row_block, cols), F32)
    dma = pltpu.SemaphoreType.DMA
    others = max(chips - 1, 1)
    gather = row_block % 128 == 0
    return pl.pallas_call(
        functools.partial(kernel, micro, n_exp, n_dp),
        out_shape=(pltpu.VMEM((tokens, width), BF16), grad, grad, grad),
        in_specs=[vmem, vmem, hbm, hbm, hbm, hbm, hbm],
        out_specs=(vmem, vmem, vmem, vmem),
        scratch_shapes=[
            pltpu.VMEM((tokens, width), BF16),
            pltpu.VMEM((rows, width), BF16),
            pltpu.VMEM((width, cols), BF16),
            pltpu.VMEM((width, cols), BF16),
            pltpu.VMEM((cols, width), BF16),
            pltpu.VMEM((n_exp, part, width), BF16),
            pltpu.VMEM((n_exp, part, width), BF16),
            pltpu.VMEM((n_exp, part, width), BF16),
            pltpu.VMEM((n_exp, part, width), BF16),
            pltpu.VMEM((3, 2, chips, row_block, cols), F32),
            pltpu.VMEM((3, 2, chips, row_block, cols), BF16),
            pltpu.VMEM((3, chips, row_block, cols), BF16),
            pltpu.VMEM((3, chips, row_block, cols), BF16),
            pltpu.VMEM((3, others, row_block, cols), BF16),
            pltpu.VMEM((n_dp, n_exp, part, row_block) if gather else (8, 128), BF16),
            pltpu.VMEM((n_dp, rows, cols) if gather else (8, 128), BF16),
            dma((5,)),
            dma((n_exp - 1,)),
            dma((n_exp - 1,)),
            dma((n_exp - 1,)),
            dma((n_exp - 1,)),
            dma((3,)),
            dma((3,)),
            dma((3, others)),
            dma((3, others)),
            dma((n_dp - 1,)),
            dma((n_dp - 1,)),
            dma((n_dp - 1,)),
            dma((n_dp - 1,)),
        ],
        compiler_params=pltpu.CompilerParams(collective_id=0, has_side_effects=True),
    )(
        routes.transpose(0, 2, 1),
        route_probs.transpose(0, 2, 1),
        grad_out.reshape(tokens, width),
        dispatched.reshape(rows, width),
        w_gate,
        w_up,
        w_down,
    )


def per_device(n_exp, n_dp, grad_out, *rest):
    pooled = n_exp == 4 and n_dp == 8 and (grad_out.shape[2] // n_dp) % 128 == 0
    call = pooled_call if pooled else spread_call
    out = settled(call(n_exp, n_dp, grad_out, *rest))
    return (out[0].reshape(grad_out.shape),) + tuple(out[1:])


def solution(mesh):
    return jax.shard_map(
        functools.partial(per_device, mesh.shape["expert"], mesh.shape["dp"]),
        mesh=mesh,
        in_specs=(
            P(None, ("dp", "expert"), None),
            P(None, ("dp", "expert"), None),
            P(None, ("dp", "expert"), None),
            P(None, ("dp", "expert"), None),
            P(None, "expert"),
            P(None, "expert"),
            P("expert", None),
        ),
        out_specs=(
            P(None, ("dp", "expert"), None),
            P("dp", "expert"),
            P("dp", "expert"),
            P("dp", "expert"),
        ),
        check_vma=False,
    )
```
